256 devices in a mesh: band: 32 (over z, y_hi, core), chan: 8 (over x, y_lo).
Axes of the slice: x: 4, y: 4 (y_hi: 2, y_lo: 2; y = y_hi * 2 + y_lo), z: 8, core: 2. Of those that a mesh axis runs over, the one named last changes fastest.
Arguments:
- fine_features: bfloat16 [2, 192, 256, 512], P(None, 'chan', 'band'), may hold values from -100 to 100
- coarse_level: bfloat16 [2, 256, 128, 256], P(None, 'chan', 'band'), may hold values from -100 to 100
- lat_weight: bfloat16 [256, 192], P('chan'), may hold values from -0.4375 to 0.4375
- lat_gain: bfloat16 [256], P('chan'), may hold values from 0.099609375 to 1.8984375
- lat_shift: bfloat16 [256], P('chan'), may hold values from -3 to 3
- out_weight: bfloat16 [3, 3, 256, 256], P(None, None, 'chan'), may hold values from -0.125 to 0.125
- out_gain: bfloat16 [256], P('chan'), may hold values from 0.099609375 to 1.8984375
- out_shift: bfloat16 [256], P('chan'), may hold values from -3 to 3
- mask_weight: bfloat16 [256, 256], P('chan'), may hold values from -0.375 to 0.375
- mask_bias: bfloat16 [256], P('chan'), may hold values from -1.796875 to 1.796875
- queries: bfloat16 [200, 256], replicated, may hold values from -128 to 128
Outputs:
- log_probs: float32 [2, 200, 256, 512], P(None, None, ('band', 'chan'))
The draws below stay inside these ranges and needn't reach their ends.
All inputs are finite; a program needn't handle non-finite values.
Results may differ from the reference program's by a relative error of at most 0.0058.
Values may be sent and summed in bfloat16 or wider, within the bound.
No kernel may reach another device: no remote copies, remote signals or barrier semaphores. Data moves between devices by JAX's collectives and lax.ppermute only.
A program may use at most 64 MiB of HBM per device.

```python
import jax
import jax.numpy as jnp
from jax import lax

D = 256
C4 = 192
QUERIES = 200
GROUPS = 32
IMAGES = 2
COLS = 512
H4 = 256


def banded_field(key, images, channels, height, width):
    key_noise = jax.random.fold_in(key, 0)
    key_rows = jax.random.fold_in(key, 1)
    key_cols = jax.random.fold_in(key, 2)
    key_offset = jax.random.fold_in(key, 4)
    positions = jnp.arange(height, dtype=jnp.float32) / max(height - 1, 1)
    ramp = 3.0 ** positions
    row_scale = ramp[None, :] * jnp.exp(jax.random.uniform(key_rows, (images, height), jnp.float32, -0.8, 0.8))
    col_scale = jnp.exp(jax.random.uniform(key_cols, (images, width), jnp.float32, -0.8, 0.8))
    scale = row_scale[:, None, :, None] * col_scale[:, None, None, :]
    offset = jax.random.uniform(key_offset, (images, channels, 1, 1), jnp.float32, -3.0, 3.0)
    noise = jax.random.truncated_normal(key_noise, -4.0, 4.0, (images, channels, height, width), jnp.float32)
    values = noise * scale + offset * ramp[None, None, :, None]
    return values


def draw_fine_features(key, part):
    return banded_field(jax.random.fold_in(key, 11), IMAGES, C4, H4, COLS).astype(jnp.bfloat16)


def draw_coarse_level(key, part):
    return banded_field(jax.random.fold_in(key, 12), IMAGES, D, H4 // 2, COLS // 2).astype(jnp.bfloat16)


def draw_queries(key, part):
    key_base = jax.random.fold_in(jax.random.fold_in(key, 13), 0)
    values = 0.25 * jax.random.truncated_normal(key_base, -4.0, 4.0, (QUERIES, D), jnp.float32)
    return values.astype(jnp.bfloat16)


def levels(own_key, extent, shards, smallest, high):
    factor_of = 1.0
    for axis_at, parts in shards:
        heights = jax.random.uniform(jax.random.fold_in(jax.random.fold_in(own_key, 6), axis_at), (parts,), jnp.float32, smallest / len(shards), high / len(shards))
        factor_of = factor_of * jnp.repeat(jnp.exp(heights), extent[axis_at] // parts).reshape((-1,) + (1,) * (len(extent) - 1 - axis_at))
    return factor_of


def bell_draw(stream_key, shape, spread, most, pieces=(), kind=jnp.bfloat16):
    values = jax.random.normal(stream_key, shape, jnp.float32) * spread
    if len(pieces) > 0:
        values = levels(stream_key, shape, pieces, -0.22, 0.18) * values
    return jnp.clip(values, min=-most, max=most).astype(kind)


def setup_inputs(seed: int = 0) -> dict:
    key_of = jax.random.split(jax.random.key(seed), 12)
    return {
        "fine_features": draw_fine_features(jax.random.fold_in(key_of[11], 71), 0),
        "coarse_level": draw_coarse_level(jax.random.fold_in(key_of[11], 71), 0),
        "lat_weight": bell_draw(key_of[2], (D, C4), C4 ** -0.5, 0.4375, ((0, 8),)),
        "lat_gain": jnp.clip(1.0 + 0.18 * jax.random.normal(key_of[3], (D,), jnp.float32), 0.099609375, 1.8984375).astype(jnp.bfloat16),
        "lat_shift": bell_draw(key_of[4], (D,), 0.5, 3.0, ((0, 8),)),
        "out_weight": bell_draw(key_of[5], (3, 3, D, D), (9 * D) ** -0.5, 0.125, ((2, 8),)),
        "out_gain": jnp.clip(1.0 + 0.18 * jax.random.normal(key_of[6], (D,), jnp.float32), 0.099609375, 1.8984375).astype(jnp.bfloat16),
        "out_shift": bell_draw(key_of[7], (D,), 0.5, 3.0, ((0, 8),)),
        "mask_weight": bell_draw(key_of[8], (D, D), D ** -0.5, 0.375, ((0, 8),)),
        "mask_bias": bell_draw(key_of[9], (D,), 0.3, 1.796875, ((0, 8),)),
        "queries": draw_queries(jax.random.fold_in(key_of[11], 71), 0),
    }


epsilon = 1e-05

def interp(padded, axis):
    length = padded.shape[axis] - 2
    before = lax.slice_in_dim(padded, 0, length, axis=axis)
    middle = lax.slice_in_dim(padded, 1, length + 1, axis=axis)
    after = lax.slice_in_dim(padded, 2, length + 2, axis=axis)
    even_part = 0.25 * before + 0.75 * middle
    odd_part = 0.75 * middle + 0.25 * after
    paired = jnp.stack([even_part, odd_part], axis + 1)
    new_shape = list(middle.shape)
    new_shape[axis] = 2 * length
    return paired.reshape(new_shape)

def group_norm(values, gain, shift, group_size):
    channels, height, width = values.shape
    blocks = values.reshape(channels // group_size, group_size * height * width)
    mean_value = lax.optimization_barrier(jnp.mean(blocks, axis=1, keepdims=True))
    deviation = blocks - mean_value
    variance = lax.optimization_barrier(jnp.mean(deviation * deviation, axis=1, keepdims=True))
    scaled = ((blocks - mean_value) * lax.rsqrt(variance + epsilon)).reshape(channels, height, width)
    return scaled * gain.astype(jnp.float32)[:, None, None] + shift.astype(jnp.float32)[:, None, None]

def reference(fine_features, coarse_level, lat_weight, lat_gain, lat_shift, out_weight, out_gain, out_shift, mask_weight, mask_bias, queries):
    group_size = D // GROUPS

    def one_image(pair):
        fine_image, coarse_image = pair
        lateral = jnp.dot(lat_weight, fine_image.reshape(C4, H4 * COLS), preferred_element_type=jnp.float32).reshape(D, H4, COLS)
        lat_normed = group_norm(lateral, lat_gain, lat_shift, group_size)
        extended = jnp.pad(coarse_image.astype(jnp.float32), ((0, 0), (1, 1), (1, 1)), mode='edge')
        upsampled = interp(interp(extended, 1), 2)
        joined = (lat_normed + upsampled).astype(jnp.bfloat16)
        padded = jnp.pad(joined, ((0, 0), (1, 1), (1, 1)))
        conv_out = jnp.zeros((D, H4 * COLS), jnp.float32)
        for row_tap in range(3):
            for col_tap in range(3):
                window = padded[:, row_tap:row_tap + H4, col_tap:col_tap + COLS].reshape(D, H4 * COLS)
                conv_out = conv_out + jnp.dot(out_weight[row_tap, col_tap], window, preferred_element_type=jnp.float32)
        conv_out = conv_out.reshape(D, H4, COLS)
        activated = jnp.maximum(group_norm(conv_out, out_gain, out_shift, group_size), 0.0).astype(jnp.bfloat16)
        features = jnp.dot(mask_weight, activated.reshape(D, H4 * COLS), preferred_element_type=jnp.float32)
        features = (features + mask_bias.astype(jnp.float32)[:, None]).astype(jnp.bfloat16)
        logits = jnp.dot(queries, features, preferred_element_type=jnp.float32)
        peak = lax.optimization_barrier(jnp.max(logits, axis=0, keepdims=True))
        shifted = logits - peak
        result = shifted - jnp.log(lax.optimization_barrier(jnp.sum(jnp.exp(shifted), axis=0, keepdims=True)))
        return result.reshape(QUERIES, H4, COLS)
    return lax.map(one_image, (fine_features, coarse_level))
```

```python
import functools

import jax
import jax.numpy as jnp
from jax import lax
from jax.experimental import pallas as pl
from jax.experimental.pallas import tpu as pltpu
from jax.sharding import Mesh
from jax.sharding import PartitionSpec as P

D = 256
GROUPS = 32
IN_CH = 192
COLS = 512
QUERIES = 200
BAND = ("band_0", "band_1", "band_2")
CHAN = ("chan_0", "chan_1")
ALL = BAND + CHAN
EPS = 1e-05
F32 = jnp.float32
BF16 = jnp.bfloat16
FINE_ROWS = 96
COARSE_AT = 96
CONV_AT = 192
MASK_AT = 264
VEC_AT = 280
BULK_ROWS = 288


def dot(a, b):
    return lax.dot_general(a, b, (((1,), (0,)), ((), ())), preferred_element_type=F32)


def local_stats(values, lane, offset):
    blocks = values.reshape(GROUPS, D // GROUPS, COLS)
    count = D // GROUPS * COLS
    mean = jnp.sum(jnp.sum(blocks, axis=2, keepdims=True), axis=1, keepdims=True) / count
    dev = blocks - mean
    m2 = jnp.sum(jnp.sum(dev * dev, axis=2, keepdims=True), axis=1, keepdims=True)
    group = lax.broadcasted_iota(jnp.int32, (GROUPS, 1, 128), 0)
    row = jnp.where(lane == group + offset, mean, 0.0)
    row = row + jnp.where(lane == group + (offset + GROUPS), m2, 0.0)
    return jnp.sum(row, axis=0)


def combined_stats(stats, image):
    devices = stats.shape[0]
    count = D // GROUPS * COLS
    mean = jnp.sum(stats, axis=0, keepdims=True) / devices
    dev = stats - mean
    spread = jnp.sum(dev * dev, axis=0, keepdims=True) * (1.0 / devices)
    inner = mean * (1.0 / count)
    lane = lax.broadcasted_iota(jnp.int32, (D, 128), 1)
    group = lax.broadcasted_iota(jnp.int32, (D, 128), 0) // (D // GROUPS)
    at_mean = lane == group + image * 2 * GROUPS
    at_m2 = lane == group + (image * 2 + 1) * GROUPS
    mean_col = jnp.sum(jnp.where(at_mean, mean, 0.0), axis=1, keepdims=True)
    var_col = jnp.sum(
        jnp.where(at_mean, spread, 0.0) + jnp.where(at_m2, inner, 0.0), axis=1, keepdims=True
    )
    return mean_col, var_col


def vector_col(bulk_ref, index):
    lane = lax.broadcasted_iota(jnp.int32, (32, 128), 1)
    row = lax.broadcasted_iota(jnp.int32, (32, 128), 0)
    pieces = []
    for s in range(8):
        vec = bulk_ref[s, VEC_AT : VEC_AT + 8, 0:128].astype(F32)[index : index + 1, :]
        pieces.append(jnp.sum(jnp.where(lane == row, vec, 0.0), axis=1, keepdims=True))
    return jnp.concatenate(pieces, axis=0)


def fine_row(ref, at):
    return jnp.concatenate([ref[s, at : at + 24, :] for s in range(8)], axis=0)


def lateral_kernel(own_ref, weight_ref, stats_ref):
    for s in range(8):
        for half in range(2):
            weight_ref[32 * s + 16 * half : 32 * s + 16 * half + 16, :] = own_ref[
                s, 48:64, 256 * half : 256 * half + 256
            ]
    lane = lax.broadcasted_iota(jnp.int32, (GROUPS, 1, 128), 2)
    total = jnp.zeros((1, 128), F32)
    for n in range(2):
        lateral = dot(weight_ref[:, 0:IN_CH], fine_row(own_ref, 24 * n))
        total = total + local_stats(lateral, lane, 64 * n)
    stats_ref[...] = jnp.broadcast_to(total[None], stats_ref.shape)


def conv_kernel(
    own_ref, bulk_ref, other_ref, lat_weight_ref, lat_stats_ref, out_ref, stats_ref,
    weight, joined, up, taps,
):
    core = lax.axis_index("band_2")
    band = (lax.axis_index("band_0") * 2 + lax.axis_index("band_1")) * 2 + core
    parity = lax.axis_index("chan_1")
    chan = lax.axis_index("chan_0") * 2 + parity
    row_at = band * 8 + chan
    for part, ref, base in ((core, bulk_ref, CONV_AT), (1 - core, other_ref, 0)):
        for s in range(8):
            at = pl.multiple_of(32 * s + 16 * part, 16)
            for a in range(3):
                for b in range(3):
                    rows = ref[s, base + (a * 3 + b) * 8 : base + (a * 3 + b) * 8 + 8, :]
                    both = jnp.concatenate([rows[:, 0:256], rows[:, 256:512]], axis=0)
                    weight[b, pl.ds(at, 16), 256 * a : 256 * a + 256] = both
    source = lax.broadcasted_iota(jnp.int32, (256, COLS), 0)
    column = lax.broadcasted_iota(jnp.int32, (256, COLS), 1)
    near = column // 2
    far = jnp.clip(near - 1 + 2 * (column % 2), 0, 255)
    spread = (
        jnp.where(source == near, 0.75, 0.0) + jnp.where(source == far, 0.25, 0.0)
    ).astype(BF16)
    gain = vector_col(bulk_ref, 0)
    shift = vector_col(bulk_ref, 1)
    stats = lat_stats_ref[...].reshape(lat_stats_ref.shape[0], 128)
    lane = lax.broadcasted_iota(jnp.int32, (GROUPS, 1, 128), 2)
    lane_at = lax.broadcasted_iota(jnp.int32, (D, COLS), 1)
    total = jnp.zeros((1, 128), F32)
    for n in range(2):
        mean, var = combined_stats(stats, n)
        scale = lax.rsqrt(var + EPS) * gain
        for k in range(3):
            at = COARSE_AT + 32 * k
            coarse = jnp.concatenate(
                [bulk_ref[s, at : at + 32, 256 * n : 256 * n + 256] for s in range(8)], axis=0
            )
            up[k] = dot(coarse, spread)
        for h in range(3):
            if h == 1:
                fine = fine_row(own_ref, 24 * n)
            else:
                fine = fine_row(bulk_ref, 24 * h + 24 * n)
            lateral = dot(lat_weight_ref[:, 0:IN_CH], fine)
            odd = (parity + h + 1) % 2
            first = (parity + h) // 2
            low = jnp.where(odd == 1, 0.75, 0.25).astype(F32)
            upsampled = low * up[first] + (1.0 - low) * up[first + 1]
            value = ((lateral - mean) * scale + shift + upsampled).astype(BF16)
            inside = jnp.logical_and(row_at + h - 1 >= 0, row_at + h - 1 < 256)
            joined[256 * h : 256 * h + 256, :] = jnp.where(inside, value, jnp.zeros_like(value))
        for b in range(3):
            taps[b] = dot(weight[b], joined[...])
        left = jnp.where(lane_at == 0, 0.0, pltpu.roll(taps[0], 1, axis=1))
        right = jnp.where(lane_at == COLS - 1, 0.0, pltpu.roll(taps[2], COLS - 1, axis=1))
        conv_out = taps[1] + left + right
        out_ref[n] = conv_out
        total = total + local_stats(conv_out, lane, 64 * n)
    stats_ref[...] = jnp.broadcast_to(total[None], stats_ref.shape)


def query_kernel(conv_ref, out_stats_ref, bulk_ref, query_ref, out_ref, weight):
    for s in range(8):
        for half in range(2):
            weight[32 * s + 16 * half : 32 * s + 16 * half + 16, :] = bulk_ref[
                s, MASK_AT : MASK_AT + 16, 256 * half : 256 * half + 256
            ]
    gain = vector_col(bulk_ref, 2)
    shift = vector_col(bulk_ref, 3)
    bias = vector_col(bulk_ref, 4)
    stats = out_stats_ref[...].reshape(out_stats_ref.shape[0], 128)
    for n in range(2):
        mean, var = combined_stats(stats, n)
        scale = lax.rsqrt(var + EPS) * gain
        activated = jnp.maximum((conv_ref[n] - mean) * scale + shift, 0.0).astype(BF16)
        features = (dot(weight[...], activated) + bias).astype(BF16)
        logits = dot(query_ref[...], features)
        shifted = logits - jnp.max(logits, axis=0, keepdims=True)
        result = shifted - jnp.log(jnp.sum(jnp.exp(shifted), axis=0, keepdims=True))
        out_ref[n, :, 0, :] = result


def call(kernel, out_shape, scratch=(), flops=0):
    vmem = pl.BlockSpec(memory_space=pltpu.VMEM)
    single = not isinstance(out_shape, (tuple, list))
    return functools.partial(
        lambda *args: pl.pallas_call(
            kernel,
            out_shape=out_shape,
            in_specs=[vmem] * len(args),
            out_specs=vmem if single else [vmem] * len(out_shape),
            scratch_shapes=list(scratch),
            cost_estimate=pl.CostEstimate(flops=flops, bytes_accessed=1 << 20, transcendentals=0),
            compiler_params=pltpu.CompilerParams(vmem_limit_bytes=40 << 20),
        )(*args)
    )


def per_device(
    fine_features,
    coarse_level,
    lat_weight,
    lat_gain,
    lat_shift,
    out_weight,
    out_gain,
    out_shift,
    mask_weight,
    mask_bias,
    queries,
):
    bands = lax.axis_size(BAND)
    everyone = lax.axis_size(ALL)
    band = lax.axis_index(BAND)
    core = lax.axis_index("band_2")
    fine = jnp.moveaxis(fine_features, 2, 0).reshape(8, 48, COLS)
    coarse = coarse_level.transpose(2, 1, 0, 3).reshape(4, 32, COLS)
    up = [(i, i + 1) for i in range(bands - 1)]
    down = [(i + 1, i) for i in range(bands - 1)]
    above = lax.ppermute(jnp.concatenate([fine[7], coarse[3]], 0), BAND, up)
    below = lax.ppermute(jnp.concatenate([fine[0], coarse[0]], 0), BAND, down)

    weight_rows = jnp.pad(lat_weight, ((0, 0), (0, 256 - IN_CH)))
    weight_rows = weight_rows.reshape(2, 16, 256).transpose(1, 0, 2).reshape(16, 512)
    own = jnp.concatenate([fine, jnp.broadcast_to(weight_rows[None], (8, 16, 512))], 1)
    own = lax.all_to_all(own, CHAN, 0, 0, tiled=True)

    coarse_above = jnp.where(band == 0, coarse[0], above[48:])
    coarse_below = jnp.where(band == bands - 1, coarse[3], below[48:])
    fine_all = jnp.concatenate([above[None, :48], fine, below[None, :48]], 0)
    coarse_all = jnp.concatenate([coarse_above[None], coarse, coarse_below[None]], 0)
    conv = out_weight.reshape(9, 2, 2, 8, 256)
    conv = jnp.where(core == 0, conv[:, 0], conv[:, 1])
    conv = conv.transpose(0, 2, 1, 3).reshape(72, 512)
    mask = mask_weight.reshape(2, 16, 256).transpose(1, 0, 2).reshape(16, 512)
    vectors = jnp.stack([lat_gain, lat_shift, out_gain, out_shift, mask_bias])
    vectors = jnp.pad(vectors, ((0, 3), (0, 512 - 32)))
    shared = jnp.concatenate([conv, mask, vectors], 0)
    bulk = jnp.concatenate(
        [
            fine_all[0:8],
            fine_all[2:10],
            jnp.repeat(coarse_all[0:4], 2, axis=0),
            jnp.repeat(coarse_all[1:5], 2, axis=0),
            jnp.repeat(coarse_all[2:6], 2, axis=0),
            jnp.broadcast_to(shared[None], (8, 96, 512)),
        ],
        1,
    )
    bulk = lax.all_to_all(bulk, CHAN, 0, 0, tiled=True)
    other = lax.ppermute(bulk[:, CONV_AT:MASK_AT], "band_2", [(0, 1), (1, 0)])

    stats_shape = jax.ShapeDtypeStruct((everyone, 1, 128), F32)
    full_lat, stats = call(
        lateral_kernel,
        [jax.ShapeDtypeStruct((D, 256), BF16), stats_shape],
        flops=2 * 2 * 256 * 256 * 512,
    )(own)
    stats = lax.all_to_all(stats, ALL, 0, 0, tiled=True)
    conv_out, stats = call(
        conv_kernel,
        [jax.ShapeDtypeStruct((2, D, COLS), F32), stats_shape],
        (
            pltpu.VMEM((3, D, 3 * D), BF16),
            pltpu.VMEM((3 * D, COLS), BF16),
            pltpu.VMEM((3, D, COLS), F32),
            pltpu.VMEM((3, D, COLS), F32),
        ),
        flops=2 * 2 * 256 * 256 * 512 * 16,
    )(own, bulk, other, full_lat, stats)
    stats = lax.all_to_all(stats, ALL, 0, 0, tiled=True)
    return call(
        query_kernel,
        jax.ShapeDtypeStruct((2, QUERIES, 1, COLS), F32),
        (pltpu.VMEM((D, D), BF16),),
        flops=2 * 2 * 256 * 256 * 512 * 2,
    )(conv_out, stats, bulk, queries)


def solution(mesh):
    finer = Mesh(
        mesh.devices.reshape(8, 2, 2, 4, 2), ("band_0", "band_1", "band_2", "chan_0", "chan_1")
    )
    return jax.shard_map(
        per_device,
        mesh=finer,
        in_specs=(
            P(None, CHAN, BAND, None),
            P(None, CHAN, BAND, None),
            P(CHAN, None),
            P(CHAN),
            P(CHAN),
            P(None, None, CHAN, None),
            P(CHAN),
            P(CHAN),
            P(CHAN, None),
            P(CHAN),
            P(),
        ),
        out_specs=P(None, None, BAND + CHAN, None),
        check_vma=False,
    )
```

```python
import functools

import jax
import jax.numpy as jnp
from jax import lax
from jax.experimental import pallas as pl
from jax.experimental.pallas import tpu as pltpu
from jax.sharding import Mesh
from jax.sharding import PartitionSpec as P

D = 256
GROUPS = 32
IN_CH = 192
COLS = 512
QUERIES = 200
BAND = ("band_0", "band_1", "band_2")
CHAN = ("chan_0", "chan_1")
ALL = BAND + CHAN
EPS = 1e-05
F32 = jnp.float32
BF16 = jnp.bfloat16
FINE_ROWS = 96
COARSE_AT = 96
CONV_AT = 192
MASK_AT = 264
VEC_AT = 280
BULK_ROWS = 288


def dot(a, b):
    return lax.dot_general(a, b, (((1,), (0,)), ((), ())), preferred_element_type=F32)


def local_stats(values, lane, offset):
    blocks = values.reshape(GROUPS, D // GROUPS, COLS)
    count = D // GROUPS * COLS
    mean = jnp.sum(jnp.sum(blocks, axis=2, keepdims=True), axis=1, keepdims=True) / count
    dev = blocks - mean
    m2 = jnp.sum(jnp.sum(dev * dev, axis=2, keepdims=True), axis=1, keepdims=True)
    group = lax.broadcasted_iota(jnp.int32, (GROUPS, 1, 128), 0)
    row = jnp.where(lane == group + offset, mean, 0.0)
    row = row + jnp.where(lane == group + (offset + GROUPS), m2, 0.0)
    return jnp.sum(row, axis=0)


def combined_stats(stats, image):
    devices = stats.shape[0]
    count = D // GROUPS * COLS
    mean = jnp.sum(stats, axis=0, keepdims=True) / devices
    dev = stats - mean
    spread = jnp.sum(dev * dev, axis=0, keepdims=True) * (1.0 / devices)
    inner = mean * (1.0 / count)
    lane = lax.broadcasted_iota(jnp.int32, (D, 128), 1)
    group = lax.broadcasted_iota(jnp.int32, (D, 128), 0) // (D // GROUPS)
    at_mean = lane == group + image * 2 * GROUPS
    at_m2 = lane == group + (image * 2 + 1) * GROUPS
    mean_col = jnp.sum(jnp.where(at_mean, mean, 0.0), axis=1, keepdims=True)
    var_col = jnp.sum(
        jnp.where(at_mean, spread, 0.0) + jnp.where(at_m2, inner, 0.0), axis=1, keepdims=True
    )
    return mean_col, var_col


def vector_col(bulk_ref, index):
    lane = lax.broadcasted_iota(jnp.int32, (32, 128), 1)
    row = lax.broadcasted_iota(jnp.int32, (32, 128), 0)
    pieces = []
    for s in range(8):
        vec = bulk_ref[s, VEC_AT : VEC_AT + 8, 0:128].astype(F32)[index : index + 1, :]
        pieces.append(jnp.sum(jnp.where(lane == row, vec, 0.0), axis=1, keepdims=True))
    return jnp.concatenate(pieces, axis=0)


def fine_row(ref, at):
    return jnp.concatenate([ref[s, at : at + 24, :] for s in range(8)], axis=0)


def pack_own_kernel(fine_ref, weight_ref, own_ref, rows):
    for t in range(4):
        piece = fine_ref[:, :, :, 128 * t : 128 * t + 128].astype(F32)
        rows[t] = piece.reshape(48 * 8, 128)
        for d in range(8):
            row = rows[t, pl.ds(d, 48, stride=8), :]
            own_ref[d, 0:48, 128 * t : 128 * t + 128] = row.astype(BF16)
    weight = jnp.concatenate(
        [weight_ref[...].astype(F32), jnp.zeros((32, 256 - IN_CH), F32)], axis=1
    )
    packed = jnp.concatenate([weight[0:16], weight[16:32]], axis=1).astype(BF16)
    for d in range(8):
        own_ref[d, 48:64, :] = packed


def pack_bulk_kernel(
    own_ref, above_ref, below_ref, coarse_ref, conv_ref, mask_ref, vec_ref, bulk_ref
):
    core = lax.axis_index("band_2")
    band = (lax.axis_index("band_0") * 2 + lax.axis_index("band_1")) * 2 + core
    top = jnp.where(band == 0, coarse_ref[0], above_ref[48:80])
    bottom = jnp.where(band == 31, coarse_ref[3], below_ref[48:80])
    for d in range(8):
        bulk_ref[d, 0:48] = own_ref[d - 1, 0:48] if d else above_ref[0:48]
        bulk_ref[d, 48:96] = own_ref[d + 1, 0:48] if d < 7 else below_ref[0:48]
        for k in range(3):
            at = d // 2 - 1 + k
            row = top if at < 0 else bottom if at > 3 else coarse_ref[at]
            bulk_ref[d, COARSE_AT + 32 * k : COARSE_AT + 32 * k + 32] = row
        bulk_ref[d, VEC_AT : VEC_AT + 8] = vec_ref[...]
    half = pl.multiple_of(16 * core, 16)
    for a in range(3):
        for b in range(3):
            piece = conv_ref[a, b, pl.ds(half, 16), :].astype(F32)
            piece = jnp.concatenate([piece[0:8], piece[8:16]], axis=1).astype(BF16)
            at = CONV_AT + 8 * (3 * a + b)
            for d in range(8):
                bulk_ref[d, at : at + 8] = piece
    mask = jnp.concatenate([mask_ref[0:16], mask_ref[16:32]], axis=1)
    for d in range(8):
        bulk_ref[d, MASK_AT : MASK_AT + 16] = mask


def lateral_kernel(own_ref, weight_ref, stats_ref):
    for s in range(8):
        for half in range(2):
            weight_ref[32 * s + 16 * half : 32 * s + 16 * half + 16, :] = own_ref[
                s, 48:64, 256 * half : 256 * half + 256
            ]
    lane = lax.broadcasted_iota(jnp.int32, (GROUPS, 1, 128), 2)
    total = jnp.zeros((1, 128), F32)
    for n in range(2):
        lateral = dot(weight_ref[:, 0:IN_CH], fine_row(own_ref, 24 * n))
        total = total + local_stats(lateral, lane, 64 * n)
    stats_ref[...] = jnp.broadcast_to(total[None], stats_ref.shape)


def conv_kernel(
    own_ref, bulk_ref, other_ref, lat_weight_ref, lat_stats_ref, out_ref, stats_ref,
    weight, joined, up, taps,
):
    core = lax.axis_index("band_2")
    band = (lax.axis_index("band_0") * 2 + lax.axis_index("band_1")) * 2 + core
    parity = lax.axis_index("chan_1")
    chan = lax.axis_index("chan_0") * 2 + parity
    row_at = band * 8 + chan
    for part, ref, base in ((core, bulk_ref, CONV_AT), (1 - core, other_ref, 0)):
        for s in range(8):
            at = pl.multiple_of(32 * s + 16 * part, 16)
            for a in range(3):
                for b in range(3):
                    rows = ref[s, base + (a * 3 + b) * 8 : base + (a * 3 + b) * 8 + 8, :]
                    both = jnp.concatenate([rows[:, 0:256], rows[:, 256:512]], axis=0)
                    weight[b, pl.ds(at, 16), 256 * a : 256 * a + 256] = both
    source = lax.broadcasted_iota(jnp.int32, (256, COLS), 0)
    column = lax.broadcasted_iota(jnp.int32, (256, COLS), 1)
    near = column // 2
    far = jnp.clip(near - 1 + 2 * (column % 2), 0, 255)
    spread = (
        jnp.where(source == near, 0.75, 0.0) + jnp.where(source == far, 0.25, 0.0)
    ).astype(BF16)
    gain = vector_col(bulk_ref, 0)
    shift = vector_col(bulk_ref, 1)
    stats = lat_stats_ref[...].reshape(lat_stats_ref.shape[0], 128)
    lane = lax.broadcasted_iota(jnp.int32, (GROUPS, 1, 128), 2)
    lane_at = lax.broadcasted_iota(jnp.int32, (D, COLS), 1)
    total = jnp.zeros((1, 128), F32)
    for n in range(2):
        mean, var = combined_stats(stats, n)
        scale = lax.rsqrt(var + EPS) * gain
        for k in range(3):
            at = COARSE_AT + 32 * k
            coarse = jnp.concatenate(
                [bulk_ref[s, at : at + 32, 256 * n : 256 * n + 256] for s in range(8)], axis=0
            )
            up[k] = dot(coarse, spread)
        for h in range(3):
            if h == 1:
                fine = fine_row(own_ref, 24 * n)
            else:
                fine = fine_row(bulk_ref, 24 * h + 24 * n)
            lateral = dot(lat_weight_ref[:, 0:IN_CH], fine)
            odd = (parity + h + 1) % 2
            first = (parity + h) // 2
            low = jnp.where(odd == 1, 0.75, 0.25).astype(F32)
            upsampled = low * up[first] + (1.0 - low) * up[first + 1]
            value = ((lateral - mean) * scale + shift + upsampled).astype(BF16)
            inside = jnp.logical_and(row_at + h - 1 >= 0, row_at + h - 1 < 256)
            joined[256 * h : 256 * h + 256, :] = jnp.where(inside, value, jnp.zeros_like(value))
        for b in range(3):
            taps[b] = dot(weight[b], joined[...])
        left = jnp.where(lane_at == 0, 0.0, pltpu.roll(taps[0], 1, axis=1))
        right = jnp.where(lane_at == COLS - 1, 0.0, pltpu.roll(taps[2], COLS - 1, axis=1))
        conv_out = taps[1] + left + right
        out_ref[n] = conv_out
        total = total + local_stats(conv_out, lane, 64 * n)
    stats_ref[...] = jnp.broadcast_to(total[None], stats_ref.shape)


def query_kernel(conv_ref, out_stats_ref, bulk_ref, query_ref, out_ref, weight):
    for s in range(8):
        for half in range(2):
            weight[32 * s + 16 * half : 32 * s + 16 * half + 16, :] = bulk_ref[
                s, MASK_AT : MASK_AT + 16, 256 * half : 256 * half + 256
            ]
    gain = vector_col(bulk_ref, 2)
    shift = vector_col(bulk_ref, 3)
    bias = vector_col(bulk_ref, 4)
    stats = out_stats_ref[...].reshape(out_stats_ref.shape[0], 128)
    for n in range(2):
        mean, var = combined_stats(stats, n)
        scale = lax.rsqrt(var + EPS) * gain
        activated = jnp.maximum((conv_ref[n] - mean) * scale + shift, 0.0).astype(BF16)
        features = (dot(weight[...], activated) + bias).astype(BF16)
        logits = dot(query_ref[...], features)
        shifted = logits - jnp.max(logits, axis=0, keepdims=True)
        result = shifted - jnp.log(jnp.sum(jnp.exp(shifted), axis=0, keepdims=True))
        out_ref[n, :, 0, :] = result


def call(kernel, out_shape, scratch=(), flops=0):
    vmem = pl.BlockSpec(memory_space=pltpu.VMEM)
    single = not isinstance(out_shape, (tuple, list))
    return functools.partial(
        lambda *args: pl.pallas_call(
            kernel,
            out_shape=out_shape,
            in_specs=[vmem] * len(args),
            out_specs=vmem if single else [vmem] * len(out_shape),
            scratch_shapes=list(scratch),
            cost_estimate=pl.CostEstimate(flops=flops, bytes_accessed=1 << 20, transcendentals=0),
            compiler_params=pltpu.CompilerParams(vmem_limit_bytes=40 << 20),
        )(*args)
    )


def per_device(
    fine_features,
    coarse_level,
    lat_weight,
    lat_gain,
    lat_shift,
    out_weight,
    out_gain,
    out_shift,
    mask_weight,
    mask_bias,
    queries,
):
    bands = lax.axis_size(BAND)
    everyone = lax.axis_size(ALL)
    up = [(i, i + 1) for i in range(bands - 1)]
    down = [(i + 1, i) for i in range(bands - 1)]
    own_out = call(
        pack_own_kernel,
        jax.ShapeDtypeStruct((8, 64, COLS), BF16),
        (pltpu.VMEM((4, 48 * 8, 128), F32),),
    )(fine_features, lat_weight)
    own = lax.all_to_all(own_out, CHAN, 0, 0, tiled=True)

    coarse = coarse_level.transpose(2, 1, 0, 3).reshape(4, 32, COLS)
    above = lax.ppermute(jnp.concatenate([own_out[7, :48], coarse[3]], 0), BAND, up)
    below = lax.ppermute(jnp.concatenate([own_out[0, :48], coarse[0]], 0), BAND, down)
    vectors = jnp.stack([lat_gain, lat_shift, out_gain, out_shift, mask_bias])
    vectors = jnp.pad(vectors, ((0, 3), (0, 512 - 32)))
    bulk_out = call(pack_bulk_kernel, jax.ShapeDtypeStruct((8, BULK_ROWS, COLS), BF16))(
        own_out, above, below, coarse, out_weight, mask_weight, vectors
    )
    own, bulk_out = lax.optimization_barrier((own, bulk_out))
    bulk = lax.all_to_all(bulk_out, CHAN, 0, 0, tiled=True)

    stats_shape = jax.ShapeDtypeStruct((everyone, 1, 128), F32)
    full_lat, stats = call(
        lateral_kernel,
        [jax.ShapeDtypeStruct((D, 256), BF16), stats_shape],
        flops=2 * 2 * 256 * 256 * 512,
    )(own)
    stats = lax.all_to_all(stats, ALL, 0, 0, tiled=True)
    stats, bulk = lax.optimization_barrier((stats, bulk))
    other = lax.ppermute(bulk[:, CONV_AT:MASK_AT], "band_2", [(0, 1), (1, 0)])
    conv_out, stats = call(
        conv_kernel,
        [jax.ShapeDtypeStruct((2, D, COLS), F32), stats_shape],
        (
            pltpu.VMEM((3, D, 3 * D), BF16),
            pltpu.VMEM((3 * D, COLS), BF16),
            pltpu.VMEM((3, D, COLS), F32),
            pltpu.VMEM((3, D, COLS), F32),
        ),
        flops=2 * 2 * 256 * 256 * 512 * 16,
    )(own, bulk, other, full_lat, stats)
    stats = lax.all_to_all(stats, ALL, 0, 0, tiled=True)
    return call(
        query_kernel,
        jax.ShapeDtypeStruct((2, QUERIES, 1, COLS), F32),
        (pltpu.VMEM((D, D), BF16),),
        flops=2 * 2 * 256 * 256 * 512 * 2,
    )(conv_out, stats, bulk, queries)


def solution(mesh):
    finer = Mesh(
        mesh.devices.reshape(8, 2, 2, 4, 2), ("band_0", "band_1", "band_2", "chan_0", "chan_1")
    )
    return jax.shard_map(
        per_device,
        mesh=finer,
        in_specs=(
            P(None, CHAN, BAND, None),
            P(None, CHAN, BAND, None),
            P(CHAN, None),
            P(CHAN),
            P(CHAN),
            P(None, None, CHAN, None),
            P(CHAN),
            P(CHAN),
            P(CHAN, None),
            P(CHAN),
            P(),
        ),
        out_specs=P(None, None, BAND + CHAN, None),
        check_vma=False,
    )
```

```python
import functools

import jax
import jax.numpy as jnp
from jax import lax
from jax.experimental import pallas as pl
from jax.experimental.pallas import tpu as pltpu
from jax.sharding import Mesh
from jax.sharding import PartitionSpec as P

D = 256
GROUPS = 32
IN_CH = 192
COLS = 512
HALF = 256
QUERIES = 200
BAND = ("band_0", "band_1", "band_2")
CHAN = ("chan_0", "chan_1")
ALL = BAND + CHAN
EPS = 1e-05
F32 = jnp.float32
BF16 = jnp.bfloat16
OWN_ROWS = 96
SIDE_ROWS = 112
MASK_AT = 72
VEC_AT = 80
SHARD_ROWS = 88


def dot(a, b):
    return lax.dot_general(a, b, (((1,), (0,)), ((), ())), preferred_element_type=F32)


def local_stats(values, lane, offset):
    blocks = values.reshape(GROUPS, D // GROUPS, COLS)
    count = D // GROUPS * COLS
    mean = jnp.sum(jnp.sum(blocks, axis=2, keepdims=True), axis=1, keepdims=True) / count
    dev = blocks - mean
    m2 = jnp.sum(jnp.sum(dev * dev, axis=2, keepdims=True), axis=1, keepdims=True)
    group = lax.broadcasted_iota(jnp.int32, (GROUPS, 1, 128), 0)
    row = jnp.where(lane == group + offset, mean, 0.0)
    row = row + jnp.where(lane == group + (offset + GROUPS), m2, 0.0)
    return jnp.sum(row, axis=0)


def combine(stats):
    devices = stats.shape[0]
    count = D // GROUPS * COLS
    mean = jnp.sum(stats, axis=0, keepdims=True) / devices
    dev = stats - mean
    spread = jnp.sum(dev * dev, axis=0, keepdims=True) * (1.0 / devices)
    return mean, spread, mean * (1.0 / count)


def stat_cols(rows, image):
    mean, spread, inner = rows
    lane = lax.broadcasted_iota(jnp.int32, (D, 128), 1)
    group = lax.broadcasted_iota(jnp.int32, (D, 128), 0) // (D // GROUPS)
    at_mean = lane == group + image * 2 * GROUPS
    at_m2 = lane == group + (image * 2 + 1) * GROUPS
    mean_col = jnp.sum(jnp.where(at_mean, mean, 0.0), axis=1, keepdims=True)
    var_col = jnp.sum(
        jnp.where(at_mean, spread, 0.0) + jnp.where(at_m2, inner, 0.0), axis=1, keepdims=True
    )
    return mean_col, var_col


def vector_col(ref, index):
    lane = lax.broadcasted_iota(jnp.int32, (32, 128), 1)
    row = lax.broadcasted_iota(jnp.int32, (32, 128), 0)
    pieces = []
    for s in range(8):
        vec = ref[s, VEC_AT : VEC_AT + 8, 0:128].astype(F32)[index : index + 1, :]
        pieces.append(jnp.sum(jnp.where(lane == row, vec, 0.0), axis=1, keepdims=True))
    return jnp.concatenate(pieces, axis=0)


def lanes_of(shape):
    return lax.broadcasted_iota(jnp.int32, shape, len(shape) - 1)


def fine_rows(ref, image, low, high):
    return jnp.concatenate(
        [ref[s, 24 * image : 24 * image + 24, low:high] for s in range(8)], axis=0
    )


def pack_own_kernel(fine_ref, weight_ref, coarse_ref, own_ref, rows, coarse):
    for t in range(4):
        piece = fine_ref[:, :, :, 128 * t : 128 * t + 128].astype(F32)
        rows[t] = piece.reshape(48 * 8, 128)
    for n in range(2):
        for t in range(2):
            piece = coarse_ref[n, :, :, 128 * t : 128 * t + 128].astype(F32)
            coarse[n, t, :, 0:4, :] = piece
    weight = jnp.concatenate(
        [weight_ref[...].astype(F32), jnp.zeros((32, 256 - IN_CH), F32)], axis=1
    )
    packed = jnp.concatenate([weight[0:16], weight[16:32]], axis=1).astype(BF16)
    fine_lane = lanes_of((24, 128))
    coarse_lane = lanes_of((32, 128))
    for q in range(4):
        for h in range(2):
            d = 2 * q + h
            fine_extra = jnp.zeros((24, 128), F32)
            for r in range(2):
                for t in range(2):
                    row = rows[2 * h + t, pl.ds(2 * q + r, 48, stride=8), :]
                    at = 256 * r + 128 * t
                    own_ref[d, 0:48, at : at + 128] = row.astype(BF16)
                row = rows[2 - h, pl.ds(2 * q + r, 48, stride=8), :]
                edge = row[:, 0:1] if h == 0 else row[:, 127:128]
                for n in range(2):
                    at = 4 * n + 1 + r
                    fine_extra += jnp.where(fine_lane == at, edge[24 * n : 24 * n + 24], 0.0)
            own_ref[d, 48:64, :] = packed
            coarse_extra = jnp.zeros((32, 128), F32)
            for n in range(2):
                row = coarse[n, h, :, q, :].astype(BF16)
                own_ref[d, 64:80, 128 * n : 128 * n + 128] = row[0:16]
                own_ref[d, 64:80, 256 + 128 * n : 384 + 128 * n] = row[16:32]
                row = coarse[n, 1 - h, :, q, :]
                edge = row[:, 0:1] if h == 0 else row[:, 127:128]
                coarse_extra += jnp.where(coarse_lane // 4 == n, edge, 0.0)
            extra = [
                fine_extra[0:16],
                jnp.concatenate([fine_extra[16:24], jnp.zeros((8, 128), F32)], axis=0),
                coarse_extra[0:16],
                coarse_extra[16:32],
            ]
            own_ref[d, 80:96, :] = jnp.concatenate(extra, axis=1).astype(BF16)


def pack_weights_kernel(conv_ref, mask_ref, vec_ref, shard_ref):
    half = pl.multiple_of(16 * lax.axis_index("band_2"), 16)
    for k in range(10):
        if k < 9:
            piece = conv_ref[k // 3, k % 3, pl.ds(half, 16), :].astype(F32)
        else:
            piece = mask_ref[pl.ds(half, 16), :].astype(F32)
        piece = jnp.concatenate([piece[0:8], piece[8:16]], axis=1).astype(BF16)
        shard_ref[8 * k : 8 * k + 8] = piece
    shard_ref[VEC_AT : VEC_AT + 8] = vec_ref[...]


def arrange_kernel(own_ref, one_ref, two_ref, three_ref, all_ref):
    x = lax.axis_index("chan_0")
    yl = lax.axis_index("chan_1")
    for k, ref in enumerate((own_ref, one_ref, two_ref, three_ref)):
        for j in range(2):
            at = ((x - k + 4) % 4) * 2 + (yl + j) % 2
            all_ref[at] = ref[j]


def lateral_kernel(own_ref, weight_ref, stats_ref, next_ref, prev_ref):
    for s in range(8):
        for half in range(2):
            weight_ref[32 * s + 16 * half : 32 * s + 16 * half + 16, :] = own_ref[
                s, 48:64, 256 * half : 256 * half + 256
            ]
    for ref, at in ((next_ref, 256), (prev_ref, 0)):
        for s in range(8):
            ref[s, 0:48, :] = own_ref[s, 0:48, at : at + 256]
            ref[s, 48:64, :] = own_ref[s, 64:80, 0:256]
            ref[s, 64:80, :] = own_ref[s, 64:80, 256:512]
            ref[s, 80:96, :] = own_ref[s, 80:96, 0:256]
            ref[s, 96:112, :] = own_ref[s, 80:96, 256:512]
    lane = lax.broadcasted_iota(jnp.int32, (GROUPS, 1, 128), 2)
    total = jnp.zeros((1, 128), F32)
    for n in range(2):
        lateral = dot(weight_ref[:, 0:IN_CH], fine_rows(own_ref, n, 0, COLS))
        total = total + local_stats(lateral, lane, 64 * n)
    stats_ref[...] = jnp.broadcast_to(total[None], stats_ref.shape)


def conv_kernel(
    own_ref, above_ref, below_ref, lat_weight_ref, lat_stats_ref, mine_ref, other_ref,
    keep_ref, send_ref, stats_ref,
    weight, joined, taps,
):
    core = lax.axis_index("band_2")
    band = (lax.axis_index("band_0") * 2 + lax.axis_index("band_1")) * 2 + core
    side = lax.axis_index("chan_1")
    pair = band * 4 + lax.axis_index("chan_0")
    at_top = pair == 0
    at_bottom = pair == 127
    for part, ref in ((core, mine_ref), (1 - core, other_ref)):
        for s in range(8):
            at = pl.multiple_of(32 * s + 16 * part, 16)
            for a in range(3):
                for b in range(3):
                    piece = ref[s, (a * 3 + b) * 8 : (a * 3 + b) * 8 + 8, :]
                    both = jnp.concatenate([piece[:, 0:256], piece[:, 256:512]], axis=0)
                    weight[b, pl.ds(at, 16), 256 * a : 256 * a + 256] = both
    source = lax.broadcasted_iota(jnp.int32, (128, HALF), 0)
    column = lanes_of((128, HALF))
    inner_edge = jnp.where(side == 0, HALF - 1, 0)
    near = column // 2
    far = jnp.clip(near - 1 + 2 * (column % 2), 0, 127)
    spread = (
        jnp.where(source == near, 0.75, 0.0)
        + jnp.where(jnp.logical_and(source == far, column != inner_edge), 0.25, 0.0)
    ).astype(BF16)
    gain = vector_col(mine_ref, 0)
    shift = vector_col(mine_ref, 1)
    stats = combine(lat_stats_ref[...].reshape(lat_stats_ref.shape[0], 128))
    lane = lax.broadcasted_iota(jnp.int32, (GROUPS, 1, 128), 2)
    lane_at = lanes_of((D, HALF))
    small = lanes_of((D, 128))
    first_image = small < 4
    time = small % 4
    norm = [stat_cols(stats, n) for n in range(2)]
    norm = [(mean, lax.rsqrt(var + EPS) * gain) for mean, var in norm]
    lat_weight = lat_weight_ref[:, 0:IN_CH]

    def coarse_main(ref, low, high, n):
        at = 128 * n
        if high is None:
            pieces = [ref[s, low : low + 32, at : at + 128] for s in range(8)]
        else:
            pieces = []
            for s in range(8):
                pieces.append(ref[s, low : low + 16, at : at + 128])
                pieces.append(ref[s, low : low + 16, high + at : high + at + 128])
        return jnp.concatenate(pieces, axis=0)

    def extras(ref, low, at):
        fine, coarse = [], []
        for s in range(8):
            fine.append(ref[s, low : low + 16, 0:128])
            fine.append(ref[s, low : low + 8, 128:256])
            if at:
                coarse.append(ref[s, low : low + 16, at : at + 128])
                coarse.append(ref[s, low : low + 16, at + 128 : at + 256])
            else:
                coarse.append(ref[s, low + 16 : low + 32, 0:128])
                coarse.append(ref[s, low + 16 : low + 32, 128:256])
        fine = dot(lat_weight, jnp.concatenate(fine, axis=0))
        return fine, jnp.concatenate(coarse, axis=0).astype(F32)

    fine_above, extra_above = extras(above_ref, 80, 0)
    fine_own, extra_own = extras(own_ref, 80, 256)
    fine_below, extra_below = extras(below_ref, 80, 0)
    extra_above = jnp.where(at_top, extra_own, extra_above)
    extra_below = jnp.where(at_bottom, extra_own, extra_below)
    mains = []
    for n in range(2):
        middle = coarse_main(own_ref, 64, 256, n)
        upper = coarse_main(above_ref, 48, None, n)
        lower = coarse_main(below_ref, 48, None, n)
        upper = jnp.where(at_top, middle, upper)
        lower = jnp.where(at_bottom, middle, lower)
        mains.append((upper, middle, lower))
    edge_at = jnp.where(side == 0, 127, 0)
    ups, columns = [], []
    for k, extra in enumerate((extra_above, extra_own, extra_below)):
        edges = []
        for n in range(2):
            main = mains[n][k]
            edges.append(
                jnp.sum(jnp.where(small == edge_at, main.astype(F32), 0.0), axis=1, keepdims=True)
            )
        columns.append(0.75 * extra + 0.25 * jnp.where(first_image, edges[0], edges[1]))
        ups.append(
            [
                dot(mains[n][k], spread)
                + jnp.where(lane_at == inner_edge, 0.25 * extra[:, 4 * n : 4 * n + 1], 0.0)
                for n in range(2)
            ]
        )

    lateral = jnp.where(
        time == 0,
        pltpu.roll(fine_above, 126, axis=1),
        jnp.where(time == 3, pltpu.roll(fine_below, 2, axis=1), fine_own),
    )
    upsampled = jnp.where(
        time == 0,
        0.75 * columns[0] + 0.25 * columns[1],
        jnp.where(
            time == 1,
            0.25 * columns[0] + 0.75 * columns[1],
            jnp.where(
                time == 2,
                0.75 * columns[1] + 0.25 * columns[2],
                0.25 * columns[1] + 0.75 * columns[2],
            ),
        ),
    )
    mean = jnp.where(first_image, norm[0][0], norm[1][0])
    scale = jnp.where(first_image, norm[0][1], norm[1][1])
    value = (lateral - mean) * scale + shift + upsampled
    outside = jnp.logical_or(
        jnp.logical_and(time == 0, at_top), jnp.logical_and(time == 3, at_bottom)
    )
    value = jnp.where(outside, 0.0, value)
    beside = jnp.concatenate(
        [value, pltpu.roll(value, 127, axis=1), pltpu.roll(value, 126, axis=1)], axis=0
    ).astype(BF16)
    beside = dot(weight[jnp.where(side == 0, 2, 0)], beside)

    total = jnp.zeros((1, 128), F32)
    for n in range(2):
        mean, scale = norm[n]
        up = [ups[k][n] for k in range(3)]
        rows = (
            (fine_rows(above_ref, n, 0, HALF), 0.75 * up[0] + 0.25 * up[1]),
            (fine_rows(own_ref, n, 0, HALF), 0.25 * up[0] + 0.75 * up[1]),
            (fine_rows(own_ref, n, HALF, COLS), 0.75 * up[1] + 0.25 * up[2]),
            (fine_rows(below_ref, n, 0, HALF), 0.25 * up[1] + 0.75 * up[2]),
        )
        for t, (fine, upsampled) in enumerate(rows):
            value = ((dot(lat_weight, fine) - mean) * scale + shift + upsampled).astype(BF16)
            if t == 0:
                value = jnp.where(at_top, jnp.zeros_like(value), value)
            if t == 3:
                value = jnp.where(at_bottom, jnp.zeros_like(value), value)
            for r in range(2):
                if 0 <= t - r <= 2:
                    joined[
                        256 * (t - r) : 256 * (t - r) + 256, HALF * r : HALF * r + HALF
                    ] = value
        for b in range(3):
            taps[b] = dot(weight[b], joined[...])
        out = []
        for r in range(2):
            at = HALF * r
            left = pltpu.roll(taps[0, :, at : at + HALF], 1, axis=1)
            right = pltpu.roll(taps[2, :, at : at + HALF], HALF - 1, axis=1)
            value = taps[1, :, at : at + HALF] + jnp.where(lane_at == 0, 0.0, left)
            value = value + jnp.where(lane_at == HALF - 1, 0.0, right)
            column = beside[:, 4 * n + r : 4 * n + r + 1]
            out.append(value + jnp.where(lane_at == inner_edge, column, 0.0))
        keep_ref[n] = jnp.where(side == 0, out[0], out[1])
        send_ref[n] = jnp.where(side == 0, out[1], out[0])
        total = total + local_stats(jnp.concatenate(out, axis=1), lane, 64 * n)
    stats_ref[...] = jnp.broadcast_to(total[None], stats_ref.shape)


def query_kernel(
    keep_ref, taken_ref, out_stats_ref, mine_ref, other_ref, query_ref, out_ref, weight
):
    core = lax.axis_index("band_2")
    side = lax.axis_index("chan_1")
    for part, ref in ((core, mine_ref), (1 - core, other_ref)):
        for s in range(8):
            at = pl.multiple_of(32 * s + 16 * part, 16)
            piece = ref[s, MASK_AT : MASK_AT + 8, :]
            both = jnp.concatenate([piece[:, 0:256], piece[:, 256:512]], axis=0)
            weight[pl.ds(at, 16), :] = both
    gain = vector_col(mine_ref, 2)
    shift = vector_col(mine_ref, 3)
    bias = vector_col(mine_ref, 4)
    rows = combine(out_stats_ref[...].reshape(out_stats_ref.shape[0], 128))
    for n in range(2):
        mean, var = stat_cols(rows, n)
        scale = lax.rsqrt(var + EPS) * gain
        for ref, half in ((keep_ref, side), (taken_ref, 1 - side)):
            activated = jnp.maximum((ref[n] - mean) * scale + shift, 0.0).astype(BF16)
            features = (dot(weight[...], activated) + bias).astype(BF16)
            logits = dot(query_ref[...], features)
            shifted = logits - jnp.max(logits, axis=0, keepdims=True)
            result = shifted - jnp.log(jnp.sum(jnp.exp(shifted), axis=0, keepdims=True))
            at = pl.multiple_of(half * HALF, HALF)
            out_ref[n, :, 0, pl.ds(at, HALF)] = result


def call(kernel, out_shape, scratch=(), flops=0):
    vmem = pl.BlockSpec(memory_space=pltpu.VMEM)
    single = not isinstance(out_shape, (tuple, list))
    return functools.partial(
        lambda *args: pl.pallas_call(
            kernel,
            out_shape=out_shape,
            in_specs=[vmem] * len(args),
            out_specs=vmem if single else [vmem] * len(out_shape),
            scratch_shapes=list(scratch),
            cost_estimate=pl.CostEstimate(flops=flops, bytes_accessed=1 << 20, transcendentals=0),
            compiler_params=pltpu.CompilerParams(vmem_limit_bytes=40 << 20),
        )(*args)
    )


def per_device(
    fine_features,
    coarse_level,
    lat_weight,
    lat_gain,
    lat_shift,
    out_weight,
    out_gain,
    out_shift,
    mask_weight,
    mask_bias,
    queries,
):
    everyone = lax.axis_size(ALL)
    stats_shape = jax.ShapeDtypeStruct((everyone, 1, 128), F32)
    shard_shape = jax.ShapeDtypeStruct((SHARD_ROWS, COLS), BF16)
    all_shape = jax.ShapeDtypeStruct((8, SHARD_ROWS, COLS), BF16)
    side_shape = jax.ShapeDtypeStruct((8, SIDE_ROWS, HALF), BF16)
    half_shape = jax.ShapeDtypeStruct((2, D, HALF), F32)
    swap = [(0, 1), (1, 0)]

    own_out = call(
        pack_own_kernel,
        jax.ShapeDtypeStruct((8, OWN_ROWS, COLS), BF16),
        (pltpu.VMEM((4, 48 * 8, 128), F32), pltpu.VMEM((2, 2, 32, 8, 128), F32)),
    )(fine_features, lat_weight, coarse_level)
    own = lax.all_to_all(own_out, CHAN, 0, 0, tiled=True)

    vectors = jnp.stack([lat_gain, lat_shift, out_gain, out_shift, mask_bias])
    vectors = jnp.pad(vectors, ((0, 3), (0, 512 - 32)))
    shard = call(pack_weights_kernel, shard_shape)(out_weight, mask_weight, vectors)
    partner = lax.ppermute(shard, "chan_1", swap)
    both = jnp.stack([shard, partner])
    moved = [
        lax.ppermute(both, "chan_0", [(i, (i + k) % 4) for i in range(4)]) for k in (1, 2, 3)
    ]
    mine = call(arrange_kernel, all_shape)(both, *moved)
    other = lax.ppermute(mine, "band_2", swap)

    full_lat, stats, to_next, to_prev = call(
        lateral_kernel,
        [jax.ShapeDtypeStruct((D, 256), BF16), stats_shape, side_shape, side_shape],
        flops=2 * 2 * 256 * 256 * 512,
    )(own)
    above = lax.ppermute(to_next, ALL, [(i, i + 2) for i in range(everyone - 2)])
    below = lax.ppermute(to_prev, ALL, [(i + 2, i) for i in range(everyone - 2)])
    stats = lax.all_to_all(stats, ALL, 0, 0, tiled=True)
    keep, send, stats = call(
        conv_kernel,
        [half_shape, half_shape, stats_shape],
        (
            pltpu.VMEM((3, D, 3 * D), BF16),
            pltpu.VMEM((3 * D, COLS), BF16),
            pltpu.VMEM((3, D, COLS), F32),
        ),
        flops=2 * 2 * 256 * 256 * 512 * 16,
    )(own, above, below, full_lat, stats, mine, other)
    taken = lax.ppermute(send, "chan_1", swap)
    stats = lax.all_to_all(stats, ALL, 0, 0, tiled=True)
    return call(
        query_kernel,
        jax.ShapeDtypeStruct((2, QUERIES, 1, COLS), F32),
        (pltpu.VMEM((D, D), BF16),),
        flops=2 * 2 * 256 * 256 * 512 * 2,
    )(keep, taken, stats, mine, other, queries)


def solution(mesh):
    finer = Mesh(
        mesh.devices.reshape(8, 2, 2, 4, 2), ("band_0", "band_1", "band_2", "chan_0", "chan_1")
    )
    return jax.shard_map(
        per_device,
        mesh=finer,
        in_specs=(
            P(None, CHAN, BAND, None),
            P(None, CHAN, BAND, None),
            P(CHAN, None),
            P(CHAN),
            P(CHAN),
            P(None, None, CHAN, None),
            P(CHAN),
            P(CHAN),
            P(CHAN, None),
            P(CHAN),
            P(),
        ),
        out_specs=P(None, None, BAND + CHAN, None),
        check_vma=False,
    )
```

```python
import jax
import jax.numpy as jnp
from jax import lax
from jax.experimental import pallas as pl
from jax.experimental.pallas import tpu as pltpu
from jax.sharding import Mesh
from jax.sharding import PartitionSpec as P


D = 256
GROUPS = 32
IN_CH = 192
COLS = 512
HALF = 256
QUERIES = 200
BAND = ("band_0", "band_1", "band_2")
CHAN = ("chan_0", "chan_1")
ALL = BAND + CHAN
EPS = 1e-05
F32 = jnp.float32
BF16 = jnp.bfloat16
OWN_ROWS = 96
SIDE_ROWS = 112
MASK_AT = 72
SHARD_ROWS = 80
XORS = (4, 1, 2, 5, 6, 3, 7)


def dot(a, b):
    return lax.dot_general(a, b, (((1,), (0,)), ((), ())), preferred_element_type=F32)


def local_stats(values, lane, offset):
    blocks = values.reshape(GROUPS, D // GROUPS, COLS)
    count = D // GROUPS * COLS
    mean = jnp.sum(jnp.sum(blocks, axis=2, keepdims=True), axis=1, keepdims=True) / count
    dev = blocks - mean
    m2 = jnp.sum(jnp.sum(dev * dev, axis=2, keepdims=True), axis=1, keepdims=True)
    group = lax.broadcasted_iota(jnp.int32, (GROUPS, 1, 128), 0)
    row = jnp.where(lane == group + offset, mean, 0.0)
    row = row + jnp.where(lane == group + (offset + GROUPS), m2, 0.0)
    return jnp.sum(row, axis=0)


def combine(stats):
    devices = stats.shape[0]
    count = D // GROUPS * COLS
    mean = jnp.sum(stats, axis=0, keepdims=True) / devices
    dev = stats - mean
    spread = jnp.sum(dev * dev, axis=0, keepdims=True) * (1.0 / devices)
    return mean, spread, mean * (1.0 / count)


def stat_cols(rows, image):
    mean, spread, inner = rows
    lane = lax.broadcasted_iota(jnp.int32, (D, 128), 1)
    group = lax.broadcasted_iota(jnp.int32, (D, 128), 0) // (D // GROUPS)
    at_mean = lane == group + image * 2 * GROUPS
    at_m2 = lane == group + (image * 2 + 1) * GROUPS
    mean_col = jnp.sum(jnp.where(at_mean, mean, 0.0), axis=1, keepdims=True)
    var_col = jnp.sum(
        jnp.where(at_mean, spread, 0.0) + jnp.where(at_m2, inner, 0.0), axis=1, keepdims=True
    )
    return mean_col, var_col


def combine_kernel(stats_ref, rows_ref):
    mean, spread, inner = combine(stats_ref[...].reshape(stats_ref.shape[0], 128))
    rows_ref[0:1] = mean
    rows_ref[1:2] = spread
    rows_ref[2:3] = inner
    rows_ref[3:8] = jnp.zeros((5, 128), F32)


def vector_col(lat_weight_ref, index):
    return lat_weight_ref[:, 128:256].astype(F32)[:, 64 + index : 65 + index]


def lanes_of(shape):
    return lax.broadcasted_iota(jnp.int32, shape, len(shape) - 1)


def fine_rows(ref, image, low, high):
    return jnp.concatenate(
        [ref[s, 24 * image : 24 * image + 24, low:high] for s in range(8)], axis=0
    )


def pack_own_kernel(
    fine_hbm, coarse_hbm, weight_hbm, *refs
):
    vec_hbm, own_ref, (fine_ref, coarse_ref, weight_ref, vec_ref, rows, coarse, sems) = (
        refs[:5], refs[5], refs[6:]
    )
    pairs = [(fine_hbm, fine_ref), (coarse_hbm, coarse_ref), (weight_hbm, weight_ref)]
    pairs += [(vec, vec_ref.at[i]) for i, vec in enumerate(vec_hbm)]
    copies = [
        pltpu.make_async_copy(source, target, sems.at[i])
        for i, (source, target) in enumerate(pairs)
    ]
    for copy in copies:
        copy.start()
    for copy in copies:
        copy.wait()
    for t in range(4):
        piece = fine_ref[:, :, :, 128 * t : 128 * t + 128].astype(F32)
        rows[t] = piece.reshape(48 * 8, 128)
    for n in range(2):
        for t in range(2):
            piece = coarse_ref[n, :, :, 128 * t : 128 * t + 128].astype(F32)
            coarse[n, t, :, 0:4, :] = piece
    vec_lane = lanes_of((32, 32))
    vec_row = lax.broadcasted_iota(jnp.int32, (32, 32), 0)
    columns = jnp.zeros((32, 256 - IN_CH), F32)
    for i in range(5):
        vec = jnp.where(vec_lane == vec_row, vec_ref[i].astype(F32), 0.0)
        column = jnp.sum(vec, axis=1, keepdims=True)
        columns += jnp.where(lanes_of((32, 256 - IN_CH)) == i, column, 0.0)
    weight = jnp.concatenate([weight_ref[...].astype(F32), columns], axis=1)
    packed = jnp.concatenate([weight[0:16], weight[16:32]], axis=1).astype(BF16)
    fine_lane = lanes_of((24, 128))
    coarse_lane = lanes_of((32, 128))
    for q in range(4):
        for h in range(2):
            d = 2 * q + h
            fine_extra = jnp.zeros((24, 128), F32)
            for r in range(2):
                for t in range(2):
                    row = rows[2 * h + t, pl.ds(2 * q + r, 48, stride=8), :]
                    at = 256 * r + 128 * t
                    own_ref[d, 0:48, at : at + 128] = row.astype(BF16)
                row = rows[2 - h, pl.ds(2 * q + r, 48, stride=8), :]
                edge = row[:, 0:1] if h == 0 else row[:, 127:128]
                for n in range(2):
                    at = 4 * n + 1 + r
                    fine_extra += jnp.where(fine_lane == at, edge[24 * n : 24 * n + 24], 0.0)
            own_ref[d, 48:64, :] = packed
            coarse_extra = jnp.zeros((32, 128), F32)
            for n in range(2):
                row = coarse[n, h, :, q, :].astype(BF16)
                own_ref[d, 64:80, 128 * n : 128 * n + 128] = row[0:16]
                own_ref[d, 64:80, 256 + 128 * n : 384 + 128 * n] = row[16:32]
                row = coarse[n, 1 - h, :, q, :]
                edge = row[:, 0:1] if h == 0 else row[:, 127:128]
                coarse_extra += jnp.where(coarse_lane // 4 == n, edge, 0.0)
            extra = [
                fine_extra[0:16],
                jnp.concatenate([fine_extra[16:24], jnp.zeros((8, 128), F32)], axis=0),
                coarse_extra[0:16],
                coarse_extra[16:32],
            ]
            own_ref[d, 80:96, :] = jnp.concatenate(extra, axis=1).astype(BF16)


def pack_weights_kernel(conv_ref, mask_ref, shard_ref):
    half = pl.multiple_of(16 * lax.axis_index("band_2"), 16)
    for k in range(10):
        if k < 9:
            piece = conv_ref[k // 3, k % 3, pl.ds(half, 16), :].astype(F32)
        else:
            piece = mask_ref[pl.ds(half, 16), :].astype(F32)
        piece = jnp.concatenate([piece[0:8], piece[8:16]], axis=1).astype(BF16)
        shard_ref[8 * k : 8 * k + 8] = piece


def arrange_kernel(*refs):
    chan = lax.axis_index("chan_0") * 2 + lax.axis_index("chan_1")
    all_ref = refs[-1]
    for k, ref in enumerate(refs[:-1]):
        all_ref[chan ^ k] = ref[...]


def lateral_kernel(own_ref, weight_ref, stats_ref, next_ref, prev_ref):
    for s in range(8):
        for half in range(2):
            weight_ref[32 * s + 16 * half : 32 * s + 16 * half + 16, :] = own_ref[
                s, 48:64, 256 * half : 256 * half + 256
            ]
    for ref, at in ((next_ref, 256), (prev_ref, 0)):
        for s in range(8):
            ref[s, 0:48, :] = own_ref[s, 0:48, at : at + 256]
            ref[s, 48:64, :] = own_ref[s, 64:80, 0:256]
            ref[s, 64:80, :] = own_ref[s, 64:80, 256:512]
            ref[s, 80:96, :] = own_ref[s, 80:96, 0:256]
            ref[s, 96:112, :] = own_ref[s, 80:96, 256:512]
    lane = lax.broadcasted_iota(jnp.int32, (GROUPS, 1, 128), 2)
    total = jnp.zeros((1, 128), F32)
    for n in range(2):
        lateral = dot(weight_ref[:, 0:IN_CH], fine_rows(own_ref, n, 0, COLS))
        total = total + local_stats(lateral, lane, 64 * n)
    stats_ref[...] = jnp.broadcast_to(total[None], stats_ref.shape)


def join_kernel(
    own_ref, above_ref, below_ref, lat_weight_ref, lat_stats_ref, joined_ref, beside_ref
):
    core = lax.axis_index("band_2")
    band = (lax.axis_index("band_0") * 2 + lax.axis_index("band_1")) * 2 + core
    side = lax.axis_index("chan_1")
    pair = band * 4 + lax.axis_index("chan_0")
    at_top = pair == 0
    at_bottom = pair == 127
    source = lax.broadcasted_iota(jnp.int32, (128, HALF), 0)
    column = lanes_of((128, HALF))
    inner_edge = jnp.where(side == 0, HALF - 1, 0)
    near = column // 2
    far = jnp.clip(near - 1 + 2 * (column % 2), 0, 127)
    spread = (
        jnp.where(source == near, 0.75, 0.0)
        + jnp.where(jnp.logical_and(source == far, column != inner_edge), 0.25, 0.0)
    ).astype(BF16)
    gain = vector_col(lat_weight_ref, 0)
    shift = vector_col(lat_weight_ref, 1)
    stats = (lat_stats_ref[0:1], lat_stats_ref[1:2], lat_stats_ref[2:3])
    lane_at = lanes_of((D, HALF))
    small = lanes_of((D, 128))
    first_image = small < 4
    time = small % 4
    norm = [stat_cols(stats, n) for n in range(2)]
    norm = [(mean, lax.rsqrt(var + EPS) * gain) for mean, var in norm]
    lat_weight = lat_weight_ref[:, 0:IN_CH]

    def coarse_main(ref, low, high, n):
        at = 128 * n
        if high is None:
            pieces = [ref[s, low : low + 32, at : at + 128] for s in range(8)]
        else:
            pieces = []
            for s in range(8):
                pieces.append(ref[s, low : low + 16, at : at + 128])
                pieces.append(ref[s, low : low + 16, high + at : high + at + 128])
        return jnp.concatenate(pieces, axis=0)

    def extras(ref, low, at):
        fine, coarse = [], []
        for s in range(8):
            fine.append(ref[s, low : low + 16, 0:128])
            fine.append(ref[s, low : low + 8, 128:256])
            if at:
                coarse.append(ref[s, low : low + 16, at : at + 128])
                coarse.append(ref[s, low : low + 16, at + 128 : at + 256])
            else:
                coarse.append(ref[s, low + 16 : low + 32, 0:128])
                coarse.append(ref[s, low + 16 : low + 32, 128:256])
        fine = dot(lat_weight, jnp.concatenate(fine, axis=0))
        return fine, jnp.concatenate(coarse, axis=0).astype(F32)

    fine_above, extra_above = extras(above_ref, 80, 0)
    fine_own, extra_own = extras(own_ref, 80, 256)
    fine_below, extra_below = extras(below_ref, 80, 0)
    extra_above = jnp.where(at_top, extra_own, extra_above)
    extra_below = jnp.where(at_bottom, extra_own, extra_below)
    mains = []
    for n in range(2):
        middle = coarse_main(own_ref, 64, 256, n)
        upper = coarse_main(above_ref, 48, None, n)
        lower = coarse_main(below_ref, 48, None, n)
        upper = jnp.where(at_top, middle, upper)
        lower = jnp.where(at_bottom, middle, lower)
        mains.append((upper, middle, lower))
    edge_at = jnp.where(side == 0, 127, 0)
    ups, columns = [], []
    for k, extra in enumerate((extra_above, extra_own, extra_below)):
        edges = []
        for n in range(2):
            main = mains[n][k]
            edges.append(
                jnp.sum(jnp.where(small == edge_at, main.astype(F32), 0.0), axis=1, keepdims=True)
            )
        columns.append(0.75 * extra + 0.25 * jnp.where(first_image, edges[0], edges[1]))
        ups.append(
            [
                dot(mains[n][k], spread)
                + jnp.where(lane_at == inner_edge, 0.25 * extra[:, 4 * n : 4 * n + 1], 0.0)
                for n in range(2)
            ]
        )

    lateral = jnp.where(
        time == 0,
        pltpu.roll(fine_above, 126, axis=1),
        jnp.where(time == 3, pltpu.roll(fine_below, 2, axis=1), fine_own),
    )
    upsampled = jnp.where(
        time == 0,
        0.75 * columns[0] + 0.25 * columns[1],
        jnp.where(
            time == 1,
            0.25 * columns[0] + 0.75 * columns[1],
            jnp.where(
                time == 2,
                0.75 * columns[1] + 0.25 * columns[2],
                0.25 * columns[1] + 0.75 * columns[2],
            ),
        ),
    )
    mean = jnp.where(first_image, norm[0][0], norm[1][0])
    scale = jnp.where(first_image, norm[0][1], norm[1][1])
    value = (lateral - mean) * scale + shift + upsampled
    outside = jnp.logical_or(
        jnp.logical_and(time == 0, at_top), jnp.logical_and(time == 3, at_bottom)
    )
    value = jnp.where(outside, 0.0, value)
    beside_ref[...] = jnp.concatenate(
        [value, pltpu.roll(value, 127, axis=1), pltpu.roll(value, 126, axis=1)], axis=0
    ).astype(BF16)

    for n in range(2):
        mean, scale = norm[n]
        up = [ups[k][n] for k in range(3)]
        rows = (
            (fine_rows(above_ref, n, 0, HALF), 0.75 * up[0] + 0.25 * up[1]),
            (fine_rows(own_ref, n, 0, HALF), 0.25 * up[0] + 0.75 * up[1]),
            (fine_rows(own_ref, n, HALF, COLS), 0.75 * up[1] + 0.25 * up[2]),
            (fine_rows(below_ref, n, 0, HALF), 0.25 * up[1] + 0.75 * up[2]),
        )
        for t, (fine, upsampled) in enumerate(rows):
            value = ((dot(lat_weight, fine) - mean) * scale + shift + upsampled).astype(BF16)
            if t == 0:
                value = jnp.where(at_top, jnp.zeros_like(value), value)
            if t == 3:
                value = jnp.where(at_bottom, jnp.zeros_like(value), value)
            for r in range(2):
                if 0 <= t - r <= 2:
                    joined_ref[
                        n, 256 * (t - r) : 256 * (t - r) + 256, HALF * r : HALF * r + HALF
                    ] = value


def conv_kernel(
    joined_ref, beside_ref, mine_ref, other_ref, keep_ref, send_ref, stats_ref, weight, taps
):
    core = lax.axis_index("band_2")
    side = lax.axis_index("chan_1")
    for part, ref in ((core, mine_ref), (1 - core, other_ref)):
        for s in range(8):
            at = pl.multiple_of(32 * s + 16 * part, 16)
            for a in range(3):
                for b in range(3):
                    piece = ref[s, (a * 3 + b) * 8 : (a * 3 + b) * 8 + 8, :]
                    both = jnp.concatenate([piece[:, 0:256], piece[:, 256:512]], axis=0)
                    weight[b, pl.ds(at, 16), 256 * a : 256 * a + 256] = both
    inner_edge = jnp.where(side == 0, HALF - 1, 0)
    lane = lax.broadcasted_iota(jnp.int32, (GROUPS, 1, 128), 2)
    lane_at = lanes_of((D, HALF))
    beside = dot(weight[jnp.where(side == 0, 2, 0)], beside_ref[...])
    total = jnp.zeros((1, 128), F32)
    for n in range(2):
        for b in range(3):
            taps[b] = dot(weight[b], joined_ref[n])
        out = []
        for r in range(2):
            at = HALF * r
            left = pltpu.roll(taps[0, :, at : at + HALF], 1, axis=1)
            right = pltpu.roll(taps[2, :, at : at + HALF], HALF - 1, axis=1)
            value = taps[1, :, at : at + HALF] + jnp.where(lane_at == 0, 0.0, left)
            value = value + jnp.where(lane_at == HALF - 1, 0.0, right)
            column = beside[:, 4 * n + r : 4 * n + r + 1]
            out.append(value + jnp.where(lane_at == inner_edge, column, 0.0))
        keep_ref[n] = jnp.where(side == 0, out[0], out[1])
        send_ref[n] = jnp.where(side == 0, out[1], out[0])
        total = total + local_stats(jnp.concatenate(out, axis=1), lane, 64 * n)
    stats_ref[...] = jnp.broadcast_to(total[None], stats_ref.shape)


def query_kernel(
    keep_ref, taken_ref, out_stats_ref, lat_weight_ref, mine_ref, other_ref,
    query_ref, out_ref, weight,
):
    core = lax.axis_index("band_2")
    side = lax.axis_index("chan_1")
    for part, ref in ((core, mine_ref), (1 - core, other_ref)):
        for s in range(8):
            at = pl.multiple_of(32 * s + 16 * part, 16)
            piece = ref[s, MASK_AT : MASK_AT + 8, :]
            both = jnp.concatenate([piece[:, 0:256], piece[:, 256:512]], axis=0)
            weight[pl.ds(at, 16), :] = both
    gain = vector_col(lat_weight_ref, 2)
    shift = vector_col(lat_weight_ref, 3)
    bias = vector_col(lat_weight_ref, 4)
    rows = combine(out_stats_ref[...].reshape(out_stats_ref.shape[0], 128))
    for n in range(2):
        mean, var = stat_cols(rows, n)
        scale = lax.rsqrt(var + EPS) * gain
        for ref, half in ((keep_ref, side), (taken_ref, 1 - side)):
            activated = jnp.maximum((ref[n] - mean) * scale + shift, 0.0).astype(BF16)
            features = (dot(weight[...], activated) + bias).astype(BF16)
            logits = dot(query_ref[...], features)
            shifted = logits - jnp.max(logits, axis=0, keepdims=True)
            result = shifted - jnp.log(jnp.sum(jnp.exp(shifted), axis=0, keepdims=True))
            at = pl.multiple_of(half * HALF, HALF)
            out_ref[n, :, 0, pl.ds(at, HALF)] = result


def call(kernel, out_shape, scratch=(), flops=0, space=pltpu.VMEM, limit=40 << 20):
    vmem = pl.BlockSpec(memory_space=pltpu.VMEM)
    single = not isinstance(out_shape, (tuple, list))
    return lambda *args: pl.pallas_call(
        kernel,
        out_shape=out_shape,
        in_specs=[pl.BlockSpec(memory_space=space)] * len(args),
        out_specs=vmem if single else [vmem] * len(out_shape),
        scratch_shapes=list(scratch),
        cost_estimate=pl.CostEstimate(flops=flops, bytes_accessed=1 << 20, transcendentals=0),
        compiler_params=pltpu.CompilerParams(vmem_limit_bytes=limit),
    )(*args)


def per_device(
    fine_features,
    coarse_level,
    lat_weight,
    lat_gain,
    lat_shift,
    out_weight,
    out_gain,
    out_shift,
    mask_weight,
    mask_bias,
    queries,
):
    everyone = lax.axis_size(ALL)
    stats_shape = jax.ShapeDtypeStruct((everyone, 1, 128), F32)
    shard_shape = jax.ShapeDtypeStruct((SHARD_ROWS, COLS), BF16)
    all_shape = jax.ShapeDtypeStruct((8, SHARD_ROWS, COLS), BF16)
    side_shape = jax.ShapeDtypeStruct((8, SIDE_ROWS, HALF), BF16)
    half_shape = jax.ShapeDtypeStruct((2, D, HALF), F32)
    swap = [(0, 1), (1, 0)]

    vectors = [v.reshape(1, 32) for v in (lat_gain, lat_shift, out_gain, out_shift, mask_bias)]
    own_out = call(
        pack_own_kernel,
        jax.ShapeDtypeStruct((8, OWN_ROWS, COLS), BF16),
        (
            pltpu.VMEM((2, 24, 8, COLS), BF16),
            pltpu.VMEM((2, 32, 4, 256), BF16),
            pltpu.VMEM((32, IN_CH), BF16),
            pltpu.VMEM((5, 1, 32), BF16),
            pltpu.VMEM((4, 48 * 8, 128), F32),
            pltpu.VMEM((2, 2, 32, 8, 128), F32),
            pltpu.SemaphoreType.DMA((8,)),
        ),
        space=pltpu.HBM,
        limit=60 << 20,
    )(fine_features, coarse_level, lat_weight, *vectors)
    own = lax.all_to_all(own_out, CHAN, 0, 0, tiled=True)
    shard = call(pack_weights_kernel, shard_shape)(out_weight, mask_weight)
    moved = [lax.ppermute(shard, CHAN, [(i, i ^ k) for i in range(8)]) for k in XORS]

    full_lat, stats, to_next, to_prev = call(
        lateral_kernel,
        [jax.ShapeDtypeStruct((D, 256), BF16), stats_shape, side_shape, side_shape],
        flops=2 * 2 * 256 * 256 * 512,
    )(own)
    above = lax.ppermute(to_next, ALL, [(i, i + 2) for i in range(everyone - 2)])
    below = lax.ppermute(to_prev, ALL, [(i + 2, i) for i in range(everyone - 2)])
    stats = lax.all_to_all(stats, ALL, 0, 0, tiled=True)
    stats = call(combine_kernel, jax.ShapeDtypeStruct((8, 128), F32), flops=1 << 20)(stats)

    by_xor = dict(zip(XORS, moved))
    mine = call(arrange_kernel, all_shape)(shard, *[by_xor[k] for k in range(1, 8)])
    other = lax.ppermute(mine, "band_2", swap)
    joined, beside = call(
        join_kernel,
        [jax.ShapeDtypeStruct((2, 3 * D, COLS), BF16), jax.ShapeDtypeStruct((3 * D, 128), BF16)],
        flops=2 * 2 * 256 * 256 * 512 * 7,
    )(own, above, below, full_lat, stats)
    keep, send, stats = call(
        conv_kernel,
        [half_shape, half_shape, stats_shape],
        (pltpu.VMEM((3, D, 3 * D), BF16), pltpu.VMEM((3, D, COLS), F32)),
        flops=2 * 2 * 256 * 256 * 512 * 9,
    )(joined, beside, mine, other)
    taken = lax.ppermute(send, "chan_1", swap)
    stats = lax.all_to_all(stats, ALL, 0, 0, tiled=True)
    return call(
        query_kernel,
        jax.ShapeDtypeStruct((2, QUERIES, 1, COLS), F32),
        (pltpu.VMEM((D, D), BF16),),
        flops=2 * 2 * 256 * 256 * 512 * 2,
    )(keep, taken, stats, full_lat, mine, other, queries)


def solution(mesh):
    finer = Mesh(
        mesh.devices.reshape(8, 2, 2, 4, 2), ("band_0", "band_1", "band_2", "chan_0", "chan_1")
    )

    return jax.shard_map(
        per_device,
        mesh=finer,
        in_specs=(
            P(None, CHAN, BAND, None),
            P(None, CHAN, BAND, None),
            P(CHAN, None),
            P(CHAN),
            P(CHAN),
            P(None, None, CHAN, None),
            P(CHAN),
            P(CHAN),
            P(CHAN, None),
            P(CHAN),
            P(),
        ),
        out_specs=P(None, None, BAND + CHAN, None),
        check_vma=False,
    )
```

```python
import jax
import jax.numpy as jnp
from jax import lax
from jax.experimental import pallas as pl
from jax.experimental.pallas import tpu as pltpu
from jax.sharding import Mesh
from jax.sharding import PartitionSpec as P


D = 256
GROUPS = 32
IN_CH = 192
COLS = 512
HALF = 256
QUERIES = 200
BAND = ("band_0", "band_1", "band_2")
CHAN = ("chan_0", "chan_1")
ALL = BAND + CHAN
EPS = 1e-05
F32 = jnp.float32
BF16 = jnp.bfloat16
OWN_ROWS = 96
SIDE_ROWS = 112
MASK_AT = 72
SHARD_ROWS = 80


def dot(a, b):
    return lax.dot_general(a, b, (((1,), (0,)), ((), ())), preferred_element_type=F32)


def local_stats(values, lane, offset):
    blocks = values.reshape(GROUPS, D // GROUPS, COLS)
    count = D // GROUPS * COLS
    mean = jnp.sum(jnp.sum(blocks, axis=2, keepdims=True), axis=1, keepdims=True) / count
    dev = blocks - mean
    m2 = jnp.sum(jnp.sum(dev * dev, axis=2, keepdims=True), axis=1, keepdims=True)
    group = lax.broadcasted_iota(jnp.int32, (GROUPS, 1, 128), 0)
    row = jnp.where(lane == group + offset, mean, 0.0)
    row = row + jnp.where(lane == group + (offset + GROUPS), m2, 0.0)
    return jnp.sum(row, axis=0)


def combine(stats):
    devices = stats.shape[0]
    count = D // GROUPS * COLS
    mean = jnp.sum(stats, axis=0, keepdims=True) / devices
    dev = stats - mean
    spread = jnp.sum(dev * dev, axis=0, keepdims=True) * (1.0 / devices)
    return mean, spread, mean * (1.0 / count)


def stat_cols(rows, image):
    mean, spread, inner = rows
    lane = lax.broadcasted_iota(jnp.int32, (D, 128), 1)
    group = lax.broadcasted_iota(jnp.int32, (D, 128), 0) // (D // GROUPS)
    at_mean = lane == group + image * 2 * GROUPS
    at_m2 = lane == group + (image * 2 + 1) * GROUPS
    mean_col = jnp.sum(jnp.where(at_mean, mean, 0.0), axis=1, keepdims=True)
    var_col = jnp.sum(
        jnp.where(at_mean, spread, 0.0) + jnp.where(at_m2, inner, 0.0), axis=1, keepdims=True
    )
    return mean_col, var_col


def combine_kernel(stats_ref, rows_ref):
    mean, spread, inner = combine(stats_ref[...])
    rows_ref[0:1] = mean
    rows_ref[1:2] = spread
    rows_ref[2:3] = inner
    rows_ref[3:8] = jnp.zeros((5, 128), F32)


def vector_col(lat_weight_ref, index):
    return lat_weight_ref[:, 128:256].astype(F32)[:, 64 + index : 65 + index]


def lanes_of(shape):
    return lax.broadcasted_iota(jnp.int32, shape, len(shape) - 1)


def fine_rows(ref, image, low, high):
    return jnp.concatenate(
        [ref[s, 24 * image : 24 * image + 24, low:high] for s in range(8)], axis=0
    )


def pack_own_kernel(
    fine_hbm, coarse_hbm, weight_hbm, *refs
):
    vec_hbm, own_ref, (fine_ref, coarse_ref, weight_ref, vec_ref, rows, coarse, sems) = (
        refs[:5], refs[5], refs[6:]
    )
    pairs = [(fine_hbm, fine_ref), (coarse_hbm, coarse_ref), (weight_hbm, weight_ref)]
    pairs += [(vec, vec_ref.at[i]) for i, vec in enumerate(vec_hbm)]
    copies = [
        pltpu.make_async_copy(source, target, sems.at[i])
        for i, (source, target) in enumerate(pairs)
    ]
    for copy in copies[1:] + copies[:1]:
        copy.start()
    for copy in copies[1:]:
        copy.wait()
    for n in range(2):
        for t in range(2):
            piece = coarse_ref[n, :, :, 128 * t : 128 * t + 128].astype(F32)
            coarse[n, t, :, 0:4, :] = piece
    vec_lane = lanes_of((32, 32))
    vec_row = lax.broadcasted_iota(jnp.int32, (32, 32), 0)
    columns = jnp.zeros((32, 256 - IN_CH), F32)
    for i in range(5):
        vec = jnp.where(vec_lane == vec_row, vec_ref[i].astype(F32), 0.0)
        column = jnp.sum(vec, axis=1, keepdims=True)
        columns += jnp.where(lanes_of((32, 256 - IN_CH)) == i, column, 0.0)
    weight = jnp.concatenate([weight_ref[...].astype(F32), columns], axis=1)
    packed = jnp.concatenate([weight[0:16], weight[16:32]], axis=1).astype(BF16)
    fine_lane = lanes_of((24, 128))
    coarse_lane = lanes_of((32, 128))
    for q in range(4):
        for h in range(2):
            d = 2 * q + h
            own_ref[d, 48:64, :] = packed
            coarse_extra = jnp.zeros((32, 128), F32)
            for n in range(2):
                row = coarse[n, h, :, q, :].astype(BF16)
                own_ref[d, 64:80, 128 * n : 128 * n + 128] = row[0:16]
                own_ref[d, 64:80, 256 + 128 * n : 384 + 128 * n] = row[16:32]
                row = coarse[n, 1 - h, :, q, :]
                edge = row[:, 0:1] if h == 0 else row[:, 127:128]
                coarse_extra += jnp.where(coarse_lane // 4 == n, edge, 0.0)
            own_ref[d, 80:96, 256:384] = coarse_extra[0:16].astype(BF16)
            own_ref[d, 80:96, 384:512] = coarse_extra[16:32].astype(BF16)
    copies[0].wait()
    for t in range(4):
        piece = fine_ref[:, :, :, 128 * t : 128 * t + 128].astype(F32)
        rows[t] = piece.reshape(48 * 8, 128)
    for q in range(4):
        for h in range(2):
            d = 2 * q + h
            fine_extra = jnp.zeros((24, 128), F32)
            for r in range(2):
                for t in range(2):
                    row = rows[2 * h + t, pl.ds(2 * q + r, 48, stride=8), :]
                    at = 256 * r + 128 * t
                    own_ref[d, 0:48, at : at + 128] = row.astype(BF16)
                row = rows[2 - h, pl.ds(2 * q + r, 48, stride=8), :]
                edge = row[:, 0:1] if h == 0 else row[:, 127:128]
                for n in range(2):
                    at = 4 * n + 1 + r
                    fine_extra += jnp.where(fine_lane == at, edge[24 * n : 24 * n + 24], 0.0)
            tail = jnp.concatenate([fine_extra[16:24], jnp.zeros((8, 128), F32)], axis=0)
            own_ref[d, 80:96, 0:128] = fine_extra[0:16].astype(BF16)
            own_ref[d, 80:96, 128:256] = tail.astype(BF16)


def pack_weights_kernel(conv_ref, mask_ref, shard_ref):
    half = pl.multiple_of(16 * lax.axis_index("band_2"), 16)
    for k in range(10):
        if k < 9:
            piece = conv_ref[k // 3, k % 3, pl.ds(half, 16), :].astype(F32)
        else:
            piece = mask_ref[pl.ds(half, 16), :].astype(F32)
        piece = jnp.concatenate([piece[0:8], piece[8:16]], axis=1).astype(BF16)
        shard_ref[8 * k : 8 * k + 8] = piece


def line_kernel(shard_ref, one_ref, two_ref, three_ref, line_ref):
    x = lax.axis_index("chan_0")
    for k, ref in enumerate((shard_ref, one_ref, two_ref, three_ref)):
        line_ref[(x - k + 4) % 4] = ref[...]


def arrange_kernel(line_ref, partner_ref, all_ref):
    side = lax.axis_index("chan_1")
    for x in range(4):
        all_ref[2 * x + side] = line_ref[x]
        all_ref[2 * x + 1 - side] = partner_ref[x]


def lateral_kernel(own_ref, weight_ref, stats_ref, next_ref, prev_ref):
    for s in range(8):
        for half in range(2):
            weight_ref[32 * s + 16 * half : 32 * s + 16 * half + 16, :] = own_ref[
                s, 48:64, 256 * half : 256 * half + 256
            ]
    for ref, at in ((next_ref, 256), (prev_ref, 0)):
        for s in range(8):
            ref[s, 0:48, :] = own_ref[s, 0:48, at : at + 256]
            ref[s, 48:64, :] = own_ref[s, 64:80, 0:256]
            ref[s, 64:80, :] = own_ref[s, 64:80, 256:512]
            ref[s, 80:96, :] = own_ref[s, 80:96, 0:256]
            ref[s, 96:112, :] = own_ref[s, 80:96, 256:512]
    lane = lax.broadcasted_iota(jnp.int32, (GROUPS, 1, 128), 2)
    total = jnp.zeros((1, 128), F32)
    for n in range(2):
        lateral = dot(weight_ref[:, 0:IN_CH], fine_rows(own_ref, n, 0, COLS))
        total = total + local_stats(lateral, lane, 64 * n)
    stats_ref[...] = jnp.broadcast_to(total, stats_ref.shape)


def join_kernel(
    own_ref, above_ref, below_ref, lat_weight_ref, lat_stats_ref, joined_ref, beside_ref
):
    core = lax.axis_index("band_2")
    band = (lax.axis_index("band_0") * 2 + lax.axis_index("band_1")) * 2 + core
    side = lax.axis_index("chan_1")
    pair = band * 4 + lax.axis_index("chan_0")
    at_top = pair == 0
    at_bottom = pair == 127
    source = lax.broadcasted_iota(jnp.int32, (128, HALF), 0)
    column = lanes_of((128, HALF))
    inner_edge = jnp.where(side == 0, HALF - 1, 0)
    near = column // 2
    far = jnp.clip(near - 1 + 2 * (column % 2), 0, 127)
    spread = (
        jnp.where(source == near, 0.75, 0.0)
        + jnp.where(jnp.logical_and(source == far, column != inner_edge), 0.25, 0.0)
    ).astype(BF16)
    gain = vector_col(lat_weight_ref, 0)
    shift = vector_col(lat_weight_ref, 1)
    stats = (lat_stats_ref[0:1], lat_stats_ref[1:2], lat_stats_ref[2:3])
    lane_at = lanes_of((D, HALF))
    small = lanes_of((D, 128))
    first_image = small < 4
    time = small % 4
    norm = [stat_cols(stats, n) for n in range(2)]
    norm = [(mean, lax.rsqrt(var + EPS) * gain) for mean, var in norm]
    lat_weight = lat_weight_ref[:, 0:IN_CH]

    def coarse_main(ref, low, high, n):
        at = 128 * n
        if high is None:
            pieces = [ref[s, low : low + 32, at : at + 128] for s in range(8)]
        else:
            pieces = []
            for s in range(8):
                pieces.append(ref[s, low : low + 16, at : at + 128])
                pieces.append(ref[s, low : low + 16, high + at : high + at + 128])
        return jnp.concatenate(pieces, axis=0)

    def extras(ref, low, at):
        fine, coarse = [], []
        for s in range(8):
            fine.append(ref[s, low : low + 16, 0:128])
            fine.append(ref[s, low : low + 8, 128:256])
            if at:
                coarse.append(ref[s, low : low + 16, at : at + 128])
                coarse.append(ref[s, low : low + 16, at + 128 : at + 256])
            else:
                coarse.append(ref[s, low + 16 : low + 32, 0:128])
                coarse.append(ref[s, low + 16 : low + 32, 128:256])
        fine = dot(lat_weight, jnp.concatenate(fine, axis=0))
        return fine, jnp.concatenate(coarse, axis=0).astype(F32)

    fine_above, extra_above = extras(above_ref, 80, 0)
    fine_own, extra_own = extras(own_ref, 80, 256)
    fine_below, extra_below = extras(below_ref, 80, 0)
    extra_above = jnp.where(at_top, extra_own, extra_above)
    extra_below = jnp.where(at_bottom, extra_own, extra_below)
    mains = []
    for n in range(2):
        middle = coarse_main(own_ref, 64, 256, n)
        upper = coarse_main(above_ref, 48, None, n)
        lower = coarse_main(below_ref, 48, None, n)
        upper = jnp.where(at_top, middle, upper)
        lower = jnp.where(at_bottom, middle, lower)
        mains.append((upper, middle, lower))
    edge_at = jnp.where(side == 0, 127, 0)
    ups, columns = [], []
    for k, extra in enumerate((extra_above, extra_own, extra_below)):
        edges = []
        for n in range(2):
            main = mains[n][k]
            edges.append(
                jnp.sum(jnp.where(small == edge_at, main.astype(F32), 0.0), axis=1, keepdims=True)
            )
        columns.append(0.75 * extra + 0.25 * jnp.where(first_image, edges[0], edges[1]))
        ups.append(
            [
                dot(mains[n][k], spread)
                + jnp.where(lane_at == inner_edge, 0.25 * extra[:, 4 * n : 4 * n + 1], 0.0)
                for n in range(2)
            ]
        )

    lateral = jnp.where(
        time == 0,
        pltpu.roll(fine_above, 126, axis=1),
        jnp.where(time == 3, pltpu.roll(fine_below, 2, axis=1), fine_own),
    )
    upsampled = jnp.where(
        time == 0,
        0.75 * columns[0] + 0.25 * columns[1],
        jnp.where(
            time == 1,
            0.25 * columns[0] + 0.75 * columns[1],
            jnp.where(
                time == 2,
                0.75 * columns[1] + 0.25 * columns[2],
                0.25 * columns[1] + 0.75 * columns[2],
            ),
        ),
    )
    mean = jnp.where(first_image, norm[0][0], norm[1][0])
    scale = jnp.where(first_image, norm[0][1], norm[1][1])
    value = (lateral - mean) * scale + shift + upsampled
    outside = jnp.logical_or(
        jnp.logical_and(time == 0, at_top), jnp.logical_and(time == 3, at_bottom)
    )
    value = jnp.where(outside, 0.0, value)
    beside_ref[...] = jnp.concatenate(
        [value, pltpu.roll(value, 127, axis=1), pltpu.roll(value, 126, axis=1)], axis=0
    ).astype(BF16)

    for n in range(2):
        mean, scale = norm[n]
        up = [ups[k][n] for k in range(3)]
        rows = (
            (fine_rows(above_ref, n, 0, HALF), 0.75 * up[0] + 0.25 * up[1]),
            (fine_rows(own_ref, n, 0, HALF), 0.25 * up[0] + 0.75 * up[1]),
            (fine_rows(own_ref, n, HALF, COLS), 0.75 * up[1] + 0.25 * up[2]),
            (fine_rows(below_ref, n, 0, HALF), 0.25 * up[1] + 0.75 * up[2]),
        )
        for t, (fine, upsampled) in enumerate(rows):
            value = ((dot(lat_weight, fine) - mean) * scale + shift + upsampled).astype(BF16)
            if t == 0:
                value = jnp.where(at_top, jnp.zeros_like(value), value)
            if t == 3:
                value = jnp.where(at_bottom, jnp.zeros_like(value), value)
            for r in range(2):
                if 0 <= t - r <= 2:
                    joined_ref[
                        n, 256 * (t - r) : 256 * (t - r) + 256, HALF * r : HALF * r + HALF
                    ] = value


def conv_kernel(
    joined_ref, beside_ref, mine_ref, other_ref, keep_ref, send_ref, stats_ref, weight, taps
):
    core = lax.axis_index("band_2")
    side = lax.axis_index("chan_1")
    for part, ref in ((core, mine_ref), (1 - core, other_ref)):
        for s in range(8):
            at = pl.multiple_of(32 * s + 16 * part, 16)
            for a in range(3):
                for b in range(3):
                    piece = ref[s, (a * 3 + b) * 8 : (a * 3 + b) * 8 + 8, :]
                    both = jnp.concatenate([piece[:, 0:256], piece[:, 256:512]], axis=0)
                    weight[b, pl.ds(at, 16), 256 * a : 256 * a + 256] = both
    inner_edge = jnp.where(side == 0, HALF - 1, 0)
    lane = lax.broadcasted_iota(jnp.int32, (GROUPS, 1, 128), 2)
    lane_at = lanes_of((D, HALF))
    beside = dot(weight[jnp.where(side == 0, 2, 0)], beside_ref[...])
    total = jnp.zeros((1, 128), F32)
    for n in range(2):
        for b in range(3):
            taps[b] = dot(weight[b], joined_ref[n])
        out = []
        for r in range(2):
            at = HALF * r
            left = pltpu.roll(taps[0, :, at : at + HALF], 1, axis=1)
            right = pltpu.roll(taps[2, :, at : at + HALF], HALF - 1, axis=1)
            value = taps[1, :, at : at + HALF] + jnp.where(lane_at == 0, 0.0, left)
            value = value + jnp.where(lane_at == HALF - 1, 0.0, right)
            column = beside[:, 4 * n + r : 4 * n + r + 1]
            out.append(value + jnp.where(lane_at == inner_edge, column, 0.0))
        keep_ref[n] = jnp.where(side == 0, out[0], out[1])
        send_ref[n] = jnp.where(side == 0, out[1], out[0])
        total = total + local_stats(jnp.concatenate(out, axis=1), lane, 64 * n)
    stats_ref[...] = jnp.broadcast_to(total, stats_ref.shape)


def query_kernel(
    keep_ref, taken_ref, out_stats_ref, lat_weight_ref, mine_ref, other_ref,
    query_ref, out_ref, weight,
):
    core = lax.axis_index("band_2")
    side = lax.axis_index("chan_1")
    for part, ref in ((core, mine_ref), (1 - core, other_ref)):
        for s in range(8):
            at = pl.multiple_of(32 * s + 16 * part, 16)
            piece = ref[s, MASK_AT : MASK_AT + 8, :]
            both = jnp.concatenate([piece[:, 0:256], piece[:, 256:512]], axis=0)
            weight[pl.ds(at, 16), :] = both
    gain = vector_col(lat_weight_ref, 2)
    shift = vector_col(lat_weight_ref, 3)
    bias = vector_col(lat_weight_ref, 4)
    rows = combine(out_stats_ref[...])
    for n in range(2):
        mean, var = stat_cols(rows, n)
        scale = lax.rsqrt(var + EPS) * gain
        for ref, half in ((keep_ref, side), (taken_ref, 1 - side)):
            activated = jnp.maximum((ref[n] - mean) * scale + shift, 0.0).astype(BF16)
            features = (dot(weight[...], activated) + bias).astype(BF16)
            logits = dot(query_ref[...], features)
            shifted = logits - jnp.max(logits, axis=0, keepdims=True)
            result = shifted - jnp.log(jnp.sum(jnp.exp(shifted), axis=0, keepdims=True))
            for t in range(2):
                at = 4 * QUERIES * n + 2 * half + t
                out_ref[pl.ds(at, QUERIES, stride=4), :] = result[:, 128 * t : 128 * t + 128]


def call(kernel, out_shape, scratch=(), flops=0, space=pltpu.VMEM, limit=40 << 20):
    vmem = pl.BlockSpec(memory_space=pltpu.VMEM)
    single = not isinstance(out_shape, (tuple, list))
    return lambda *args: pl.pallas_call(
        kernel,
        out_shape=out_shape,
        in_specs=[pl.BlockSpec(memory_space=space)] * len(args),
        out_specs=vmem if single else [vmem] * len(out_shape),
        scratch_shapes=list(scratch),
        cost_estimate=pl.CostEstimate(flops=flops, bytes_accessed=1 << 20, transcendentals=0),
        compiler_params=pltpu.CompilerParams(vmem_limit_bytes=limit),
    )(*args)


def per_device(
    fine_features,
    coarse_level,
    lat_weight,
    lat_gain,
    lat_shift,
    out_weight,
    out_gain,
    out_shift,
    mask_weight,
    mask_bias,
    queries,
):
    everyone = lax.axis_size(ALL)
    stats_shape = jax.ShapeDtypeStruct((everyone, 128), F32)
    shard_shape = jax.ShapeDtypeStruct((SHARD_ROWS, COLS), BF16)
    all_shape = jax.ShapeDtypeStruct((8, SHARD_ROWS, COLS), BF16)
    side_shape = jax.ShapeDtypeStruct((8, SIDE_ROWS, HALF), BF16)
    half_shape = jax.ShapeDtypeStruct((2, D, HALF), F32)
    swap = [(0, 1), (1, 0)]

    vectors = [v.reshape(1, 32) for v in (lat_gain, lat_shift, out_gain, out_shift, mask_bias)]
    own_out = call(
        pack_own_kernel,
        jax.ShapeDtypeStruct((8, OWN_ROWS, COLS), BF16),
        (
            pltpu.VMEM((2, 24, 8, COLS), BF16),
            pltpu.VMEM((2, 32, 4, 256), BF16),
            pltpu.VMEM((32, IN_CH), BF16),
            pltpu.VMEM((5, 1, 32), BF16),
            pltpu.VMEM((4, 48 * 8, 128), F32),
            pltpu.VMEM((2, 2, 32, 8, 128), F32),
            pltpu.SemaphoreType.DMA((8,)),
        ),
        space=pltpu.HBM,
        limit=60 << 20,
    )(fine_features, coarse_level, lat_weight, *vectors)
    own = lax.all_to_all(own_out, CHAN, 0, 0, tiled=True)
    shard = call(pack_weights_kernel, shard_shape)(out_weight, mask_weight)
    moved = [lax.ppermute(shard, "chan_0", [(i, (i + k) % 4) for i in range(4)]) for k in (1, 2, 3)]

    full_lat, stats, to_next, to_prev = call(
        lateral_kernel,
        [jax.ShapeDtypeStruct((D, 256), BF16), stats_shape, side_shape, side_shape],
        flops=2 * 2 * 256 * 256 * 512,
    )(own)
    above = lax.ppermute(to_next, ALL, [(i, (i + 2) % everyone) for i in range(everyone)])
    below = lax.ppermute(to_prev, ALL, [((i + 2) % everyone, i) for i in range(everyone)])
    line = call(line_kernel, jax.ShapeDtypeStruct((4, SHARD_ROWS, COLS), BF16))(shard, *moved)
    partner = lax.ppermute(line, "chan_1", swap)
    stats = lax.all_to_all(stats, ALL, 0, 0, tiled=True)
    stats = call(combine_kernel, jax.ShapeDtypeStruct((8, 128), F32), flops=1 << 20)(stats)

    mine = call(arrange_kernel, all_shape)(line, partner)
    other = lax.ppermute(mine, "band_2", swap)
    joined, beside = call(
        join_kernel,
        [jax.ShapeDtypeStruct((2, 3 * D, COLS), BF16), jax.ShapeDtypeStruct((3 * D, 128), BF16)],
        flops=2 * 2 * 256 * 256 * 512 * 7,
    )(own, above, below, full_lat, stats)
    keep, send, stats = call(
        conv_kernel,
        [half_shape, half_shape, stats_shape],
        (pltpu.VMEM((3, D, 3 * D), BF16), pltpu.VMEM((3, D, COLS), F32)),
        flops=2 * 2 * 256 * 256 * 512 * 9,
    )(joined, beside, mine, other)
    taken = lax.ppermute(send, "chan_1", swap)
    stats = lax.all_to_all(stats, ALL, 0, 0, tiled=True)
    log_probs = call(
        query_kernel,
        jax.ShapeDtypeStruct((2 * QUERIES * 4, 128), F32),
        (pltpu.VMEM((D, D), BF16),),
        flops=2 * 2 * 256 * 256 * 512 * 2,
    )(keep, taken, stats, full_lat, mine, other, queries)
    return log_probs.reshape(2, QUERIES, 1, COLS)


def solution(mesh):
    finer = Mesh(
        mesh.devices.reshape(8, 2, 2, 4, 2), ("band_0", "band_1", "band_2", "chan_0", "chan_1")
    )

    return jax.shard_map(
        per_device,
        mesh=finer,
        in_specs=(
            P(None, CHAN, BAND, None),
            P(None, CHAN, BAND, None),
            P(CHAN, None),
            P(CHAN),
            P(CHAN),
            P(None, None, CHAN, None),
            P(CHAN),
            P(CHAN),
            P(CHAN, None),
            P(CHAN),
            P(),
        ),
        out_specs=P(None, None, BAND + CHAN, None),
        check_vma=False,
    )
```

```python
import jax
import jax.numpy as jnp
from jax import lax
from jax.experimental import pallas as pl
from jax.experimental.pallas import tpu as pltpu
from jax.sharding import Mesh
from jax.sharding import PartitionSpec as P


D = 256
GROUPS = 32
IN_CH = 192
COLS = 512
HALF = 256
QUERIES = 200
BAND = ("band_0", "band_1", "band_2")
CHAN = ("chan_0", "chan_1")
ALL = BAND + CHAN
EPS = 1e-05
F32 = jnp.float32
BF16 = jnp.bfloat16
OWN_ROWS = 80
VECTORS = 64
FINE_EDGE = 72
COARSE_EDGE = 80
SIDE_ROWS = 96
MASK_AT = 72
XORS = (4, 1, 2, 5, 6, 3, 7)
SHARD_ROWS = 80


def dot(a, b):
    return lax.dot_general(a, b, (((1,), (0,)), ((), ())), preferred_element_type=F32)


def local_stats(values, lane, offset):
    blocks = values.reshape(GROUPS, D // GROUPS, COLS)
    count = D // GROUPS * COLS
    mean = jnp.sum(jnp.sum(blocks, axis=2, keepdims=True), axis=1, keepdims=True) / count
    dev = blocks - mean
    m2 = jnp.sum(jnp.sum(dev * dev, axis=2, keepdims=True), axis=1, keepdims=True)
    group = lax.broadcasted_iota(jnp.int32, (GROUPS, 1, 128), 0)
    row = jnp.where(lane == group + offset, mean, 0.0)
    row = row + jnp.where(lane == group + (offset + GROUPS), m2, 0.0)
    return jnp.sum(row, axis=0)


def combine(stats):
    devices = stats.shape[0]
    count = D // GROUPS * COLS
    mean = jnp.sum(stats, axis=0, keepdims=True) / devices
    dev = stats - mean
    spread = jnp.sum(dev * dev, axis=0, keepdims=True) * (1.0 / devices)
    return mean, spread, mean * (1.0 / count)


def stat_cols(rows, image):
    mean, spread, inner = rows
    lane = lax.broadcasted_iota(jnp.int32, (D, 128), 1)
    group = lax.broadcasted_iota(jnp.int32, (D, 128), 0) // (D // GROUPS)
    at_mean = lane == group + image * 2 * GROUPS
    at_m2 = lane == group + (image * 2 + 1) * GROUPS
    mean_col = jnp.sum(jnp.where(at_mean, mean, 0.0), axis=1, keepdims=True)
    var_col = jnp.sum(
        jnp.where(at_mean, spread, 0.0) + jnp.where(at_m2, inner, 0.0), axis=1, keepdims=True
    )
    return mean_col, var_col


def combine_kernel(stats_ref, rows_ref):
    mean, spread, inner = combine(stats_ref[...])
    rows_ref[0:1] = mean
    rows_ref[1:2] = spread
    rows_ref[2:3] = inner
    rows_ref[3:8] = jnp.zeros((5, 128), F32)


def vector_col(lat_weight_ref, index):
    return lat_weight_ref[:, 128:256].astype(F32)[:, VECTORS + index : VECTORS + index + 1]


def lanes_of(shape):
    return lax.broadcasted_iota(jnp.int32, shape, len(shape) - 1)


def fine_rows(ref, image, low, high):
    return jnp.concatenate(
        [ref[s, 24 * image : 24 * image + 24, low:high] for s in range(8)], axis=0
    )


def pack_own_kernel(fine_hbm, coarse_hbm, weight_hbm, *refs):
    vec_hbm, own_hbm = refs[:5], refs[5]
    fine_ref, coarse_ref, weight_ref, vec_ref, own_ref, rows, coarse, sems, out_sems = refs[6:]
    pairs = [(coarse_hbm, coarse_ref), (weight_hbm, weight_ref)]
    pairs += [(vec, vec_ref.at[i]) for i, vec in enumerate(vec_hbm)] + [(fine_hbm, fine_ref)]
    copies = [
        pltpu.make_async_copy(source, target, sems.at[i])
        for i, (source, target) in enumerate(pairs)
    ]
    for copy in copies:
        copy.start()
    for copy in copies[:-1]:
        copy.wait()
    for n in range(2):
        for t in range(2):
            piece = coarse_ref[n, :, :, 128 * t : 128 * t + 128].astype(F32)
            piece = jnp.concatenate([piece, jnp.zeros_like(piece)], axis=1)
            coarse[n, t] = piece.reshape(256, 128)
    lane = lanes_of((32, 128))
    vec_lane = lanes_of((32, 32))
    vec_row = lax.broadcasted_iota(jnp.int32, (32, 32), 0)
    weight = weight_ref[...].astype(F32)
    second = jnp.concatenate([weight[:, 128:IN_CH], jnp.zeros((32, 256 - IN_CH), F32)], axis=1)
    for i in range(5):
        vec = jnp.where(vec_lane == vec_row, vec_ref[i].astype(F32), 0.0)
        second += jnp.where(lane == VECTORS + i, jnp.sum(vec, axis=1, keepdims=True), 0.0)
    first = weight[:, 0:128].astype(BF16)
    tails = []
    for h in range(2):
        for q in range(4):
            d = 2 * q + h
            tail = second
            own_ref[d, 48:64, 0:128] = first[0:16]
            own_ref[d, 48:64, 256:384] = first[16:32]
            for n in range(2):
                row = coarse[n, h, pl.ds(q, 32, stride=8), :].astype(BF16)
                own_ref[d, 64:80, 128 * n : 128 * n + 128] = row[0:16]
                own_ref[d, 64:80, 256 + 128 * n : 384 + 128 * n] = row[16:32]
                row = coarse[n, 1 - h, pl.ds(q, 32, stride=8), :]
                edge = row[:, 0:1] if h == 0 else row[:, 127:128]
                tail = jnp.where(lane // 4 == COARSE_EDGE // 4 + n, edge, tail)
            tails.append(tail)
    copies[-1].wait()
    for t in range(4):
        piece = fine_ref[:, :, :, 128 * t : 128 * t + 128].astype(F32)
        rows[t] = piece.reshape(48 * 8, 128)
    out = []
    for h in range(2):
        for q in range(4):
            d = 2 * q + h
            tail = tails[4 * h + q]
            for r in range(2):
                for t in range(2):
                    row = rows[2 * h + t, pl.ds(2 * q + r, 48, stride=8), :]
                    at = 256 * r + 128 * t
                    own_ref[d, 0:48, at : at + 128] = row.astype(BF16)
                row = rows[2 - h, pl.ds(2 * q + r, 48, stride=8), :]
                edge = row[:, 0:1] if h == 0 else row[:, 127:128]
                for n in range(2):
                    column = jnp.concatenate(
                        [edge[24 * n : 24 * n + 24], jnp.zeros((8, 1), F32)], axis=0
                    )
                    tail = jnp.where(lane == FINE_EDGE + 4 * n + 1 + r, column, tail)
            tail = tail.astype(BF16)
            own_ref[d, 48:64, 128:256] = tail[0:16]
            own_ref[d, 48:64, 384:512] = tail[16:32]
            out.append(pltpu.make_async_copy(own_ref.at[d], own_hbm.at[d], out_sems.at[d]))
            out[-1].start()
    for copy in out:
        copy.wait()


def pack_weights_kernel(conv_ref, mask_ref, shard_ref):
    half = pl.multiple_of(16 * lax.axis_index("band_2"), 16)
    for k in range(10):
        if k < 9:
            piece = conv_ref[k // 3, k % 3, pl.ds(half, 16), :].astype(F32)
        else:
            piece = mask_ref[pl.ds(half, 16), :].astype(F32)
        piece = jnp.concatenate([piece[0:8], piece[8:16]], axis=1).astype(BF16)
        shard_ref[8 * k : 8 * k + 8] = piece


def arrange_kernel(*refs):
    chan = lax.axis_index("chan_0") * 2 + lax.axis_index("chan_1")
    all_ref = refs[-1]
    for k, ref in enumerate(refs[:-1]):
        all_ref[chan ^ k] = ref[...]


def lateral_kernel(own_ref, weight_ref, stats_ref, one_ref, two_ref):
    for s in range(8):
        for half in range(2):
            weight_ref[32 * s + 16 * half : 32 * s + 16 * half + 16, :] = own_ref[
                s, 48:64, 256 * half : 256 * half + 256
            ]
    odd = lax.axis_index("chan_0") % 2
    for ref, row in ((one_ref, 1 - odd), (two_ref, odd)):
        at = pl.multiple_of(256 * row, 256)
        for s in range(8):
            ref[s, 0:48, :] = own_ref[s, 0:48, pl.ds(at, 256)]
            ref[s, 48:64, :] = own_ref[s, 64:80, 0:256]
            ref[s, 64:80, :] = own_ref[s, 64:80, 256:512]
            ref[s, 80:96, 0:128] = own_ref[s, 48:64, 128:256]
            ref[s, 80:96, 128:256] = own_ref[s, 48:64, 384:512]
    lane = lax.broadcasted_iota(jnp.int32, (GROUPS, 1, 128), 2)
    total = jnp.zeros((1, 128), F32)
    for n in range(2):
        lateral = dot(weight_ref[:, 0:IN_CH], fine_rows(own_ref, n, 0, COLS))
        total = total + local_stats(lateral, lane, 64 * n)
    stats_ref[...] = jnp.broadcast_to(total, stats_ref.shape)


def join_kernel(
    own_ref, one_ref, two_ref, lat_weight_ref, lat_stats_ref, joined_ref, beside_ref,
    above_ref, below_ref,
):
    odd = lax.axis_index("chan_0") % 2 == 1
    for s in range(8):
        one, two = one_ref[s], two_ref[s]
        above_ref[s] = jnp.where(odd, one, two)
        below_ref[s] = jnp.where(odd, two, one)
    core = lax.axis_index("band_2")
    band = (lax.axis_index("band_0") * 2 + lax.axis_index("band_1")) * 2 + core
    side = lax.axis_index("chan_1")
    pair = band * 4 + lax.axis_index("chan_0")
    at_top = pair == 0
    at_bottom = pair == 127
    source = lax.broadcasted_iota(jnp.int32, (128, HALF), 0)
    column = lanes_of((128, HALF))
    inner_edge = jnp.where(side == 0, HALF - 1, 0)
    near = column // 2
    far = jnp.clip(near - 1 + 2 * (column % 2), 0, 127)
    spread = (
        jnp.where(source == near, 0.75, 0.0)
        + jnp.where(jnp.logical_and(source == far, column != inner_edge), 0.25, 0.0)
    ).astype(BF16)
    gain = vector_col(lat_weight_ref, 0)
    shift = vector_col(lat_weight_ref, 1)
    stats = (lat_stats_ref[0:1], lat_stats_ref[1:2], lat_stats_ref[2:3])
    lane_at = lanes_of((D, HALF))
    small = lanes_of((D, 128))
    first_image = small < 4
    time = small % 4
    norm = [stat_cols(stats, n) for n in range(2)]
    norm = [(mean, lax.rsqrt(var + EPS) * gain) for mean, var in norm]
    lat_weight = lat_weight_ref[:, 0:IN_CH]

    def coarse_main(ref, low, high, n):
        at = 128 * n
        if high is None:
            pieces = [ref[s, low : low + 32, at : at + 128] for s in range(8)]
        else:
            pieces = []
            for s in range(8):
                pieces.append(ref[s, low : low + 16, at : at + 128])
                pieces.append(ref[s, low : low + 16, high + at : high + at + 128])
        return jnp.concatenate(pieces, axis=0)

    def extras(tile, move):
        fine = jnp.concatenate([tile[32 * s : 32 * s + 24] for s in range(8)], axis=0)
        fine = pltpu.roll(dot(lat_weight, fine), 128 - FINE_EDGE + move, axis=1)
        return fine, pltpu.roll(tile.astype(F32), 128 - COARSE_EDGE, axis=1)

    def tile_of(ref):
        pieces = []
        for s in range(8):
            pieces.append(ref[s, 80:96, 0:128])
            pieces.append(ref[s, 80:96, 128:256])
        return jnp.concatenate(pieces, axis=0)

    fine_above, extra_above = extras(tile_of(above_ref), -2)
    fine_own, extra_own = extras(lat_weight_ref[:, 128:256], 0)
    fine_below, extra_below = extras(tile_of(below_ref), 2)
    extra_above = jnp.where(at_top, extra_own, extra_above)
    extra_below = jnp.where(at_bottom, extra_own, extra_below)
    mains = []
    for n in range(2):
        middle = coarse_main(own_ref, 64, 256, n)
        upper = coarse_main(above_ref, 48, None, n)
        lower = coarse_main(below_ref, 48, None, n)
        upper = jnp.where(at_top, middle, upper)
        lower = jnp.where(at_bottom, middle, lower)
        mains.append((upper, middle, lower))
    edge_at = jnp.where(side == 0, 127, 0)
    ups, columns = [], []
    for k, extra in enumerate((extra_above, extra_own, extra_below)):
        edges = []
        for n in range(2):
            main = mains[n][k]
            edges.append(
                jnp.sum(jnp.where(small == edge_at, main.astype(F32), 0.0), axis=1, keepdims=True)
            )
        columns.append(0.75 * extra + 0.25 * jnp.where(first_image, edges[0], edges[1]))
        ups.append(
            [
                dot(mains[n][k], spread)
                + jnp.where(lane_at == inner_edge, 0.25 * extra[:, 4 * n : 4 * n + 1], 0.0)
                for n in range(2)
            ]
        )

    lateral = jnp.where(
        time == 0, fine_above, jnp.where(time == 3, fine_below, fine_own)
    )
    upsampled = jnp.where(
        time == 0,
        0.75 * columns[0] + 0.25 * columns[1],
        jnp.where(
            time == 1,
            0.25 * columns[0] + 0.75 * columns[1],
            jnp.where(
                time == 2,
                0.75 * columns[1] + 0.25 * columns[2],
                0.25 * columns[1] + 0.75 * columns[2],
            ),
        ),
    )
    mean = jnp.where(first_image, norm[0][0], norm[1][0])
    scale = jnp.where(first_image, norm[0][1], norm[1][1])
    value = (lateral - mean) * scale + shift + upsampled
    outside = jnp.logical_or(
        jnp.logical_and(time == 0, at_top), jnp.logical_and(time == 3, at_bottom)
    )
    value = jnp.where(outside, 0.0, value)
    beside_ref[...] = jnp.concatenate(
        [value, pltpu.roll(value, 127, axis=1), pltpu.roll(value, 126, axis=1)], axis=0
    ).astype(BF16)

    for n in range(2):
        mean, scale = norm[n]
        up = [ups[k][n] for k in range(3)]
        rows = (
            (fine_rows(above_ref, n, 0, HALF), 0.75 * up[0] + 0.25 * up[1]),
            (fine_rows(own_ref, n, 0, HALF), 0.25 * up[0] + 0.75 * up[1]),
            (fine_rows(own_ref, n, HALF, COLS), 0.75 * up[1] + 0.25 * up[2]),
            (fine_rows(below_ref, n, 0, HALF), 0.25 * up[1] + 0.75 * up[2]),
        )
        for t, (fine, upsampled) in enumerate(rows):
            value = ((dot(lat_weight, fine) - mean) * scale + shift + upsampled).astype(BF16)
            if t == 0:
                value = jnp.where(at_top, jnp.zeros_like(value), value)
            if t == 3:
                value = jnp.where(at_bottom, jnp.zeros_like(value), value)
            for r in range(2):
                if 0 <= t - r <= 2:
                    joined_ref[
                        n, 256 * (t - r) : 256 * (t - r) + 256, HALF * r : HALF * r + HALF
                    ] = value


def conv_kernel(
    joined_ref, beside_ref, mine_ref, other_ref, keep_ref, send_ref, stats_ref, weight, taps
):
    core = lax.axis_index("band_2")
    side = lax.axis_index("chan_1")
    for part, ref in ((core, mine_ref), (1 - core, other_ref)):
        for s in range(8):
            at = pl.multiple_of(32 * s + 16 * part, 16)
            for a in range(3):
                for b in range(3):
                    piece = ref[s, (a * 3 + b) * 8 : (a * 3 + b) * 8 + 8, :]
                    both = jnp.concatenate([piece[:, 0:256], piece[:, 256:512]], axis=0)
                    weight[b, pl.ds(at, 16), 256 * a : 256 * a + 256] = both
    inner_edge = jnp.where(side == 0, HALF - 1, 0)
    lane = lax.broadcasted_iota(jnp.int32, (GROUPS, 1, 128), 2)
    lane_at = lanes_of((D, HALF))
    beside = dot(weight[jnp.where(side == 0, 2, 0)], beside_ref[...])
    total = jnp.zeros((1, 128), F32)
    for n in range(2):
        for b in range(3):
            taps[b] = dot(weight[b], joined_ref[n])
        out = []
        for r in range(2):
            at = HALF * r
            left = pltpu.roll(taps[0, :, at : at + HALF], 1, axis=1)
            right = pltpu.roll(taps[2, :, at : at + HALF], HALF - 1, axis=1)
            value = taps[1, :, at : at + HALF] + jnp.where(lane_at == 0, 0.0, left)
            value = value + jnp.where(lane_at == HALF - 1, 0.0, right)
            column = beside[:, 4 * n + r : 4 * n + r + 1]
            out.append(value + jnp.where(lane_at == inner_edge, column, 0.0))
        keep_ref[n] = jnp.where(side == 0, out[0], out[1])
        send_ref[n] = jnp.where(side == 0, out[1], out[0])
        total = total + local_stats(jnp.concatenate(out, axis=1), lane, 64 * n)
    stats_ref[...] = jnp.broadcast_to(total, stats_ref.shape)


def query_kernel(
    keep_ref, taken_ref, out_stats_ref, lat_weight_ref, mine_ref, other_ref,
    query_ref, out_ref, weight,
):
    core = lax.axis_index("band_2")
    side = lax.axis_index("chan_1")
    for part, ref in ((core, mine_ref), (1 - core, other_ref)):
        for s in range(8):
            at = pl.multiple_of(32 * s + 16 * part, 16)
            piece = ref[s, MASK_AT : MASK_AT + 8, :]
            both = jnp.concatenate([piece[:, 0:256], piece[:, 256:512]], axis=0)
            weight[pl.ds(at, 16), :] = both
    gain = vector_col(lat_weight_ref, 2)
    shift = vector_col(lat_weight_ref, 3)
    bias = vector_col(lat_weight_ref, 4)
    rows = combine(out_stats_ref[...])
    for n in range(2):
        mean, var = stat_cols(rows, n)
        scale = lax.rsqrt(var + EPS) * gain
        for ref, half in ((keep_ref, side), (taken_ref, 1 - side)):
            activated = jnp.maximum((ref[n] - mean) * scale + shift, 0.0).astype(BF16)
            features = (dot(weight[...], activated) + bias).astype(BF16)
            logits = dot(query_ref[...], features)
            shifted = logits - jnp.max(logits, axis=0, keepdims=True)
            result = shifted - jnp.log(jnp.sum(jnp.exp(shifted), axis=0, keepdims=True))
            for t in range(2):
                at = 4 * QUERIES * n + 2 * half + t
                out_ref[pl.ds(at, QUERIES, stride=4), :] = result[:, 128 * t : 128 * t + 128]


def call(kernel, out_shape, scratch=(), flops=0, space=pltpu.VMEM, out_space=pltpu.VMEM, limit=40 << 20):
    out = pl.BlockSpec(memory_space=out_space)
    single = not isinstance(out_shape, (tuple, list))
    return lambda *args: pl.pallas_call(
        kernel,
        out_shape=out_shape,
        in_specs=[pl.BlockSpec(memory_space=space)] * len(args),
        out_specs=out if single else [out] * len(out_shape),
        scratch_shapes=list(scratch),
        cost_estimate=pl.CostEstimate(flops=flops, bytes_accessed=1 << 20, transcendentals=0),
        compiler_params=pltpu.CompilerParams(vmem_limit_bytes=limit),
    )(*args)


def per_device(
    fine_features,
    coarse_level,
    lat_weight,
    lat_gain,
    lat_shift,
    out_weight,
    out_gain,
    out_shift,
    mask_weight,
    mask_bias,
    queries,
):
    everyone = lax.axis_size(ALL)
    stats_shape = jax.ShapeDtypeStruct((everyone, 128), F32)
    shard_shape = jax.ShapeDtypeStruct((SHARD_ROWS, COLS), BF16)
    all_shape = jax.ShapeDtypeStruct((8, SHARD_ROWS, COLS), BF16)
    side_shape = jax.ShapeDtypeStruct((8, SIDE_ROWS, HALF), BF16)
    half_shape = jax.ShapeDtypeStruct((2, D, HALF), F32)
    swap = [(0, 1), (1, 0)]

    vectors = [v.reshape(1, 32) for v in (lat_gain, lat_shift, out_gain, out_shift, mask_bias)]
    own_out = call(
        pack_own_kernel,
        jax.ShapeDtypeStruct((8, OWN_ROWS, COLS), BF16),
        (
            pltpu.VMEM((2, 24, 8, COLS), BF16),
            pltpu.VMEM((2, 32, 4, 256), BF16),
            pltpu.VMEM((32, IN_CH), BF16),
            pltpu.VMEM((5, 1, 32), BF16),
            pltpu.VMEM((8, OWN_ROWS, COLS), BF16),
            pltpu.VMEM((4, 48 * 8, 128), F32),
            pltpu.VMEM((2, 2, 256, 128), F32),
            pltpu.SemaphoreType.DMA((8,)),
            pltpu.SemaphoreType.DMA((8,)),
        ),
        space=pltpu.HBM,
        out_space=pltpu.HBM,
        limit=60 << 20,
    )(fine_features, coarse_level, lat_weight, *vectors)
    own = lax.all_to_all(own_out, CHAN, 0, 0, tiled=True)
    shard = call(pack_weights_kernel, shard_shape)(out_weight, mask_weight)
    moved = [lax.ppermute(shard, CHAN, [(i, i ^ k) for i in range(8)]) for k in XORS]

    full_lat, stats, first, second = call(
        lateral_kernel,
        [jax.ShapeDtypeStruct((D, 256), BF16), stats_shape, side_shape, side_shape],
        flops=2 * 2 * 256 * 256 * 512,
    )(own)
    pairs = everyone // 2
    swap_at = lambda shift: [
        (2 * p + yl, 2 * ((((p + shift) % pairs ^ 1) - shift) % pairs) + yl)
        for p in range(pairs)
        for yl in range(2)
    ]
    first = lax.ppermute(first, ALL, swap_at(0))
    second = lax.ppermute(second, ALL, swap_at(1))
    stats = lax.all_to_all(stats, ALL, 0, 0, tiled=True)
    stats = call(combine_kernel, jax.ShapeDtypeStruct((8, 128), F32), flops=1 << 20)(stats)

    by_xor = dict(zip(XORS, moved))
    mine = call(arrange_kernel, all_shape)(shard, *[by_xor[k] for k in range(1, 8)])
    other = lax.ppermute(mine, "band_2", swap)
    joined, beside = call(
        join_kernel,
        [jax.ShapeDtypeStruct((2, 3 * D, COLS), BF16), jax.ShapeDtypeStruct((3 * D, 128), BF16)],
        (
            pltpu.VMEM((8, SIDE_ROWS, HALF), BF16),
            pltpu.VMEM((8, SIDE_ROWS, HALF), BF16),
        ),
        flops=2 * 2 * 256 * 256 * 512 * 7,
    )(own, first, second, full_lat, stats)
    keep, send, stats = call(
        conv_kernel,
        [half_shape, half_shape, stats_shape],
        (pltpu.VMEM((3, D, 3 * D), BF16), pltpu.VMEM((3, D, COLS), F32)),
        flops=2 * 2 * 256 * 256 * 512 * 9,
    )(joined, beside, mine, other)
    taken = lax.ppermute(send, "chan_1", swap)
    stats = lax.all_to_all(stats, ALL, 0, 0, tiled=True)
    log_probs = call(
        query_kernel,
        jax.ShapeDtypeStruct((2 * QUERIES * 4, 128), F32),
        (pltpu.VMEM((D, D), BF16),),
        flops=2 * 2 * 256 * 256 * 512 * 2,
    )(keep, taken, stats, full_lat, mine, other, queries)
    return log_probs.reshape(2, QUERIES, 1, COLS)


def solution(mesh):
    finer = Mesh(
        mesh.devices.reshape(8, 2, 2, 4, 2), ("band_0", "band_1", "band_2", "chan_0", "chan_1")
    )

    return jax.shard_map(
        per_device,
        mesh=finer,
        in_specs=(
            P(None, CHAN, BAND, None),
            P(None, CHAN, BAND, None),
            P(CHAN, None),
            P(CHAN),
            P(CHAN),
            P(None, None, CHAN, None),
            P(CHAN),
            P(CHAN),
            P(CHAN, None),
            P(CHAN),
            P(),
        ),
        out_specs=P(None, None, BAND + CHAN, None),
        check_vma=False,
    )
```

```python
import jax
import jax.numpy as jnp
from jax import lax
from jax.experimental import pallas as pl
from jax.experimental.pallas import tpu as pltpu
from jax.sharding import Mesh
from jax.sharding import PartitionSpec as P


D = 256
GROUPS = 32
IN_CH = 192
COLS = 512
HALF = 256
QUERIES = 200
BAND = ("band_0", "band_1", "band_2")
CHAN = ("chan_0", "chan_1")
ALL = BAND + CHAN
EPS = 1e-05
F32 = jnp.float32
BF16 = jnp.bfloat16
OWN_ROWS = 80
VECTORS = 64
FINE_EDGE = 72
COARSE_EDGE = 80
SIDE_ROWS = 96
MASK_AT = 144
SHARD_ROWS = 176
XORS = (4, 1, 2, 5, 6, 3, 7)


def dot(a, b):
    return lax.dot_general(a, b, (((1,), (0,)), ((), ())), preferred_element_type=F32)


def local_stats(values, lane, offset):
    blocks = values.reshape(GROUPS, D // GROUPS, COLS)
    count = D // GROUPS * COLS
    mean = jnp.sum(jnp.sum(blocks, axis=2, keepdims=True), axis=1, keepdims=True) / count
    dev = blocks - mean
    m2 = jnp.sum(jnp.sum(dev * dev, axis=2, keepdims=True), axis=1, keepdims=True)
    group = lax.broadcasted_iota(jnp.int32, (GROUPS, 1, 128), 0)
    row = jnp.where(lane == group + offset, mean, 0.0)
    row = row + jnp.where(lane == group + (offset + GROUPS), m2, 0.0)
    return jnp.sum(row, axis=0)


def combine(stats):
    devices = stats.shape[0]
    count = D // GROUPS * COLS
    mean = jnp.sum(stats, axis=0, keepdims=True) / devices
    dev = stats - mean
    spread = jnp.sum(dev * dev, axis=0, keepdims=True) * (1.0 / devices)
    return mean, spread, mean * (1.0 / count)


def stat_cols(rows, image):
    mean, spread, inner = rows
    lane = lax.broadcasted_iota(jnp.int32, (D, 128), 1)
    group = lax.broadcasted_iota(jnp.int32, (D, 128), 0) // (D // GROUPS)
    at_mean = lane == group + image * 2 * GROUPS
    at_m2 = lane == group + (image * 2 + 1) * GROUPS
    mean_col = jnp.sum(jnp.where(at_mean, mean, 0.0), axis=1, keepdims=True)
    var_col = jnp.sum(
        jnp.where(at_mean, spread, 0.0) + jnp.where(at_m2, inner, 0.0), axis=1, keepdims=True
    )
    return mean_col, var_col


def combine_kernel(stats_ref, rows_ref):
    mean, spread, inner = combine(stats_ref[...])
    rows_ref[0:1] = mean
    rows_ref[1:2] = spread
    rows_ref[2:3] = inner
    rows_ref[3:8] = jnp.zeros((5, 128), F32)


def vector_col(lat_weight_ref, index):
    return lat_weight_ref[:, 128:256].astype(F32)[:, VECTORS + index : VECTORS + index + 1]


def lanes_of(shape):
    return lax.broadcasted_iota(jnp.int32, shape, len(shape) - 1)


def fine_rows(ref, image, low, high):
    return jnp.concatenate(
        [ref[s, 24 * image : 24 * image + 24, low:high] for s in range(8)], axis=0
    )


def pack_own_kernel(fine_hbm, coarse_hbm, weight_hbm, *refs):
    vec_hbm, own_hbm = refs[:5], refs[5]
    fine_ref, coarse_ref, weight_ref, vec_ref, own_ref, rows, coarse, sems, out_sems = refs[6:]
    pairs = [(coarse_hbm.at[n], coarse_ref.at[n]) for n in range(2)] + [(weight_hbm, weight_ref)]
    pairs += [(vec, vec_ref.at[i]) for i, vec in enumerate(vec_hbm)]
    for n in range(2):
        for j in range(3):
            at = (n, pl.ds(8 * j, 8))
            pairs.append((fine_hbm.at[at], fine_ref.at[at]))
    copies = [
        pltpu.make_async_copy(source, target, sems.at[i])
        for i, (source, target) in enumerate(pairs)
    ]
    for copy in copies:
        copy.start()
    for copy in copies[:-6]:
        copy.wait()
    for n in range(2):
        for t in range(2):
            piece = coarse_ref[n, :, :, 128 * t : 128 * t + 128].astype(F32)
            piece = jnp.concatenate([piece, jnp.zeros_like(piece)], axis=1)
            coarse[n, t, 0:256] = piece.reshape(256, 128)
    lane = lanes_of((32, 128))
    vec_lane = lanes_of((32, 32))
    vec_row = lax.broadcasted_iota(jnp.int32, (32, 32), 0)
    weight = weight_ref[...].astype(F32)
    second = jnp.concatenate([weight[:, 128:IN_CH], jnp.zeros((32, 256 - IN_CH), F32)], axis=1)
    for i in range(5):
        vec = jnp.where(vec_lane == vec_row, vec_ref[i].astype(F32), 0.0)
        second += jnp.where(lane == VECTORS + i, jnp.sum(vec, axis=1, keepdims=True), 0.0)
    first = weight[:, 0:128].astype(BF16)
    tails = []
    for h in range(2):
        for q in range(4):
            d = 2 * q + h
            tail = second
            own_ref[d, 48:64, 0:128] = first[0:16]
            own_ref[d, 48:64, 256:384] = first[16:32]
            for n in range(2):
                row = coarse[n, h, pl.ds(q, 32, stride=8), :].astype(BF16)
                own_ref[d, 64:80, 128 * n : 128 * n + 128] = row[0:16]
                own_ref[d, 64:80, 256 + 128 * n : 384 + 128 * n] = row[16:32]
                row = coarse[n, 1 - h, pl.ds(q, 32, stride=8), :]
                edge = row[:, 0:1] if h == 0 else row[:, 127:128]
                tail = jnp.where(lane // 4 == COARSE_EDGE // 4 + n, edge, tail)
            tails.append(tail)
    for copy in copies[-6:]:
        copy.wait()
    for t in range(4):
        piece = fine_ref[:, :, :, 128 * t : 128 * t + 128].astype(F32)
        rows[t, 0:384] = piece.reshape(48 * 8, 128)
    out = []
    for h in range(2):
        for q in range(4):
            d = 2 * q + h
            tail = tails[4 * h + q]
            for r in range(2):
                for t in range(2):
                    row = rows[2 * h + t, pl.ds(2 * q + r, 48, stride=8), :]
                    at = 256 * r + 128 * t
                    own_ref[d, 0:48, at : at + 128] = row.astype(BF16)
                row = rows[2 - h, pl.ds(2 * q + r, 48, stride=8), :]
                edge = row[:, 0:1] if h == 0 else row[:, 127:128]
                for n in range(2):
                    column = jnp.concatenate(
                        [edge[24 * n : 24 * n + 24], jnp.zeros((8, 1), F32)], axis=0
                    )
                    tail = jnp.where(lane == FINE_EDGE + 4 * n + 1 + r, column, tail)
            tail = tail.astype(BF16)
            own_ref[d, 48:64, 128:256] = tail[0:16]
            own_ref[d, 48:64, 384:512] = tail[16:32]
            out.append(pltpu.make_async_copy(own_ref.at[d], own_hbm.at[d], out_sems.at[d]))
            out[-1].start()
    for copy in out:
        copy.wait()


def pack_weights_kernel(conv_ref, mask_ref, shard_ref):
    half = pl.multiple_of(16 * lax.axis_index("band_2"), 16)
    for k in range(9):
        shard_ref[16 * k : 16 * k + 16] = conv_ref[k // 3, k % 3, pl.ds(half, 16), :]
    shard_ref[MASK_AT : MASK_AT + 32] = mask_ref[...]


def arrange_kernel(*refs):
    chan = lax.axis_index("chan_0") * 2 + lax.axis_index("chan_1")
    half_ref, mask_ref = refs[-2:]
    for k, ref in enumerate(refs[:-2]):
        s = chan ^ k
        for a in range(3):
            for b in range(3):
                at = pl.multiple_of(128 * b + 16 * s, 16)
                piece = ref[16 * (3 * a + b) : 16 * (3 * a + b) + 16]
                half_ref[pl.ds(at, 16), 256 * a : 256 * a + 256] = piece
        mask_ref[pl.ds(pl.multiple_of(32 * s, 32), 32)] = ref[MASK_AT : MASK_AT + 32]


def lateral_kernel(own_ref, weight_ref, stats_ref, one_ref, two_ref):
    for s in range(8):
        for half in range(2):
            weight_ref[32 * s + 16 * half : 32 * s + 16 * half + 16, :] = own_ref[
                s, 48:64, 256 * half : 256 * half + 256
            ]
    odd = lax.axis_index("chan_0") % 2
    for ref, row in ((one_ref, 1 - odd), (two_ref, odd)):
        at = pl.multiple_of(256 * row, 256)
        for s in range(8):
            ref[s, 0:48, :] = own_ref[s, 0:48, pl.ds(at, 256)]
            ref[s, 48:64, :] = own_ref[s, 64:80, 0:256]
            ref[s, 64:80, :] = own_ref[s, 64:80, 256:512]
            ref[s, 80:96, 0:128] = own_ref[s, 48:64, 128:256]
            ref[s, 80:96, 128:256] = own_ref[s, 48:64, 384:512]
    lane = lax.broadcasted_iota(jnp.int32, (GROUPS, 1, 128), 2)
    total = jnp.zeros((1, 128), F32)
    for n in range(2):
        lateral = dot(weight_ref[:, 0:IN_CH], fine_rows(own_ref, n, 0, COLS))
        total = total + local_stats(lateral, lane, 64 * n)
    stats_ref[...] = jnp.broadcast_to(total, stats_ref.shape)


def join_kernel(
    own_ref, one_ref, two_ref, lat_weight_ref, lat_stats_ref, joined_ref, beside_ref,
    above_ref, below_ref,
):
    odd = lax.axis_index("chan_0") % 2 == 1
    for s in range(8):
        one, two = one_ref[s], two_ref[s]
        above_ref[s] = jnp.where(odd, one, two)
        below_ref[s] = jnp.where(odd, two, one)
    core = lax.axis_index("band_2")
    band = (lax.axis_index("band_0") * 2 + lax.axis_index("band_1")) * 2 + core
    side = lax.axis_index("chan_1")
    pair = band * 4 + lax.axis_index("chan_0")
    at_top = pair == 0
    at_bottom = pair == 127
    source = lax.broadcasted_iota(jnp.int32, (128, HALF), 0)
    column = lanes_of((128, HALF))
    inner_edge = jnp.where(side == 0, HALF - 1, 0)
    near = column // 2
    far = jnp.clip(near - 1 + 2 * (column % 2), 0, 127)
    spread = (
        jnp.where(source == near, 0.75, 0.0)
        + jnp.where(jnp.logical_and(source == far, column != inner_edge), 0.25, 0.0)
    ).astype(BF16)
    gain = vector_col(lat_weight_ref, 0)
    shift = vector_col(lat_weight_ref, 1)
    stats = (lat_stats_ref[0:1], lat_stats_ref[1:2], lat_stats_ref[2:3])
    lane_at = lanes_of((D, HALF))
    small = lanes_of((D, 128))
    first_image = small < 4
    time = small % 4
    norm = [stat_cols(stats, n) for n in range(2)]
    norm = [(mean, lax.rsqrt(var + EPS) * gain) for mean, var in norm]
    lat_weight = lat_weight_ref[:, 0:IN_CH]

    def coarse_main(ref, low, high, n):
        at = 128 * n
        if high is None:
            pieces = [ref[s, low : low + 32, at : at + 128] for s in range(8)]
        else:
            pieces = []
            for s in range(8):
                pieces.append(ref[s, low : low + 16, at : at + 128])
                pieces.append(ref[s, low : low + 16, high + at : high + at + 128])
        return jnp.concatenate(pieces, axis=0)

    def extras(tile, move):
        fine = jnp.concatenate([tile[32 * s : 32 * s + 24] for s in range(8)], axis=0)
        fine = pltpu.roll(dot(lat_weight, fine), 128 - FINE_EDGE + move, axis=1)
        return fine, pltpu.roll(tile.astype(F32), 128 - COARSE_EDGE, axis=1)

    def tile_of(ref):
        pieces = []
        for s in range(8):
            pieces.append(ref[s, 80:96, 0:128])
            pieces.append(ref[s, 80:96, 128:256])
        return jnp.concatenate(pieces, axis=0)

    fine_above, extra_above = extras(tile_of(above_ref), -2)
    fine_own, extra_own = extras(lat_weight_ref[:, 128:256], 0)
    fine_below, extra_below = extras(tile_of(below_ref), 2)
    extra_above = jnp.where(at_top, extra_own, extra_above)
    extra_below = jnp.where(at_bottom, extra_own, extra_below)
    mains = []
    for n in range(2):
        middle = coarse_main(own_ref, 64, 256, n)
        upper = coarse_main(above_ref, 48, None, n)
        lower = coarse_main(below_ref, 48, None, n)
        upper = jnp.where(at_top, middle, upper)
        lower = jnp.where(at_bottom, middle, lower)
        mains.append((upper, middle, lower))
    edge_at = jnp.where(side == 0, 127, 0)
    ups, columns = [], []
    for k, extra in enumerate((extra_above, extra_own, extra_below)):
        edges = []
        for n in range(2):
            main = mains[n][k]
            edges.append(
                jnp.sum(jnp.where(small == edge_at, main.astype(F32), 0.0), axis=1, keepdims=True)
            )
        columns.append(0.75 * extra + 0.25 * jnp.where(first_image, edges[0], edges[1]))
        ups.append(
            [
                dot(mains[n][k], spread)
                + jnp.where(lane_at == inner_edge, 0.25 * extra[:, 4 * n : 4 * n + 1], 0.0)
                for n in range(2)
            ]
        )

    lateral = jnp.where(
        time == 0, fine_above, jnp.where(time == 3, fine_below, fine_own)
    )
    upsampled = jnp.where(
        time == 0,
        0.75 * columns[0] + 0.25 * columns[1],
        jnp.where(
            time == 1,
            0.25 * columns[0] + 0.75 * columns[1],
            jnp.where(
                time == 2,
                0.75 * columns[1] + 0.25 * columns[2],
                0.25 * columns[1] + 0.75 * columns[2],
            ),
        ),
    )
    mean = jnp.where(first_image, norm[0][0], norm[1][0])
    scale = jnp.where(first_image, norm[0][1], norm[1][1])
    value = (lateral - mean) * scale + shift + upsampled
    outside = jnp.logical_or(
        jnp.logical_and(time == 0, at_top), jnp.logical_and(time == 3, at_bottom)
    )
    value = jnp.where(outside, 0.0, value)
    beside_ref[...] = jnp.concatenate(
        [value, pltpu.roll(value, 127, axis=1), pltpu.roll(value, 126, axis=1)], axis=0
    ).astype(BF16)

    for n in range(2):
        mean, scale = norm[n]
        up = [ups[k][n] for k in range(3)]
        rows = (
            (fine_rows(above_ref, n, 0, HALF), 0.75 * up[0] + 0.25 * up[1]),
            (fine_rows(own_ref, n, 0, HALF), 0.25 * up[0] + 0.75 * up[1]),
            (fine_rows(own_ref, n, HALF, COLS), 0.75 * up[1] + 0.25 * up[2]),
            (fine_rows(below_ref, n, 0, HALF), 0.25 * up[1] + 0.75 * up[2]),
        )
        for t, (fine, upsampled) in enumerate(rows):
            value = ((dot(lat_weight, fine) - mean) * scale + shift + upsampled).astype(BF16)
            if t == 0:
                value = jnp.where(at_top, jnp.zeros_like(value), value)
            if t == 3:
                value = jnp.where(at_bottom, jnp.zeros_like(value), value)
            for r in range(2):
                if 0 <= t - r <= 2:
                    joined_ref[
                        n, 256 * (t - r) : 256 * (t - r) + 256, HALF * r : HALF * r + HALF
                    ] = value


def conv_kernel(
    joined_ref, beside_ref, mine_ref, other_ref, keep_ref, send_ref, stats_ref, taps, beside
):
    core = lax.axis_index("band_2")
    side = lax.axis_index("chan_1")
    halves = ((core, mine_ref), (1 - core, other_ref))
    edge_tap = pl.multiple_of(jnp.where(side == 0, 256, 0), 128)
    for part, ref in halves:
        value = dot(ref[pl.ds(edge_tap, 128)], beside_ref[...])
        for s in range(8):
            at = pl.multiple_of(32 * s + 16 * part, 16)
            beside[pl.ds(at, 16)] = value[16 * s : 16 * s + 16]
    inner_edge = jnp.where(side == 0, HALF - 1, 0)
    lane = lax.broadcasted_iota(jnp.int32, (GROUPS, 1, 128), 2)
    lane_at = lanes_of((D, HALF))
    total = jnp.zeros((1, 128), F32)
    for n in range(2):
        for part, ref in halves:
            value = dot(ref[...], joined_ref[n])
            for b in range(3):
                for s in range(8):
                    at = pl.multiple_of(32 * s + 16 * part, 16)
                    row = 128 * b + 16 * s
                    taps[b, pl.ds(at, 16), :] = value[row : row + 16]
        out = []
        for r in range(2):
            at = HALF * r
            left = pltpu.roll(taps[0, :, at : at + HALF], 1, axis=1)
            right = pltpu.roll(taps[2, :, at : at + HALF], HALF - 1, axis=1)
            value = taps[1, :, at : at + HALF] + jnp.where(lane_at == 0, 0.0, left)
            value = value + jnp.where(lane_at == HALF - 1, 0.0, right)
            column = beside[:, 4 * n + r : 4 * n + r + 1]
            out.append(value + jnp.where(lane_at == inner_edge, column, 0.0))
        keep_ref[n] = jnp.where(side == 0, out[0], out[1])
        send_ref[n] = jnp.where(side == 0, out[1], out[0])
        total = total + local_stats(jnp.concatenate(out, axis=1), lane, 64 * n)
    stats_ref[...] = jnp.broadcast_to(total, stats_ref.shape)


def query_kernel(
    keep_ref, taken_ref, out_stats_ref, lat_weight_ref, mask_ref, query_ref, out_hbm, out_ref, sems
):
    side = lax.axis_index("chan_1")
    gain = vector_col(lat_weight_ref, 2)
    shift = vector_col(lat_weight_ref, 3)
    bias = vector_col(lat_weight_ref, 4)
    rows = combine(out_stats_ref[...])
    copies = []
    for n in range(2):
        mean, var = stat_cols(rows, n)
        scale = lax.rsqrt(var + EPS) * gain
        for ref, half in ((keep_ref, side), (taken_ref, 1 - side)):
            activated = jnp.maximum((ref[n] - mean) * scale + shift, 0.0).astype(BF16)
            features = (dot(mask_ref[...], activated) + bias).astype(BF16)
            logits = dot(query_ref[...], features)
            shifted = logits - jnp.max(logits, axis=0, keepdims=True)
            result = shifted - jnp.log(jnp.sum(jnp.exp(shifted), axis=0, keepdims=True))
            for t in range(2):
                at = 4 * QUERIES * n + 2 * half + t
                out_ref[pl.ds(at, QUERIES, stride=4), :] = result[:, 128 * t : 128 * t + 128]
        for i in range(4):
            piece = pl.ds(QUERIES * (4 * n + i), QUERIES)
            copies.append(
                pltpu.make_async_copy(out_ref.at[piece], out_hbm.at[piece], sems.at[4 * n + i])
            )
            copies[-1].start()
    for copy in copies:
        copy.wait()


def call(kernel, out_shape, scratch=(), flops=0, space=pltpu.VMEM, out_space=pltpu.VMEM, limit=40 << 20):
    out = pl.BlockSpec(memory_space=out_space)
    single = not isinstance(out_shape, (tuple, list))
    return lambda *args: pl.pallas_call(
        kernel,
        out_shape=out_shape,
        in_specs=[pl.BlockSpec(memory_space=space)] * len(args),
        out_specs=out if single else [out] * len(out_shape),
        scratch_shapes=list(scratch),
        cost_estimate=pl.CostEstimate(flops=flops, bytes_accessed=1 << 20, transcendentals=0),
        compiler_params=pltpu.CompilerParams(vmem_limit_bytes=limit),
    )(*args)


def per_device(
    fine_features,
    coarse_level,
    lat_weight,
    lat_gain,
    lat_shift,
    out_weight,
    out_gain,
    out_shift,
    mask_weight,
    mask_bias,
    queries,
):
    everyone = lax.axis_size(ALL)
    stats_shape = jax.ShapeDtypeStruct((everyone, 128), F32)
    shard_shape = jax.ShapeDtypeStruct((SHARD_ROWS, D), BF16)
    weight_shapes = [
        jax.ShapeDtypeStruct((3 * D // 2, 3 * D), BF16),
        jax.ShapeDtypeStruct((D, D), BF16),
    ]
    side_shape = jax.ShapeDtypeStruct((8, SIDE_ROWS, HALF), BF16)
    half_shape = jax.ShapeDtypeStruct((2, D, HALF), F32)
    swap = [(0, 1), (1, 0)]

    vectors = [v.reshape(1, 32) for v in (lat_gain, lat_shift, out_gain, out_shift, mask_bias)]
    own_out = call(
        pack_own_kernel,
        jax.ShapeDtypeStruct((8, OWN_ROWS, COLS), BF16),
        (
            pltpu.VMEM((2, 24, 8, COLS), BF16),
            pltpu.VMEM((2, 32, 4, 256), BF16),
            pltpu.VMEM((32, IN_CH), BF16),
            pltpu.VMEM((5, 1, 32), BF16),
            pltpu.VMEM((8, OWN_ROWS, COLS), BF16),
            pltpu.VMEM((4, 48 * 8 + 8, 128), F32),
            pltpu.VMEM((2, 2, 256 + 8, 128), F32),
            pltpu.SemaphoreType.DMA((14,)),
            pltpu.SemaphoreType.DMA((8,)),
        ),
        space=pltpu.HBM,
        out_space=pltpu.HBM,
        limit=60 << 20,
    )(fine_features, coarse_level, lat_weight, *vectors)
    own = lax.all_to_all(own_out, CHAN, 0, 0, tiled=True)
    shard = call(pack_weights_kernel, shard_shape)(out_weight, mask_weight)
    moved = [lax.ppermute(shard, CHAN, [(i, i ^ k) for i in range(8)]) for k in XORS]

    full_lat, stats, first, second = call(
        lateral_kernel,
        [jax.ShapeDtypeStruct((D, 256), BF16), stats_shape, side_shape, side_shape],
        flops=2 * 2 * 256 * 256 * 512,
    )(own)
    pairs = everyone // 2
    swap_at = lambda shift: [
        (2 * p + yl, 2 * ((((p + shift) % pairs ^ 1) - shift) % pairs) + yl)
        for p in range(pairs)
        for yl in range(2)
    ]
    first = lax.ppermute(first, ALL, swap_at(0))
    second = lax.ppermute(second, ALL, swap_at(1))
    stats = lax.all_to_all(stats, ALL, 0, 0, tiled=True)
    stats = call(combine_kernel, jax.ShapeDtypeStruct((8, 128), F32), flops=1 << 20)(stats)

    by_xor = dict(zip(XORS, moved))
    mine, mask = call(arrange_kernel, weight_shapes)(
        shard, *[by_xor[k] for k in range(1, 8)]
    )
    other = lax.ppermute(mine, "band_2", swap)
    joined, beside = call(
        join_kernel,
        [jax.ShapeDtypeStruct((2, 3 * D, COLS), BF16), jax.ShapeDtypeStruct((3 * D, 128), BF16)],
        (
            pltpu.VMEM((8, SIDE_ROWS, HALF), BF16),
            pltpu.VMEM((8, SIDE_ROWS, HALF), BF16),
        ),
        flops=2 * 2 * 256 * 256 * 512 * 7,
    )(own, first, second, full_lat, stats)
    keep, send, stats = call(
        conv_kernel,
        [half_shape, half_shape, stats_shape],
        (pltpu.VMEM((3, D, COLS), F32), pltpu.VMEM((D, 128), F32)),
        flops=2 * 2 * 256 * 256 * 512 * 9,
    )(joined, beside, mine, other)
    taken = lax.ppermute(send, "chan_1", swap)
    stats = lax.all_to_all(stats, ALL, 0, 0, tiled=True)
    log_probs = call(
        query_kernel,
        jax.ShapeDtypeStruct((2 * QUERIES * 4, 128), F32),
        (
            pltpu.VMEM((2 * QUERIES * 4 + 8, 128), F32),
            pltpu.SemaphoreType.DMA((8,)),
        ),
        flops=2 * 2 * 256 * 256 * 512 * 2,
        out_space=pltpu.HBM,
    )(keep, taken, stats, full_lat, mask, queries)
    return log_probs.reshape(2, QUERIES, 1, COLS)


def solution(mesh):
    finer = Mesh(
        mesh.devices.reshape(8, 2, 2, 4, 2), ("band_0", "band_1", "band_2", "chan_0", "chan_1")
    )

    return jax.shard_map(
        per_device,
        mesh=finer,
        in_specs=(
            P(None, CHAN, BAND, None),
            P(None, CHAN, BAND, None),
            P(CHAN, None),
            P(CHAN),
            P(CHAN),
            P(None, None, CHAN, None),
            P(CHAN),
            P(CHAN),
            P(CHAN, None),
            P(CHAN),
            P(),
        ),
        out_specs=P(None, None, BAND + CHAN, None),
        check_vma=False,
    )
```

```python
import jax
import jax.numpy as jnp
from jax import lax
from jax.experimental import pallas as pl
from jax.experimental.pallas import tpu as pltpu
from jax.sharding import Mesh
from jax.sharding import PartitionSpec as P


D = 256
GROUPS = 32
IN_CH = 192
COLS = 512
HALF = 256
QUERIES = 200
BAND = ("band_0", "band_1", "band_2")
CHAN = ("chan_0", "chan_1")
ALL = BAND + CHAN
EPS = 1e-05
F32 = jnp.float32
BF16 = jnp.bfloat16
OWN_ROWS = 120
VECTORS = 64
FINE_EDGE = 72
COARSE_EDGE = 80
SIDE_ROWS = 96
BLOCKS = 5
MASK_AT = 144


def dot(a, b):
    return lax.dot_general(a, b, (((1,), (0,)), ((), ())), preferred_element_type=F32)


def local_stats(values, lane, offset):
    blocks = values.reshape(GROUPS, D // GROUPS, COLS)
    count = D // GROUPS * COLS
    mean = jnp.sum(jnp.sum(blocks, axis=2, keepdims=True), axis=1, keepdims=True) / count
    dev = blocks - mean
    m2 = jnp.sum(jnp.sum(dev * dev, axis=2, keepdims=True), axis=1, keepdims=True)
    group = lax.broadcasted_iota(jnp.int32, (GROUPS, 1, 128), 0)
    row = jnp.where(lane == group + offset, mean, 0.0)
    row = row + jnp.where(lane == group + (offset + GROUPS), m2, 0.0)
    return jnp.sum(row, axis=0)


def combine(stats):
    devices = stats.shape[0]
    count = D // GROUPS * COLS
    mean = jnp.sum(stats, axis=0, keepdims=True) / devices
    dev = stats - mean
    spread = jnp.sum(dev * dev, axis=0, keepdims=True) * (1.0 / devices)
    return mean, spread, mean * (1.0 / count)


def stat_cols(rows, image):
    mean, spread, inner = rows
    lane = lax.broadcasted_iota(jnp.int32, (D, 128), 1)
    group = lax.broadcasted_iota(jnp.int32, (D, 128), 0) // (D // GROUPS)
    at_mean = lane == group + image * 2 * GROUPS
    at_m2 = lane == group + (image * 2 + 1) * GROUPS
    mean_col = jnp.sum(jnp.where(at_mean, mean, 0.0), axis=1, keepdims=True)
    var_col = jnp.sum(
        jnp.where(at_mean, spread, 0.0) + jnp.where(at_m2, inner, 0.0), axis=1, keepdims=True
    )
    return mean_col, var_col


def combine_kernel(stats_ref, rows_ref):
    mean, spread, inner = combine(stats_ref[...])
    rows_ref[0:1] = mean
    rows_ref[1:2] = spread
    rows_ref[2:3] = inner
    rows_ref[3:8] = jnp.zeros((5, 128), F32)


def vector_col(lat_weight_ref, index):
    return lat_weight_ref[:, 128:256].astype(F32)[:, VECTORS + index : VECTORS + index + 1]


def lanes_of(shape):
    return lax.broadcasted_iota(jnp.int32, shape, len(shape) - 1)


def fine_rows(ref, image, low, high):
    return jnp.concatenate(
        [ref[s, 24 * image : 24 * image + 24, low:high] for s in range(8)], axis=0
    )


def pack_own_kernel(fine_hbm, coarse_hbm, weight_hbm, conv_hbm, mask_hbm, *refs):
    vec_hbm, own_ref = refs[:5], refs[5]
    fine_ref, coarse_ref, weight_ref, conv_ref, vec_ref, rows, coarse, sems = refs[6:]
    pairs = [(coarse_hbm, coarse_ref), (weight_hbm, weight_ref)]
    pairs += [(vec, vec_ref.at[i]) for i, vec in enumerate(vec_hbm)]
    pairs += [(conv_hbm, conv_ref.at[pl.ds(0, 9)]), (mask_hbm, conv_ref.at[9]), (fine_hbm, fine_ref)]
    copies = [
        pltpu.make_async_copy(source, target, sems.at[i])
        for i, (source, target) in enumerate(pairs)
    ]
    for copy in copies:
        copy.start()
    for copy in copies[:-1]:
        copy.wait()
    for n in range(2):
        for t in range(2):
            piece = coarse_ref[n, :, :, 128 * t : 128 * t + 128].astype(F32)
            piece = jnp.concatenate([piece, jnp.zeros_like(piece)], axis=1)
            coarse[n, t, 0:256] = piece.reshape(256, 128)
    lane = lanes_of((32, 128))
    vec_lane = lanes_of((32, 32))
    vec_row = lax.broadcasted_iota(jnp.int32, (32, 32), 0)
    weight = weight_ref[...].astype(F32)
    second = jnp.concatenate([weight[:, 128:IN_CH], jnp.zeros((32, 256 - IN_CH), F32)], axis=1)
    for i in range(5):
        vec = jnp.where(vec_lane == vec_row, vec_ref[i].astype(F32), 0.0)
        second += jnp.where(lane == VECTORS + i, jnp.sum(vec, axis=1, keepdims=True), 0.0)
    first = weight[:, 0:128].astype(BF16)
    half = pl.multiple_of(16 * lax.axis_index("band_2"), 16)
    block = BLOCKS * (lax.axis_index("band_0") % 2)
    blocks = [conv_ref[block + i, pl.ds(half, 16), :] for i in range(BLOCKS)]
    last = blocks[4].astype(F32)
    last = jnp.concatenate([last[0:8], last[8:16]], axis=1).astype(BF16)
    tails = []
    for h in range(2):
        for q in range(4):
            d = 2 * q + h
            tail = second
            own_ref[d, 48:64, 0:128] = first[0:16]
            own_ref[d, 48:64, 256:384] = first[16:32]
            for i in range(4):
                at = 80 + 16 * (i // 2)
                own_ref[d, at : at + 16, 256 * (i % 2) : 256 * (i % 2) + 256] = blocks[i]
            own_ref[d, 112:120, :] = last
            for n in range(2):
                row = coarse[n, h, pl.ds(q, 32, stride=8), :].astype(BF16)
                own_ref[d, 64:80, 128 * n : 128 * n + 128] = row[0:16]
                own_ref[d, 64:80, 256 + 128 * n : 384 + 128 * n] = row[16:32]
                row = coarse[n, 1 - h, pl.ds(q, 32, stride=8), :]
                edge = row[:, 0:1] if h == 0 else row[:, 127:128]
                tail = jnp.where(lane // 4 == COARSE_EDGE // 4 + n, edge, tail)
            tails.append(tail)
    copies[-1].wait()
    for t in range(4):
        piece = fine_ref[:, :, :, 128 * t : 128 * t + 128].astype(F32)
        rows[t, 0:384] = piece.reshape(48 * 8, 128)
    for h in range(2):
        for q in range(4):
            d = 2 * q + h
            tail = tails[4 * h + q]
            for r in range(2):
                for t in range(2):
                    row = rows[2 * h + t, pl.ds(2 * q + r, 48, stride=8), :]
                    at = 256 * r + 128 * t
                    own_ref[d, 0:48, at : at + 128] = row.astype(BF16)
                row = rows[2 - h, pl.ds(2 * q + r, 48, stride=8), :]
                edge = row[:, 0:1] if h == 0 else row[:, 127:128]
                for n in range(2):
                    column = jnp.concatenate(
                        [edge[24 * n : 24 * n + 24], jnp.zeros((8, 1), F32)], axis=0
                    )
                    tail = jnp.where(lane == FINE_EDGE + 4 * n + 1 + r, column, tail)
            tail = tail.astype(BF16)
            own_ref[d, 48:64, 128:256] = tail[0:16]
            own_ref[d, 48:64, 384:512] = tail[16:32]


def arrange_kernel(quarter_ref, other_ref, all_ref):
    parity = lax.axis_index("band_0") % 2
    rows = 16 * BLOCKS
    all_ref[:, pl.ds(pl.multiple_of(rows * parity, 16), rows), :] = quarter_ref[...]
    all_ref[:, pl.ds(pl.multiple_of(rows - rows * parity, 16), rows), :] = other_ref[...]


def lateral_kernel(own_ref, weight_ref, stats_ref, one_ref, two_ref, quarter_ref):
    for s in range(8):
        for half in range(2):
            weight_ref[32 * s + 16 * half : 32 * s + 16 * half + 16, :] = own_ref[
                s, 48:64, 256 * half : 256 * half + 256
            ]
    for s in range(8):
        for i in range(4):
            at = 80 + 16 * (i // 2)
            quarter_ref[s, 16 * i : 16 * i + 16] = own_ref[
                s, at : at + 16, 256 * (i % 2) : 256 * (i % 2) + 256
            ]
        last = own_ref[s, 112:120, :]
        quarter_ref[s, 64:80] = jnp.concatenate([last[:, 0:256], last[:, 256:512]], axis=0)
    odd = lax.axis_index("chan_0") % 2
    for ref, row in ((one_ref, 1 - odd), (two_ref, odd)):
        at = pl.multiple_of(256 * row, 256)
        for s in range(8):
            ref[s, 0:48, :] = own_ref[s, 0:48, pl.ds(at, 256)]
            ref[s, 48:64, :] = own_ref[s, 64:80, 0:256]
            ref[s, 64:80, :] = own_ref[s, 64:80, 256:512]
            ref[s, 80:96, 0:128] = own_ref[s, 48:64, 128:256]
            ref[s, 80:96, 128:256] = own_ref[s, 48:64, 384:512]
    lane = lax.broadcasted_iota(jnp.int32, (GROUPS, 1, 128), 2)
    total = jnp.zeros((1, 128), F32)
    for n in range(2):
        lateral = dot(weight_ref[:, 0:IN_CH], fine_rows(own_ref, n, 0, COLS))
        total = total + local_stats(lateral, lane, 64 * n)
    stats_ref[...] = jnp.broadcast_to(total, stats_ref.shape)


def join_kernel(
    own_ref, one_ref, two_ref, lat_weight_ref, lat_stats_ref, joined_ref, beside_ref,
    above_ref, below_ref,
):
    odd = lax.axis_index("chan_0") % 2 == 1
    for s in range(8):
        one, two = one_ref[s], two_ref[s]
        above_ref[s] = jnp.where(odd, one, two)
        below_ref[s] = jnp.where(odd, two, one)
    core = lax.axis_index("band_2")
    band = (lax.axis_index("band_0") * 2 + lax.axis_index("band_1")) * 2 + core
    side = lax.axis_index("chan_1")
    pair = band * 4 + lax.axis_index("chan_0")
    at_top = pair == 0
    at_bottom = pair == 127
    source = lax.broadcasted_iota(jnp.int32, (128, HALF), 0)
    column = lanes_of((128, HALF))
    inner_edge = jnp.where(side == 0, HALF - 1, 0)
    near = column // 2
    far = jnp.clip(near - 1 + 2 * (column % 2), 0, 127)
    spread = (
        jnp.where(source == near, 0.75, 0.0)
        + jnp.where(jnp.logical_and(source == far, column != inner_edge), 0.25, 0.0)
    ).astype(BF16)
    gain = vector_col(lat_weight_ref, 0)
    shift = vector_col(lat_weight_ref, 1)
    stats = (lat_stats_ref[0:1], lat_stats_ref[1:2], lat_stats_ref[2:3])
    lane_at = lanes_of((D, HALF))
    small = lanes_of((D, 128))
    first_image = small < 4
    time = small % 4
    norm = [stat_cols(stats, n) for n in range(2)]
    norm = [(mean, lax.rsqrt(var + EPS) * gain) for mean, var in norm]
    lat_weight = lat_weight_ref[:, 0:IN_CH]

    def coarse_main(ref, low, high, n):
        at = 128 * n
        if high is None:
            pieces = [ref[s, low : low + 32, at : at + 128] for s in range(8)]
        else:
            pieces = []
            for s in range(8):
                pieces.append(ref[s, low : low + 16, at : at + 128])
                pieces.append(ref[s, low : low + 16, high + at : high + at + 128])
        return jnp.concatenate(pieces, axis=0)

    def extras(tile, move):
        fine = jnp.concatenate([tile[32 * s : 32 * s + 24] for s in range(8)], axis=0)
        fine = pltpu.roll(dot(lat_weight, fine), 128 - FINE_EDGE + move, axis=1)
        return fine, pltpu.roll(tile.astype(F32), 128 - COARSE_EDGE, axis=1)

    def tile_of(ref):
        pieces = []
        for s in range(8):
            pieces.append(ref[s, 80:96, 0:128])
            pieces.append(ref[s, 80:96, 128:256])
        return jnp.concatenate(pieces, axis=0)

    fine_above, extra_above = extras(tile_of(above_ref), -2)
    fine_own, extra_own = extras(lat_weight_ref[:, 128:256], 0)
    fine_below, extra_below = extras(tile_of(below_ref), 2)
    extra_above = jnp.where(at_top, extra_own, extra_above)
    extra_below = jnp.where(at_bottom, extra_own, extra_below)
    mains = []
    for n in range(2):
        middle = coarse_main(own_ref, 64, 256, n)
        upper = coarse_main(above_ref, 48, None, n)
        lower = coarse_main(below_ref, 48, None, n)
        upper = jnp.where(at_top, middle, upper)
        lower = jnp.where(at_bottom, middle, lower)
        mains.append((upper, middle, lower))
    edge_at = jnp.where(side == 0, 127, 0)
    ups, columns = [], []
    for k, extra in enumerate((extra_above, extra_own, extra_below)):
        edges = []
        for n in range(2):
            main = mains[n][k]
            edges.append(
                jnp.sum(jnp.where(small == edge_at, main.astype(F32), 0.0), axis=1, keepdims=True)
            )
        columns.append(0.75 * extra + 0.25 * jnp.where(first_image, edges[0], edges[1]))
        ups.append(
            [
                dot(mains[n][k], spread)
                + jnp.where(lane_at == inner_edge, 0.25 * extra[:, 4 * n : 4 * n + 1], 0.0)
                for n in range(2)
            ]
        )

    lateral = jnp.where(
        time == 0, fine_above, jnp.where(time == 3, fine_below, fine_own)
    )
    upsampled = jnp.where(
        time == 0,
        0.75 * columns[0] + 0.25 * columns[1],
        jnp.where(
            time == 1,
            0.25 * columns[0] + 0.75 * columns[1],
            jnp.where(
                time == 2,
                0.75 * columns[1] + 0.25 * columns[2],
                0.25 * columns[1] + 0.75 * columns[2],
            ),
        ),
    )
    mean = jnp.where(first_image, norm[0][0], norm[1][0])
    scale = jnp.where(first_image, norm[0][1], norm[1][1])
    value = (lateral - mean) * scale + shift + upsampled
    outside = jnp.logical_or(
        jnp.logical_and(time == 0, at_top), jnp.logical_and(time == 3, at_bottom)
    )
    value = jnp.where(outside, 0.0, value)
    beside_ref[...] = jnp.concatenate(
        [value, pltpu.roll(value, 127, axis=1), pltpu.roll(value, 126, axis=1)], axis=0
    ).astype(BF16)

    for n in range(2):
        mean, scale = norm[n]
        up = [ups[k][n] for k in range(3)]
        rows = (
            (fine_rows(above_ref, n, 0, HALF), 0.75 * up[0] + 0.25 * up[1]),
            (fine_rows(own_ref, n, 0, HALF), 0.25 * up[0] + 0.75 * up[1]),
            (fine_rows(own_ref, n, HALF, COLS), 0.75 * up[1] + 0.25 * up[2]),
            (fine_rows(below_ref, n, 0, HALF), 0.25 * up[1] + 0.75 * up[2]),
        )
        for t, (fine, upsampled) in enumerate(rows):
            value = ((dot(lat_weight, fine) - mean) * scale + shift + upsampled).astype(BF16)
            if t == 0:
                value = jnp.where(at_top, jnp.zeros_like(value), value)
            if t == 3:
                value = jnp.where(at_bottom, jnp.zeros_like(value), value)
            for r in range(2):
                if 0 <= t - r <= 2:
                    joined_ref[
                        n, 256 * (t - r) : 256 * (t - r) + 256, HALF * r : HALF * r + HALF
                    ] = value


def conv_kernel(
    joined_ref, beside_ref, mine_ref, other_ref, keep_ref, send_ref, stats_ref, weight, taps
):
    core = lax.axis_index("band_2")
    side = lax.axis_index("chan_1")
    for part, ref in ((core, mine_ref), (1 - core, other_ref)):
        for s in range(8):
            at = pl.multiple_of(32 * s + 16 * part, 16)
            for a in range(3):
                for b in range(3):
                    block = ref[s, 16 * (3 * a + b) : 16 * (3 * a + b) + 16, :]
                    weight[b, pl.ds(at, 16), 256 * a : 256 * a + 256] = block
    inner_edge = jnp.where(side == 0, HALF - 1, 0)
    lane = lax.broadcasted_iota(jnp.int32, (GROUPS, 1, 128), 2)
    lane_at = lanes_of((D, HALF))
    beside = dot(weight[jnp.where(side == 0, 2, 0)], beside_ref[...])
    total = jnp.zeros((1, 128), F32)
    for n in range(2):
        for b in range(3):
            taps[b] = dot(weight[b], joined_ref[n])
        out = []
        for r in range(2):
            at = HALF * r
            left = pltpu.roll(taps[0, :, at : at + HALF], 1, axis=1)
            right = pltpu.roll(taps[2, :, at : at + HALF], HALF - 1, axis=1)
            value = taps[1, :, at : at + HALF] + jnp.where(lane_at == 0, 0.0, left)
            value = value + jnp.where(lane_at == HALF - 1, 0.0, right)
            column = beside[:, 4 * n + r : 4 * n + r + 1]
            out.append(value + jnp.where(lane_at == inner_edge, column, 0.0))
        keep_ref[n] = jnp.where(side == 0, out[0], out[1])
        send_ref[n] = jnp.where(side == 0, out[1], out[0])
        total = total + local_stats(jnp.concatenate(out, axis=1), lane, 64 * n)
    stats_ref[...] = jnp.broadcast_to(total, stats_ref.shape)


def query_kernel(
    keep_ref, taken_ref, out_stats_ref, lat_weight_ref, mine_ref, other_ref,
    query_ref, out_ref, weight,
):
    core = lax.axis_index("band_2")
    side = lax.axis_index("chan_1")
    for part, ref in ((core, mine_ref), (1 - core, other_ref)):
        for s in range(8):
            at = pl.multiple_of(32 * s + 16 * part, 16)
            weight[pl.ds(at, 16), :] = ref[s, MASK_AT : MASK_AT + 16, :]
    gain = vector_col(lat_weight_ref, 2)
    shift = vector_col(lat_weight_ref, 3)
    bias = vector_col(lat_weight_ref, 4)
    rows = combine(out_stats_ref[...])
    for n in range(2):
        mean, var = stat_cols(rows, n)
        scale = lax.rsqrt(var + EPS) * gain
        for ref, half in ((keep_ref, side), (taken_ref, 1 - side)):
            activated = jnp.maximum((ref[n] - mean) * scale + shift, 0.0).astype(BF16)
            features = (dot(weight[...], activated) + bias).astype(BF16)
            logits = dot(query_ref[...], features)
            shifted = logits - jnp.max(logits, axis=0, keepdims=True)
            result = shifted - jnp.log(jnp.sum(jnp.exp(shifted), axis=0, keepdims=True))
            for t in range(2):
                at = 4 * QUERIES * n + 2 * half + t
                out_ref[pl.ds(at, QUERIES, stride=4), :] = result[:, 128 * t : 128 * t + 128]


def call(kernel, out_shape, scratch=(), flops=0, space=pltpu.VMEM, out_space=pltpu.VMEM, limit=40 << 20):
    out = pl.BlockSpec(memory_space=out_space)
    single = not isinstance(out_shape, (tuple, list))
    return lambda *args: pl.pallas_call(
        kernel,
        out_shape=out_shape,
        in_specs=[pl.BlockSpec(memory_space=space)] * len(args),
        out_specs=out if single else [out] * len(out_shape),
        scratch_shapes=list(scratch),
        cost_estimate=pl.CostEstimate(flops=flops, bytes_accessed=1 << 20, transcendentals=0),
        compiler_params=pltpu.CompilerParams(vmem_limit_bytes=limit),
    )(*args)


def per_device(
    fine_features,
    coarse_level,
    lat_weight,
    lat_gain,
    lat_shift,
    out_weight,
    out_gain,
    out_shift,
    mask_weight,
    mask_bias,
    queries,
):
    everyone = lax.axis_size(ALL)
    stats_shape = jax.ShapeDtypeStruct((everyone, 128), F32)
    quarter_shape = jax.ShapeDtypeStruct((8, 16 * BLOCKS, D), BF16)
    all_shape = jax.ShapeDtypeStruct((8, 32 * BLOCKS, D), BF16)
    side_shape = jax.ShapeDtypeStruct((8, SIDE_ROWS, HALF), BF16)
    half_shape = jax.ShapeDtypeStruct((2, D, HALF), F32)
    swap = [(0, 1), (1, 0)]

    vectors = [v.reshape(1, 32) for v in (lat_gain, lat_shift, out_gain, out_shift, mask_bias)]
    own_out = call(
        pack_own_kernel,
        pltpu.VMEM((8, OWN_ROWS, COLS), BF16),
        (
            pltpu.VMEM((2, 24, 8, COLS), BF16),
            pltpu.VMEM((2, 32, 4, 256), BF16),
            pltpu.VMEM((32, IN_CH), BF16),
            pltpu.VMEM((10, 32, D), BF16),
            pltpu.VMEM((5, 1, 32), BF16),
            pltpu.VMEM((4, 48 * 8 + 8, 128), F32),
            pltpu.VMEM((2, 2, 256 + 8, 128), F32),
            pltpu.SemaphoreType.DMA((10,)),
        ),
        space=pltpu.HBM,
        limit=60 << 20,
    )(fine_features, coarse_level, lat_weight, out_weight.reshape(9, 32, D), mask_weight, *vectors)
    own = lax.all_to_all(own_out, CHAN, 0, 0, tiled=True)
    full_lat, stats, first, second, quarter = call(
        lateral_kernel,
        [jax.ShapeDtypeStruct((D, 256), BF16), stats_shape, side_shape, side_shape, quarter_shape],
        flops=2 * 2 * 256 * 256 * 512,
    )(own)
    pairs = everyone // 2
    swap_at = lambda shift: [
        (2 * p + yl, 2 * ((((p + shift) % pairs ^ 1) - shift) % pairs) + yl)
        for p in range(pairs)
        for yl in range(2)
    ]
    first = lax.ppermute(first, ALL, swap_at(0))
    second = lax.ppermute(second, ALL, swap_at(1))
    depth = lax.axis_size("band_0")
    other_quarter = lax.ppermute(quarter, "band_0", [(i, i ^ 1) for i in range(depth)])
    stats = lax.all_to_all(stats, ALL, 0, 0, tiled=True)
    stats = call(combine_kernel, jax.ShapeDtypeStruct((8, 128), F32), flops=1 << 20)(stats)

    mine = call(arrange_kernel, all_shape)(quarter, other_quarter)
    other = lax.ppermute(mine, "band_2", swap)
    joined, beside = call(
        join_kernel,
        [jax.ShapeDtypeStruct((2, 3 * D, COLS), BF16), jax.ShapeDtypeStruct((3 * D, 128), BF16)],
        (
            pltpu.VMEM((8, SIDE_ROWS, HALF), BF16),
            pltpu.VMEM((8, SIDE_ROWS, HALF), BF16),
        ),
        flops=2 * 2 * 256 * 256 * 512 * 7,
    )(own, first, second, full_lat, stats)
    keep, send, stats = call(
        conv_kernel,
        [half_shape, half_shape, stats_shape],
        (pltpu.VMEM((3, D, 3 * D), BF16), pltpu.VMEM((3, D, COLS), F32)),
        flops=2 * 2 * 256 * 256 * 512 * 9,
    )(joined, beside, mine, other)
    taken = lax.ppermute(send, "chan_1", swap)
    stats = lax.all_to_all(stats, ALL, 0, 0, tiled=True)
    log_probs = call(
        query_kernel,
        jax.ShapeDtypeStruct((2 * QUERIES * 4, 128), F32),
        (pltpu.VMEM((D, D), BF16),),
        flops=2 * 2 * 256 * 256 * 512 * 2,
    )(keep, taken, stats, full_lat, mine, other, queries)
    return log_probs.reshape(2, QUERIES, 1, COLS)


def solution(mesh):
    finer = Mesh(
        mesh.devices.reshape(8, 2, 2, 4, 2), ("band_0", "band_1", "band_2", "chan_0", "chan_1")
    )

    return jax.shard_map(
        per_device,
        mesh=finer,
        in_specs=(
            P(None, CHAN, BAND, None),
            P(None, CHAN, BAND, None),
            P(CHAN, None),
            P(CHAN),
            P(CHAN),
            P(None, None, CHAN, None),
            P(CHAN),
            P(CHAN),
            P(CHAN, None),
            P(CHAN),
            P(),
        ),
        out_specs=P(None, None, BAND + CHAN, None),
        check_vma=False,
    )
```

```python
import jax
import jax.numpy as jnp
from jax import lax
from jax.experimental import pallas as pl
from jax.experimental.pallas import tpu as pltpu
from jax.sharding import Mesh
from jax.sharding import PartitionSpec as P


D = 256
GROUPS = 32
IN_CH = 192
COLS = 512
HALF = 256
QUERIES = 200
BAND = ("band_0", "band_1", "band_2")
CHAN = ("chan_0", "chan_1")
ALL = BAND + CHAN
EPS = 1e-05
F32 = jnp.float32
BF16 = jnp.bfloat16
OWN_ROWS = 80
VECTORS = 64
FINE_EDGE = 72
COARSE_EDGE = 80
SIDE_ROWS = 96
MASK_AT = 72
SHARD_ROWS = 80


def dot(a, b):
    return lax.dot_general(a, b, (((1,), (0,)), ((), ())), preferred_element_type=F32)


def local_stats(values, lane, offset):
    blocks = values.reshape(GROUPS, D // GROUPS, COLS)
    count = D // GROUPS * COLS
    mean = jnp.sum(jnp.sum(blocks, axis=2, keepdims=True), axis=1, keepdims=True) / count
    dev = blocks - mean
    m2 = jnp.sum(jnp.sum(dev * dev, axis=2, keepdims=True), axis=1, keepdims=True)
    group = lax.broadcasted_iota(jnp.int32, (GROUPS, 1, 128), 0)
    row = jnp.where(lane == group + offset, mean, 0.0)
    row = row + jnp.where(lane == group + (offset + GROUPS), m2, 0.0)
    return jnp.sum(row, axis=0)


def combine(stats):
    devices = stats.shape[0]
    count = D // GROUPS * COLS
    mean = jnp.sum(stats, axis=0, keepdims=True) / devices
    dev = stats - mean
    spread = jnp.sum(dev * dev, axis=0, keepdims=True) * (1.0 / devices)
    return mean, spread, mean * (1.0 / count)


def stat_cols(rows, image):
    mean, spread, inner = rows
    lane = lax.broadcasted_iota(jnp.int32, (D, 128), 1)
    group = lax.broadcasted_iota(jnp.int32, (D, 128), 0) // (D // GROUPS)
    at_mean = lane == group + image * 2 * GROUPS
    at_m2 = lane == group + (image * 2 + 1) * GROUPS
    mean_col = jnp.sum(jnp.where(at_mean, mean, 0.0), axis=1, keepdims=True)
    var_col = jnp.sum(
        jnp.where(at_mean, spread, 0.0) + jnp.where(at_m2, inner, 0.0), axis=1, keepdims=True
    )
    return mean_col, var_col


def combine_kernel(stats_ref, rows_ref):
    mean, spread, inner = combine(stats_ref[...])
    rows_ref[0:1] = mean
    rows_ref[1:2] = spread
    rows_ref[2:3] = inner
    rows_ref[3:8] = jnp.zeros((5, 128), F32)


def vector_col(lat_weight_ref, index):
    return lat_weight_ref[:, 128:256].astype(F32)[:, VECTORS + index : VECTORS + index + 1]


def lanes_of(shape):
    return lax.broadcasted_iota(jnp.int32, shape, len(shape) - 1)


def fine_rows(ref, image, low, high):
    return jnp.concatenate(
        [ref[s, 24 * image : 24 * image + 24, low:high] for s in range(8)], axis=0
    )


def pack_own_kernel(fine_hbm, coarse_hbm, weight_hbm, *refs):
    vec_hbm, own_refs = refs[:5], refs[5:13]
    fine_ref, coarse_ref, weight_ref, vec_ref, rows, coarse, sems = refs[13:]
    chan = lax.axis_index("chan_0") * 2 + lax.axis_index("chan_1")
    pairs = [(coarse_hbm, coarse_ref), (weight_hbm, weight_ref)]
    pairs += [(vec, vec_ref.at[i]) for i, vec in enumerate(vec_hbm)] + [(fine_hbm, fine_ref)]
    copies = [
        pltpu.make_async_copy(source, target, sems.at[i])
        for i, (source, target) in enumerate(pairs)
    ]
    for copy in copies:
        copy.start()
    for copy in copies[:-1]:
        copy.wait()
    for n in range(2):
        for t in range(2):
            piece = coarse_ref[n, :, :, 128 * t : 128 * t + 128].astype(F32)
            piece = jnp.concatenate([piece, jnp.zeros_like(piece)], axis=1)
            coarse[n, t, 0:256] = piece.reshape(256, 128)
    lane = lanes_of((32, 128))
    vec_lane = lanes_of((32, 32))
    vec_row = lax.broadcasted_iota(jnp.int32, (32, 32), 0)
    weight = weight_ref[...].astype(F32)
    second = jnp.concatenate([weight[:, 128:IN_CH], jnp.zeros((32, 256 - IN_CH), F32)], axis=1)
    for i in range(5):
        vec = jnp.where(vec_lane == vec_row, vec_ref[i].astype(F32), 0.0)
        second += jnp.where(lane == VECTORS + i, jnp.sum(vec, axis=1, keepdims=True), 0.0)
    first = weight[:, 0:128].astype(BF16)
    tails = []
    for k in range(8):
        own_ref = own_refs[k]
        q, h = (chan ^ k) // 2, (chan ^ k) % 2
        tail = second
        own_ref[48:64, 0:128] = first[0:16]
        own_ref[48:64, 256:384] = first[16:32]
        for n in range(2):
            row = coarse[n, h, pl.ds(q, 32, stride=8), :].astype(BF16)
            own_ref[64:80, 128 * n : 128 * n + 128] = row[0:16]
            own_ref[64:80, 256 + 128 * n : 384 + 128 * n] = row[16:32]
            row = coarse[n, 1 - h, pl.ds(q, 32, stride=8), :]
            edge = jnp.where(h == 0, row[:, 0:1], row[:, 127:128])
            tail = jnp.where(lane // 4 == COARSE_EDGE // 4 + n, edge, tail)
        tails.append(tail)
    copies[-1].wait()
    for t in range(4):
        piece = fine_ref[:, :, :, 128 * t : 128 * t + 128].astype(F32)
        rows[t, 0:384] = piece.reshape(48 * 8, 128)
    for k in range(8):
        own_ref = own_refs[k]
        q, h = (chan ^ k) // 2, (chan ^ k) % 2
        tail = tails[k]
        for r in range(2):
            for t in range(2):
                row = rows[2 * h + t, pl.ds(2 * q + r, 48, stride=8), :]
                at = 256 * r + 128 * t
                own_ref[0:48, at : at + 128] = row.astype(BF16)
            row = rows[2 - h, pl.ds(2 * q + r, 48, stride=8), :]
            edge = jnp.where(h == 0, row[:, 0:1], row[:, 127:128])
            for n in range(2):
                column = jnp.concatenate(
                    [edge[24 * n : 24 * n + 24], jnp.zeros((8, 1), F32)], axis=0
                )
                tail = jnp.where(lane == FINE_EDGE + 4 * n + 1 + r, column, tail)
        tail = tail.astype(BF16)
        own_ref[48:64, 128:256] = tail[0:16]
        own_ref[48:64, 384:512] = tail[16:32]


def pack_weights_kernel(conv_ref, mask_ref, shard_ref):
    half = pl.multiple_of(16 * lax.axis_index("band_2"), 16)
    for k in range(10):
        if k < 9:
            piece = conv_ref[k // 3, k % 3, pl.ds(half, 16), :].astype(F32)
        else:
            piece = mask_ref[pl.ds(half, 16), :].astype(F32)
        piece = jnp.concatenate([piece[0:8], piece[8:16]], axis=1).astype(BF16)
        shard_ref[8 * k : 8 * k + 8] = piece


def line_kernel(shard_ref, one_ref, two_ref, three_ref, line_ref):
    x = lax.axis_index("chan_0")
    for k, ref in enumerate((shard_ref, one_ref, two_ref, three_ref)):
        line_ref[x ^ k] = ref[...]


def arrange_kernel(line_ref, partner_ref, all_ref):
    side = lax.axis_index("chan_1")
    for x in range(4):
        all_ref[2 * x + side] = line_ref[x]
        all_ref[2 * x + 1 - side] = partner_ref[x]


def lateral_kernel(*refs):
    own_ref, weight_ref, stats_ref, one_ref, two_ref = refs[8:]
    chan = lax.axis_index("chan_0") * 2 + lax.axis_index("chan_1")
    for k in range(8):
        own_ref[chan ^ k] = refs[k][...]
    for s in range(8):
        for half in range(2):
            weight_ref[32 * s + 16 * half : 32 * s + 16 * half + 16, :] = own_ref[
                s, 48:64, 256 * half : 256 * half + 256
            ]
    odd = lax.axis_index("chan_0") % 2
    for ref, row in ((one_ref, 1 - odd), (two_ref, odd)):
        at = pl.multiple_of(256 * row, 256)
        for s in range(8):
            ref[s, 0:48, :] = own_ref[s, 0:48, pl.ds(at, 256)]
            ref[s, 48:64, :] = own_ref[s, 64:80, 0:256]
            ref[s, 64:80, :] = own_ref[s, 64:80, 256:512]
            ref[s, 80:96, 0:128] = own_ref[s, 48:64, 128:256]
            ref[s, 80:96, 128:256] = own_ref[s, 48:64, 384:512]
    lane = lax.broadcasted_iota(jnp.int32, (GROUPS, 1, 128), 2)
    total = jnp.zeros((1, 128), F32)
    for n in range(2):
        lateral = dot(weight_ref[:, 0:IN_CH], fine_rows(own_ref, n, 0, COLS))
        total = total + local_stats(lateral, lane, 64 * n)
    stats_ref[...] = jnp.broadcast_to(total, stats_ref.shape)


def join_kernel(
    own_ref, one_ref, two_ref, lat_weight_ref, lat_stats_ref, joined_ref, beside_ref,
    above_ref, below_ref,
):
    odd = lax.axis_index("chan_0") % 2 == 1
    for s in range(8):
        one, two = one_ref[s], two_ref[s]
        above_ref[s] = jnp.where(odd, one, two)
        below_ref[s] = jnp.where(odd, two, one)
    core = lax.axis_index("band_2")
    band = (lax.axis_index("band_0") * 2 + lax.axis_index("band_1")) * 2 + core
    side = lax.axis_index("chan_1")
    pair = band * 4 + lax.axis_index("chan_0")
    at_top = pair == 0
    at_bottom = pair == 127
    source = lax.broadcasted_iota(jnp.int32, (128, HALF), 0)
    column = lanes_of((128, HALF))
    inner_edge = jnp.where(side == 0, HALF - 1, 0)
    near = column // 2
    far = jnp.clip(near - 1 + 2 * (column % 2), 0, 127)
    spread = (
        jnp.where(source == near, 0.75, 0.0)
        + jnp.where(jnp.logical_and(source == far, column != inner_edge), 0.25, 0.0)
    ).astype(BF16)
    gain = vector_col(lat_weight_ref, 0)
    shift = vector_col(lat_weight_ref, 1)
    stats = (lat_stats_ref[0:1], lat_stats_ref[1:2], lat_stats_ref[2:3])
    lane_at = lanes_of((D, HALF))
    small = lanes_of((D, 128))
    first_image = small < 4
    time = small % 4
    norm = [stat_cols(stats, n) for n in range(2)]
    norm = [(mean, lax.rsqrt(var + EPS) * gain) for mean, var in norm]
    lat_weight = lat_weight_ref[:, 0:IN_CH]

    def coarse_main(ref, low, high, n):
        at = 128 * n
        if high is None:
            pieces = [ref[s, low : low + 32, at : at + 128] for s in range(8)]
        else:
            pieces = []
            for s in range(8):
                pieces.append(ref[s, low : low + 16, at : at + 128])
                pieces.append(ref[s, low : low + 16, high + at : high + at + 128])
        return jnp.concatenate(pieces, axis=0)

    def extras(tile, move):
        fine = jnp.concatenate([tile[32 * s : 32 * s + 24] for s in range(8)], axis=0)
        fine = pltpu.roll(dot(lat_weight, fine), 128 - FINE_EDGE + move, axis=1)
        return fine, pltpu.roll(tile.astype(F32), 128 - COARSE_EDGE, axis=1)

    def tile_of(ref):
        pieces = []
        for s in range(8):
            pieces.append(ref[s, 80:96, 0:128])
            pieces.append(ref[s, 80:96, 128:256])
        return jnp.concatenate(pieces, axis=0)

    fine_above, extra_above = extras(tile_of(above_ref), -2)
    fine_own, extra_own = extras(lat_weight_ref[:, 128:256], 0)
    fine_below, extra_below = extras(tile_of(below_ref), 2)
    extra_above = jnp.where(at_top, extra_own, extra_above)
    extra_below = jnp.where(at_bottom, extra_own, extra_below)
    mains = []
    for n in range(2):
        middle = coarse_main(own_ref, 64, 256, n)
        upper = coarse_main(above_ref, 48, None, n)
        lower = coarse_main(below_ref, 48, None, n)
        upper = jnp.where(at_top, middle, upper)
        lower = jnp.where(at_bottom, middle, lower)
        mains.append((upper, middle, lower))
    edge_at = jnp.where(side == 0, 127, 0)
    ups, columns = [], []
    for k, extra in enumerate((extra_above, extra_own, extra_below)):
        edges = []
        for n in range(2):
            main = mains[n][k]
            edges.append(
                jnp.sum(jnp.where(small == edge_at, main.astype(F32), 0.0), axis=1, keepdims=True)
            )
        columns.append(0.75 * extra + 0.25 * jnp.where(first_image, edges[0], edges[1]))
        ups.append(
            [
                dot(mains[n][k], spread)
                + jnp.where(lane_at == inner_edge, 0.25 * extra[:, 4 * n : 4 * n + 1], 0.0)
                for n in range(2)
            ]
        )

    lateral = jnp.where(
        time == 0, fine_above, jnp.where(time == 3, fine_below, fine_own)
    )
    upsampled = jnp.where(
        time == 0,
        0.75 * columns[0] + 0.25 * columns[1],
        jnp.where(
            time == 1,
            0.25 * columns[0] + 0.75 * columns[1],
            jnp.where(
                time == 2,
                0.75 * columns[1] + 0.25 * columns[2],
                0.25 * columns[1] + 0.75 * columns[2],
            ),
        ),
    )
    mean = jnp.where(first_image, norm[0][0], norm[1][0])
    scale = jnp.where(first_image, norm[0][1], norm[1][1])
    value = (lateral - mean) * scale + shift + upsampled
    outside = jnp.logical_or(
        jnp.logical_and(time == 0, at_top), jnp.logical_and(time == 3, at_bottom)
    )
    value = jnp.where(outside, 0.0, value)
    beside_ref[...] = jnp.concatenate(
        [value, pltpu.roll(value, 127, axis=1), pltpu.roll(value, 126, axis=1)], axis=0
    ).astype(BF16)

    for n in range(2):
        mean, scale = norm[n]
        up = [ups[k][n] for k in range(3)]
        rows = (
            (fine_rows(above_ref, n, 0, HALF), 0.75 * up[0] + 0.25 * up[1]),
            (fine_rows(own_ref, n, 0, HALF), 0.25 * up[0] + 0.75 * up[1]),
            (fine_rows(own_ref, n, HALF, COLS), 0.75 * up[1] + 0.25 * up[2]),
            (fine_rows(below_ref, n, 0, HALF), 0.25 * up[1] + 0.75 * up[2]),
        )
        for t, (fine, upsampled) in enumerate(rows):
            value = ((dot(lat_weight, fine) - mean) * scale + shift + upsampled).astype(BF16)
            if t == 0:
                value = jnp.where(at_top, jnp.zeros_like(value), value)
            if t == 3:
                value = jnp.where(at_bottom, jnp.zeros_like(value), value)
            for r in range(2):
                if 0 <= t - r <= 2:
                    joined_ref[
                        n, 256 * (t - r) : 256 * (t - r) + 256, HALF * r : HALF * r + HALF
                    ] = value


def conv_kernel(
    joined_ref, beside_ref, mine_ref, other_ref, keep_ref, send_ref, stats_ref, weight, taps
):
    core = lax.axis_index("band_2")
    side = lax.axis_index("chan_1")
    for part, ref in ((core, mine_ref), (1 - core, other_ref)):
        for s in range(8):
            at = pl.multiple_of(32 * s + 16 * part, 16)
            for a in range(3):
                for b in range(3):
                    piece = ref[s, (a * 3 + b) * 8 : (a * 3 + b) * 8 + 8, :]
                    both = jnp.concatenate([piece[:, 0:256], piece[:, 256:512]], axis=0)
                    weight[b, pl.ds(at, 16), 256 * a : 256 * a + 256] = both
    inner_edge = jnp.where(side == 0, HALF - 1, 0)
    lane = lax.broadcasted_iota(jnp.int32, (GROUPS, 1, 128), 2)
    lane_at = lanes_of((D, HALF))
    beside = dot(weight[jnp.where(side == 0, 2, 0)], beside_ref[...])
    total = jnp.zeros((1, 128), F32)
    for n in range(2):
        for b in range(3):
            taps[b] = dot(weight[b], joined_ref[n])
        out = []
        for r in range(2):
            at = HALF * r
            left = pltpu.roll(taps[0, :, at : at + HALF], 1, axis=1)
            right = pltpu.roll(taps[2, :, at : at + HALF], HALF - 1, axis=1)
            value = taps[1, :, at : at + HALF] + jnp.where(lane_at == 0, 0.0, left)
            value = value + jnp.where(lane_at == HALF - 1, 0.0, right)
            column = beside[:, 4 * n + r : 4 * n + r + 1]
            out.append(value + jnp.where(lane_at == inner_edge, column, 0.0))
        keep_ref[n] = jnp.where(side == 0, out[0], out[1])
        send_ref[n] = jnp.where(side == 0, out[1], out[0])
        total = total + local_stats(jnp.concatenate(out, axis=1), lane, 64 * n)
    stats_ref[...] = jnp.broadcast_to(total, stats_ref.shape)


def query_kernel(
    keep_ref, taken_ref, out_stats_ref, lat_weight_ref, mine_ref, other_ref,
    query_ref, out_ref, weight,
):
    core = lax.axis_index("band_2")
    side = lax.axis_index("chan_1")
    for part, ref in ((core, mine_ref), (1 - core, other_ref)):
        for s in range(8):
            at = pl.multiple_of(32 * s + 16 * part, 16)
            piece = ref[s, MASK_AT : MASK_AT + 8, :]
            both = jnp.concatenate([piece[:, 0:256], piece[:, 256:512]], axis=0)
            weight[pl.ds(at, 16), :] = both
    gain = vector_col(lat_weight_ref, 2)
    shift = vector_col(lat_weight_ref, 3)
    bias = vector_col(lat_weight_ref, 4)
    rows = combine(out_stats_ref[...])
    for n in range(2):
        mean, var = stat_cols(rows, n)
        scale = lax.rsqrt(var + EPS) * gain
        for ref, half in ((keep_ref, side), (taken_ref, 1 - side)):
            activated = jnp.maximum((ref[n] - mean) * scale + shift, 0.0).astype(BF16)
            features = (dot(weight[...], activated) + bias).astype(BF16)
            logits = dot(query_ref[...], features)
            shifted = logits - jnp.max(logits, axis=0, keepdims=True)
            result = shifted - jnp.log(jnp.sum(jnp.exp(shifted), axis=0, keepdims=True))
            for t in range(2):
                at = 4 * QUERIES * n + 2 * half + t
                out_ref[pl.ds(at, QUERIES, stride=4), :] = result[:, 128 * t : 128 * t + 128]


def call(kernel, out_shape, scratch=(), flops=0, space=pltpu.VMEM, out_space=pltpu.VMEM, limit=40 << 20):
    out = pl.BlockSpec(memory_space=out_space)
    single = not isinstance(out_shape, (tuple, list))
    return lambda *args: pl.pallas_call(
        kernel,
        out_shape=out_shape,
        in_specs=[pl.BlockSpec(memory_space=space)] * len(args),
        out_specs=out if single else [out] * len(out_shape),
        scratch_shapes=list(scratch),
        cost_estimate=pl.CostEstimate(flops=flops, bytes_accessed=1 << 20, transcendentals=0),
        compiler_params=pltpu.CompilerParams(vmem_limit_bytes=limit),
    )(*args)


def per_device(
    fine_features,
    coarse_level,
    lat_weight,
    lat_gain,
    lat_shift,
    out_weight,
    out_gain,
    out_shift,
    mask_weight,
    mask_bias,
    queries,
):
    everyone = lax.axis_size(ALL)
    stats_shape = jax.ShapeDtypeStruct((everyone, 128), F32)
    shard_shape = jax.ShapeDtypeStruct((SHARD_ROWS, COLS), BF16)
    all_shape = jax.ShapeDtypeStruct((8, SHARD_ROWS, COLS), BF16)
    side_shape = jax.ShapeDtypeStruct((8, SIDE_ROWS, HALF), BF16)
    half_shape = jax.ShapeDtypeStruct((2, D, HALF), F32)
    own_shape = jax.ShapeDtypeStruct((8, OWN_ROWS, COLS), BF16)
    swap = [(0, 1), (1, 0)]

    vectors = [v.reshape(1, 32) for v in (lat_gain, lat_shift, out_gain, out_shift, mask_bias)]
    blocks = call(
        pack_own_kernel,
        [pltpu.VMEM((OWN_ROWS, COLS), BF16)] * 8,
        (
            pltpu.VMEM((2, 24, 8, COLS), BF16),
            pltpu.VMEM((2, 32, 4, 256), BF16),
            pltpu.VMEM((32, IN_CH), BF16),
            pltpu.VMEM((5, 1, 32), BF16),
            pltpu.VMEM((4, 48 * 8 + 8, 128), F32),
            pltpu.VMEM((2, 2, 256 + 8, 128), F32),
            pltpu.SemaphoreType.DMA((8,)),
        ),
        space=pltpu.HBM,
        limit=60 << 20,
    )(fine_features, coarse_level, lat_weight, *vectors)
    taken_in = [blocks[0]] + [
        lax.ppermute(blocks[k], CHAN, [(i, i ^ k) for i in range(8)]) for k in range(1, 8)
    ]
    shard = call(pack_weights_kernel, shard_shape)(out_weight, mask_weight)
    moved = [
        lax.ppermute(shard, "chan_0", [(i, i ^ k) for i in range(4)]) for k in (1, 2, 3)
    ]

    own, full_lat, stats, first, second = call(
        lateral_kernel,
        [own_shape, jax.ShapeDtypeStruct((D, 256), BF16), stats_shape, side_shape, side_shape],
        flops=2 * 2 * 256 * 256 * 512,
    )(*taken_in)
    pairs = everyone // 2
    swap_at = lambda shift: [
        (2 * p + yl, 2 * ((((p + shift) % pairs ^ 1) - shift) % pairs) + yl)
        for p in range(pairs)
        for yl in range(2)
    ]
    first = lax.ppermute(first, ALL, swap_at(0))
    second = lax.ppermute(second, ALL, swap_at(1))
    line = call(line_kernel, jax.ShapeDtypeStruct((4, SHARD_ROWS, COLS), BF16))(shard, *moved)
    partner = lax.ppermute(line, "chan_1", swap)
    stats = lax.all_to_all(stats, ALL, 0, 0, tiled=True)
    stats = call(combine_kernel, jax.ShapeDtypeStruct((8, 128), F32), flops=1 << 20)(stats)

    mine = call(arrange_kernel, all_shape)(line, partner)
    other = lax.ppermute(mine, "band_2", swap)
    joined, beside = call(
        join_kernel,
        [jax.ShapeDtypeStruct((2, 3 * D, COLS), BF16), jax.ShapeDtypeStruct((3 * D, 128), BF16)],
        (
            pltpu.VMEM((8, SIDE_ROWS, HALF), BF16),
            pltpu.VMEM((8, SIDE_ROWS, HALF), BF16),
        ),
        flops=2 * 2 * 256 * 256 * 512 * 7,
    )(own, first, second, full_lat, stats)
    keep, send, stats = call(
        conv_kernel,
        [half_shape, half_shape, stats_shape],
        (pltpu.VMEM((3, D, 3 * D), BF16), pltpu.VMEM((3, D, COLS), F32)),
        flops=2 * 2 * 256 * 256 * 512 * 9,
    )(joined, beside, mine, other)
    taken = lax.ppermute(send, "chan_1", swap)
    stats = lax.all_to_all(stats, ALL, 0, 0, tiled=True)
    log_probs = call(
        query_kernel,
        jax.ShapeDtypeStruct((2 * QUERIES * 4, 128), F32),
        (pltpu.VMEM((D, D), BF16),),
        flops=2 * 2 * 256 * 256 * 512 * 2,
    )(keep, taken, stats, full_lat, mine, other, queries)
    return log_probs.reshape(2, QUERIES, 1, COLS)


def solution(mesh):
    finer = Mesh(
        mesh.devices.reshape(8, 2, 2, 4, 2), ("band_0", "band_1", "band_2", "chan_0", "chan_1")
    )

    return jax.shard_map(
        per_device,
        mesh=finer,
        in_specs=(
            P(None, CHAN, BAND, None),
            P(None, CHAN, BAND, None),
            P(CHAN, None),
            P(CHAN),
            P(CHAN),
            P(None, None, CHAN, None),
            P(CHAN),
            P(CHAN),
            P(CHAN, None),
            P(CHAN),
            P(),
        ),
        out_specs=P(None, None, BAND + CHAN, None),
        check_vma=False,
    )
```

```python
import jax
import jax.numpy as jnp
from jax import lax
from jax.experimental import pallas as pl
from jax.experimental.pallas import tpu as pltpu
from jax.sharding import Mesh
from jax.sharding import PartitionSpec as P


D = 256
GROUPS = 32
IN_CH = 192
COLS = 512
HALF = 256
QUERIES = 200
BAND = ("band_0", "band_1", "band_2")
CHAN = ("chan_0", "chan_1")
ALL = BAND + CHAN
EPS = 1e-05
F32 = jnp.float32
BF16 = jnp.bfloat16
OWN_ROWS = 120
VECTORS = 64
FINE_EDGE = 72
COARSE_EDGE = 80
SIDE_ROWS = 96
BLOCKS = 5
MASK_AT = 144


def dot(a, b):
    return lax.dot_general(a, b, (((1,), (0,)), ((), ())), preferred_element_type=F32)


def local_stats(values, lane, offset):
    blocks = values.reshape(GROUPS, D // GROUPS, COLS)
    count = D // GROUPS * COLS
    mean = jnp.sum(jnp.sum(blocks, axis=2, keepdims=True), axis=1, keepdims=True) / count
    dev = blocks - mean
    m2 = jnp.sum(jnp.sum(dev * dev, axis=2, keepdims=True), axis=1, keepdims=True)
    group = lax.broadcasted_iota(jnp.int32, (GROUPS, 1, 128), 0)
    row = jnp.where(lane == group + offset, mean, 0.0)
    row = row + jnp.where(lane == group + (offset + GROUPS), m2, 0.0)
    return jnp.sum(row, axis=0)


def combine(stats):
    devices = stats.shape[0]
    count = D // GROUPS * COLS
    mean = jnp.sum(stats, axis=0, keepdims=True) / devices
    dev = stats - mean
    spread = jnp.sum(dev * dev, axis=0, keepdims=True) * (1.0 / devices)
    return mean, spread, mean * (1.0 / count)


def stat_cols(rows, image):
    mean, spread, inner = rows
    lane = lax.broadcasted_iota(jnp.int32, (D, 128), 1)
    group = lax.broadcasted_iota(jnp.int32, (D, 128), 0) // (D // GROUPS)
    at_mean = lane == group + image * 2 * GROUPS
    at_m2 = lane == group + (image * 2 + 1) * GROUPS
    mean_col = jnp.sum(jnp.where(at_mean, mean, 0.0), axis=1, keepdims=True)
    var_col = jnp.sum(
        jnp.where(at_mean, spread, 0.0) + jnp.where(at_m2, inner, 0.0), axis=1, keepdims=True
    )
    return mean_col, var_col


def combine_kernel(stats_ref, rows_ref):
    mean, spread, inner = combine(stats_ref[...])
    rows_ref[0:1] = mean
    rows_ref[1:2] = spread
    rows_ref[2:3] = inner
    rows_ref[3:8] = jnp.zeros((5, 128), F32)


def vector_col(lat_weight_ref, index):
    return lat_weight_ref[:, 128:256].astype(F32)[:, VECTORS + index : VECTORS + index + 1]


def lanes_of(shape):
    return lax.broadcasted_iota(jnp.int32, shape, len(shape) - 1)


def fine_rows(ref, image, low, high):
    return jnp.concatenate(
        [ref[s, 24 * image : 24 * image + 24, low:high] for s in range(8)], axis=0
    )


def pack_own_kernel(fine_hbm, coarse_hbm, weight_hbm, conv_hbm, mask_hbm, *refs):
    vec_hbm, own_refs = refs[:5], refs[5:13]
    fine_ref, coarse_ref, weight_ref, conv_ref, vec_ref, rows, coarse, sems = refs[13:]
    chan = lax.axis_index("chan_0") * 2 + lax.axis_index("chan_1")
    pairs = [(coarse_hbm, coarse_ref), (weight_hbm, weight_ref)]
    pairs += [(vec, vec_ref.at[i]) for i, vec in enumerate(vec_hbm)]
    pairs += [(conv_hbm, conv_ref.at[pl.ds(0, 9)]), (mask_hbm, conv_ref.at[9]), (fine_hbm, fine_ref)]
    copies = [
        pltpu.make_async_copy(source, target, sems.at[i])
        for i, (source, target) in enumerate(pairs)
    ]
    for copy in copies:
        copy.start()
    for copy in copies[:-1]:
        copy.wait()
    for n in range(2):
        for t in range(2):
            piece = coarse_ref[n, :, :, 128 * t : 128 * t + 128].astype(F32)
            piece = jnp.concatenate([piece, jnp.zeros_like(piece)], axis=1)
            coarse[n, t, 0:256] = piece.reshape(256, 128)
    lane = lanes_of((32, 128))
    vec_lane = lanes_of((32, 32))
    vec_row = lax.broadcasted_iota(jnp.int32, (32, 32), 0)
    weight = weight_ref[...].astype(F32)
    second = jnp.concatenate([weight[:, 128:IN_CH], jnp.zeros((32, 256 - IN_CH), F32)], axis=1)
    for i in range(5):
        vec = jnp.where(vec_lane == vec_row, vec_ref[i].astype(F32), 0.0)
        second += jnp.where(lane == VECTORS + i, jnp.sum(vec, axis=1, keepdims=True), 0.0)
    first = weight[:, 0:128].astype(BF16)
    half = pl.multiple_of(16 * lax.axis_index("band_2"), 16)
    block = BLOCKS * (lax.axis_index("band_0") % 2)
    blocks = [conv_ref[block + i, pl.ds(half, 16), :] for i in range(BLOCKS)]
    last = blocks[4].astype(F32)
    last = jnp.concatenate([last[0:8], last[8:16]], axis=1).astype(BF16)
    tails = []
    for k in range(8):
        own_ref = own_refs[k]
        q, h = (chan ^ k) // 2, (chan ^ k) % 2
        tail = second
        own_ref[48:64, 0:128] = first[0:16]
        own_ref[48:64, 256:384] = first[16:32]
        for i in range(4):
            at = 80 + 16 * (i // 2)
            own_ref[at : at + 16, 256 * (i % 2) : 256 * (i % 2) + 256] = blocks[i]
        own_ref[112:120, :] = last
        for n in range(2):
            row = coarse[n, h, pl.ds(q, 32, stride=8), :].astype(BF16)
            own_ref[64:80, 128 * n : 128 * n + 128] = row[0:16]
            own_ref[64:80, 256 + 128 * n : 384 + 128 * n] = row[16:32]
            row = coarse[n, 1 - h, pl.ds(q, 32, stride=8), :]
            edge = jnp.where(h == 0, row[:, 0:1], row[:, 127:128])
            tail = jnp.where(lane // 4 == COARSE_EDGE // 4 + n, edge, tail)
        tails.append(tail)
    copies[-1].wait()
    for t in range(4):
        piece = fine_ref[:, :, :, 128 * t : 128 * t + 128].astype(F32)
        rows[t, 0:384] = piece.reshape(48 * 8, 128)
    for k in range(8):
        own_ref = own_refs[k]
        q, h = (chan ^ k) // 2, (chan ^ k) % 2
        tail = tails[k]
        for r in range(2):
            for t in range(2):
                row = rows[2 * h + t, pl.ds(2 * q + r, 48, stride=8), :]
                at = 256 * r + 128 * t
                own_ref[0:48, at : at + 128] = row.astype(BF16)
            row = rows[2 - h, pl.ds(2 * q + r, 48, stride=8), :]
            edge = jnp.where(h == 0, row[:, 0:1], row[:, 127:128])
            for n in range(2):
                column = jnp.concatenate(
                    [edge[24 * n : 24 * n + 24], jnp.zeros((8, 1), F32)], axis=0
                )
                tail = jnp.where(lane == FINE_EDGE + 4 * n + 1 + r, column, tail)
        tail = tail.astype(BF16)
        own_ref[48:64, 128:256] = tail[0:16]
        own_ref[48:64, 384:512] = tail[16:32]


def arrange_kernel(quarter_ref, other_ref, all_ref):
    parity = lax.axis_index("band_0") % 2
    rows = 16 * BLOCKS
    all_ref[:, pl.ds(pl.multiple_of(rows * parity, 16), rows), :] = quarter_ref[...]
    all_ref[:, pl.ds(pl.multiple_of(rows - rows * parity, 16), rows), :] = other_ref[...]


def lateral_kernel(*refs):
    own_ref, weight_ref, stats_ref, one_ref, two_ref, quarter_ref = refs[8:]
    chan = lax.axis_index("chan_0") * 2 + lax.axis_index("chan_1")
    for k in range(8):
        own_ref[chan ^ k] = refs[k][...]
    for s in range(8):
        for half in range(2):
            weight_ref[32 * s + 16 * half : 32 * s + 16 * half + 16, :] = own_ref[
                s, 48:64, 256 * half : 256 * half + 256
            ]
    for s in range(8):
        for i in range(4):
            at = 80 + 16 * (i // 2)
            quarter_ref[s, 16 * i : 16 * i + 16] = own_ref[
                s, at : at + 16, 256 * (i % 2) : 256 * (i % 2) + 256
            ]
        last = own_ref[s, 112:120, :]
        quarter_ref[s, 64:80] = jnp.concatenate([last[:, 0:256], last[:, 256:512]], axis=0)
    odd = lax.axis_index("chan_0") % 2
    for ref, row in ((one_ref, 1 - odd), (two_ref, odd)):
        at = pl.multiple_of(256 * row, 256)
        for s in range(8):
            ref[s, 0:48, :] = own_ref[s, 0:48, pl.ds(at, 256)]
            ref[s, 48:64, :] = own_ref[s, 64:80, 0:256]
            ref[s, 64:80, :] = own_ref[s, 64:80, 256:512]
            ref[s, 80:96, 0:128] = own_ref[s, 48:64, 128:256]
            ref[s, 80:96, 128:256] = own_ref[s, 48:64, 384:512]
    lane = lax.broadcasted_iota(jnp.int32, (GROUPS, 1, 128), 2)
    total = jnp.zeros((1, 128), F32)
    for n in range(2):
        lateral = dot(weight_ref[:, 0:IN_CH], fine_rows(own_ref, n, 0, COLS))
        total = total + local_stats(lateral, lane, 64 * n)
    stats_ref[...] = jnp.broadcast_to(total, stats_ref.shape)


def join_kernel(
    own_ref, one_ref, two_ref, lat_weight_ref, lat_stats_ref, joined_ref, beside_ref,
    above_ref, below_ref,
):
    odd = lax.axis_index("chan_0") % 2 == 1
    for s in range(8):
        one, two = one_ref[s], two_ref[s]
        above_ref[s] = jnp.where(odd, one, two)
        below_ref[s] = jnp.where(odd, two, one)
    core = lax.axis_index("band_2")
    band = (lax.axis_index("band_0") * 2 + lax.axis_index("band_1")) * 2 + core
    side = lax.axis_index("chan_1")
    pair = band * 4 + lax.axis_index("chan_0")
    at_top = pair == 0
    at_bottom = pair == 127
    source = lax.broadcasted_iota(jnp.int32, (128, HALF), 0)
    column = lanes_of((128, HALF))
    inner_edge = jnp.where(side == 0, HALF - 1, 0)
    near = column // 2
    far = jnp.clip(near - 1 + 2 * (column % 2), 0, 127)
    spread = (
        jnp.where(source == near, 0.75, 0.0)
        + jnp.where(jnp.logical_and(source == far, column != inner_edge), 0.25, 0.0)
    ).astype(BF16)
    gain = vector_col(lat_weight_ref, 0)
    shift = vector_col(lat_weight_ref, 1)
    stats = (lat_stats_ref[0:1], lat_stats_ref[1:2], lat_stats_ref[2:3])
    lane_at = lanes_of((D, HALF))
    small = lanes_of((D, 128))
    first_image = small < 4
    time = small % 4
    norm = [stat_cols(stats, n) for n in range(2)]
    norm = [(mean, lax.rsqrt(var + EPS) * gain) for mean, var in norm]
    lat_weight = lat_weight_ref[:, 0:IN_CH]

    def coarse_main(ref, low, high, n):
        at = 128 * n
        if high is None:
            pieces = [ref[s, low : low + 32, at : at + 128] for s in range(8)]
        else:
            pieces = []
            for s in range(8):
                pieces.append(ref[s, low : low + 16, at : at + 128])
                pieces.append(ref[s, low : low + 16, high + at : high + at + 128])
        return jnp.concatenate(pieces, axis=0)

    def extras(tile, move):
        fine = jnp.concatenate([tile[32 * s : 32 * s + 24] for s in range(8)], axis=0)
        fine = pltpu.roll(dot(lat_weight, fine), 128 - FINE_EDGE + move, axis=1)
        return fine, pltpu.roll(tile.astype(F32), 128 - COARSE_EDGE, axis=1)

    def tile_of(ref):
        pieces = []
        for s in range(8):
            pieces.append(ref[s, 80:96, 0:128])
            pieces.append(ref[s, 80:96, 128:256])
        return jnp.concatenate(pieces, axis=0)

    fine_above, extra_above = extras(tile_of(above_ref), -2)
    fine_own, extra_own = extras(lat_weight_ref[:, 128:256], 0)
    fine_below, extra_below = extras(tile_of(below_ref), 2)
    extra_above = jnp.where(at_top, extra_own, extra_above)
    extra_below = jnp.where(at_bottom, extra_own, extra_below)
    mains = []
    for n in range(2):
        middle = coarse_main(own_ref, 64, 256, n)
        upper = coarse_main(above_ref, 48, None, n)
        lower = coarse_main(below_ref, 48, None, n)
        upper = jnp.where(at_top, middle, upper)
        lower = jnp.where(at_bottom, middle, lower)
        mains.append((upper, middle, lower))
    edge_at = jnp.where(side == 0, 127, 0)
    ups, columns = [], []
    for k, extra in enumerate((extra_above, extra_own, extra_below)):
        edges = []
        for n in range(2):
            main = mains[n][k]
            edges.append(
                jnp.sum(jnp.where(small == edge_at, main.astype(F32), 0.0), axis=1, keepdims=True)
            )
        columns.append(0.75 * extra + 0.25 * jnp.where(first_image, edges[0], edges[1]))
        ups.append(
            [
                dot(mains[n][k], spread)
                + jnp.where(lane_at == inner_edge, 0.25 * extra[:, 4 * n : 4 * n + 1], 0.0)
                for n in range(2)
            ]
        )

    lateral = jnp.where(
        time == 0, fine_above, jnp.where(time == 3, fine_below, fine_own)
    )
    upsampled = jnp.where(
        time == 0,
        0.75 * columns[0] + 0.25 * columns[1],
        jnp.where(
            time == 1,
            0.25 * columns[0] + 0.75 * columns[1],
            jnp.where(
                time == 2,
                0.75 * columns[1] + 0.25 * columns[2],
                0.25 * columns[1] + 0.75 * columns[2],
            ),
        ),
    )
    mean = jnp.where(first_image, norm[0][0], norm[1][0])
    scale = jnp.where(first_image, norm[0][1], norm[1][1])
    value = (lateral - mean) * scale + shift + upsampled
    outside = jnp.logical_or(
        jnp.logical_and(time == 0, at_top), jnp.logical_and(time == 3, at_bottom)
    )
    value = jnp.where(outside, 0.0, value)
    beside_ref[...] = jnp.concatenate(
        [value, pltpu.roll(value, 127, axis=1), pltpu.roll(value, 126, axis=1)], axis=0
    ).astype(BF16)

    for n in range(2):
        mean, scale = norm[n]
        up = [ups[k][n] for k in range(3)]
        rows = (
            (fine_rows(above_ref, n, 0, HALF), 0.75 * up[0] + 0.25 * up[1]),
            (fine_rows(own_ref, n, 0, HALF), 0.25 * up[0] + 0.75 * up[1]),
            (fine_rows(own_ref, n, HALF, COLS), 0.75 * up[1] + 0.25 * up[2]),
            (fine_rows(below_ref, n, 0, HALF), 0.25 * up[1] + 0.75 * up[2]),
        )
        for t, (fine, upsampled) in enumerate(rows):
            value = ((dot(lat_weight, fine) - mean) * scale + shift + upsampled).astype(BF16)
            if t == 0:
                value = jnp.where(at_top, jnp.zeros_like(value), value)
            if t == 3:
                value = jnp.where(at_bottom, jnp.zeros_like(value), value)
            for r in range(2):
                if 0 <= t - r <= 2:
                    joined_ref[
                        n, 256 * (t - r) : 256 * (t - r) + 256, HALF * r : HALF * r + HALF
                    ] = value


def conv_kernel(
    joined_ref, beside_ref, mine_ref, other_ref, keep_ref, send_ref, stats_ref, weight, taps
):
    core = lax.axis_index("band_2")
    side = lax.axis_index("chan_1")
    for part, ref in ((core, mine_ref), (1 - core, other_ref)):
        for s in range(8):
            at = pl.multiple_of(32 * s + 16 * part, 16)
            for a in range(3):
                for b in range(3):
                    block = ref[s, 16 * (3 * a + b) : 16 * (3 * a + b) + 16, :]
                    weight[b, pl.ds(at, 16), 256 * a : 256 * a + 256] = block
    inner_edge = jnp.where(side == 0, HALF - 1, 0)
    lane = lax.broadcasted_iota(jnp.int32, (GROUPS, 1, 128), 2)
    lane_at = lanes_of((D, HALF))
    beside = dot(weight[jnp.where(side == 0, 2, 0)], beside_ref[...])
    total = jnp.zeros((1, 128), F32)
    for n in range(2):
        for b in range(3):
            taps[b] = dot(weight[b], joined_ref[n])
        out = []
        for r in range(2):
            at = HALF * r
            left = pltpu.roll(taps[0, :, at : at + HALF], 1, axis=1)
            right = pltpu.roll(taps[2, :, at : at + HALF], HALF - 1, axis=1)
            value = taps[1, :, at : at + HALF] + jnp.where(lane_at == 0, 0.0, left)
            value = value + jnp.where(lane_at == HALF - 1, 0.0, right)
            column = beside[:, 4 * n + r : 4 * n + r + 1]
            out.append(value + jnp.where(lane_at == inner_edge, column, 0.0))
        keep_ref[n] = jnp.where(side == 0, out[0], out[1])
        send_ref[n] = jnp.where(side == 0, out[1], out[0])
        total = total + local_stats(jnp.concatenate(out, axis=1), lane, 64 * n)
    stats_ref[...] = jnp.broadcast_to(total, stats_ref.shape)


def query_kernel(
    keep_ref, taken_ref, out_stats_ref, lat_weight_ref, mine_ref, other_ref,
    query_ref, out_ref, weight,
):
    core = lax.axis_index("band_2")
    side = lax.axis_index("chan_1")
    for part, ref in ((core, mine_ref), (1 - core, other_ref)):
        for s in range(8):
            at = pl.multiple_of(32 * s + 16 * part, 16)
            weight[pl.ds(at, 16), :] = ref[s, MASK_AT : MASK_AT + 16, :]
    gain = vector_col(lat_weight_ref, 2)
    shift = vector_col(lat_weight_ref, 3)
    bias = vector_col(lat_weight_ref, 4)
    rows = combine(out_stats_ref[...])
    for n in range(2):
        mean, var = stat_cols(rows, n)
        scale = lax.rsqrt(var + EPS) * gain
        for ref, half in ((keep_ref, side), (taken_ref, 1 - side)):
            activated = jnp.maximum((ref[n] - mean) * scale + shift, 0.0).astype(BF16)
            features = (dot(weight[...], activated) + bias).astype(BF16)
            logits = dot(query_ref[...], features)
            shifted = logits - jnp.max(logits, axis=0, keepdims=True)
            result = shifted - jnp.log(jnp.sum(jnp.exp(shifted), axis=0, keepdims=True))
            for t in range(2):
                at = 4 * QUERIES * n + 2 * half + t
                out_ref[pl.ds(at, QUERIES, stride=4), :] = result[:, 128 * t : 128 * t + 128]


def call(kernel, out_shape, scratch=(), flops=0, space=pltpu.VMEM, out_space=pltpu.VMEM, limit=40 << 20):
    out = pl.BlockSpec(memory_space=out_space)
    single = not isinstance(out_shape, (tuple, list))
    return lambda *args: pl.pallas_call(
        kernel,
        out_shape=out_shape,
        in_specs=[pl.BlockSpec(memory_space=space)] * len(args),
        out_specs=out if single else [out] * len(out_shape),
        scratch_shapes=list(scratch),
        cost_estimate=pl.CostEstimate(flops=flops, bytes_accessed=1 << 20, transcendentals=0),
        compiler_params=pltpu.CompilerParams(vmem_limit_bytes=limit),
    )(*args)


def per_device(
    fine_features,
    coarse_level,
    lat_weight,
    lat_gain,
    lat_shift,
    out_weight,
    out_gain,
    out_shift,
    mask_weight,
    mask_bias,
    queries,
):
    everyone = lax.axis_size(ALL)
    stats_shape = jax.ShapeDtypeStruct((everyone, 128), F32)
    quarter_shape = jax.ShapeDtypeStruct((8, 16 * BLOCKS, D), BF16)
    all_shape = jax.ShapeDtypeStruct((8, 32 * BLOCKS, D), BF16)
    side_shape = jax.ShapeDtypeStruct((8, SIDE_ROWS, HALF), BF16)
    half_shape = jax.ShapeDtypeStruct((2, D, HALF), F32)
    own_shape = jax.ShapeDtypeStruct((8, OWN_ROWS, COLS), BF16)
    swap = [(0, 1), (1, 0)]

    vectors = [v.reshape(1, 32) for v in (lat_gain, lat_shift, out_gain, out_shift, mask_bias)]
    blocks = call(
        pack_own_kernel,
        [pltpu.VMEM((OWN_ROWS, COLS), BF16)] * 8,
        (
            pltpu.VMEM((2, 24, 8, COLS), BF16),
            pltpu.VMEM((2, 32, 4, 256), BF16),
            pltpu.VMEM((32, IN_CH), BF16),
            pltpu.VMEM((10, 32, D), BF16),
            pltpu.VMEM((5, 1, 32), BF16),
            pltpu.VMEM((4, 48 * 8 + 8, 128), F32),
            pltpu.VMEM((2, 2, 256 + 8, 128), F32),
            pltpu.SemaphoreType.DMA((10,)),
        ),
        space=pltpu.HBM,
        limit=60 << 20,
    )(
        fine_features, coarse_level, lat_weight, out_weight.reshape(9, 32, D), mask_weight, *vectors
    )
    taken_in = [blocks[0]] + [
        lax.ppermute(blocks[k], CHAN, [(i, i ^ k) for i in range(8)]) for k in range(1, 8)
    ]

    own, full_lat, stats, first, second, quarter = call(
        lateral_kernel,
        [
            own_shape, jax.ShapeDtypeStruct((D, 256), BF16), stats_shape,
            side_shape, side_shape, quarter_shape,
        ],
        flops=2 * 2 * 256 * 256 * 512,
    )(*taken_in)
    pairs = everyone // 2
    swap_at = lambda shift: [
        (2 * p + yl, 2 * ((((p + shift) % pairs ^ 1) - shift) % pairs) + yl)
        for p in range(pairs)
        for yl in range(2)
    ]
    first = lax.ppermute(first, ALL, swap_at(0))
    second = lax.ppermute(second, ALL, swap_at(1))
    depth = lax.axis_size("band_0")
    other_quarter = lax.ppermute(quarter, "band_0", [(i, i ^ 1) for i in range(depth)])
    stats = lax.all_to_all(stats, ALL, 0, 0, tiled=True)
    stats = call(combine_kernel, jax.ShapeDtypeStruct((8, 128), F32), flops=1 << 20)(stats)

    mine = call(arrange_kernel, all_shape)(quarter, other_quarter)
    other = lax.ppermute(mine, "band_2", swap)
    joined, beside = call(
        join_kernel,
        [jax.ShapeDtypeStruct((2, 3 * D, COLS), BF16), jax.ShapeDtypeStruct((3 * D, 128), BF16)],
        (
            pltpu.VMEM((8, SIDE_ROWS, HALF), BF16),
            pltpu.VMEM((8, SIDE_ROWS, HALF), BF16),
        ),
        flops=2 * 2 * 256 * 256 * 512 * 7,
    )(own, first, second, full_lat, stats)
    keep, send, stats = call(
        conv_kernel,
        [half_shape, half_shape, stats_shape],
        (pltpu.VMEM((3, D, 3 * D), BF16), pltpu.VMEM((3, D, COLS), F32)),
        flops=2 * 2 * 256 * 256 * 512 * 9,
    )(joined, beside, mine, other)
    taken = lax.ppermute(send, "chan_1", swap)
    stats = lax.all_to_all(stats, ALL, 0, 0, tiled=True)
    log_probs = call(
        query_kernel,
        jax.ShapeDtypeStruct((2 * QUERIES * 4, 128), F32),
        (pltpu.VMEM((D, D), BF16),),
        flops=2 * 2 * 256 * 256 * 512 * 2,
    )(keep, taken, stats, full_lat, mine, other, queries)
    return log_probs.reshape(2, QUERIES, 1, COLS)


def solution(mesh):
    finer = Mesh(
        mesh.devices.reshape(8, 2, 2, 4, 2), ("band_0", "band_1", "band_2", "chan_0", "chan_1")
    )

    return jax.shard_map(
        per_device,
        mesh=finer,
        in_specs=(
            P(None, CHAN, BAND, None),
            P(None, CHAN, BAND, None),
            P(CHAN, None),
            P(CHAN),
            P(CHAN),
            P(None, None, CHAN, None),
            P(CHAN),
            P(CHAN),
            P(CHAN, None),
            P(CHAN),
            P(),
        ),
        out_specs=P(None, None, BAND + CHAN, None),
        check_vma=False,
    )
```

```python
import jax
import jax.numpy as jnp
from jax import lax
from jax.experimental import pallas as pl
from jax.experimental.pallas import tpu as pltpu
from jax.sharding import Mesh
from jax.sharding import PartitionSpec as P


D = 256
GROUPS = 32
IN_CH = 192
COLS = 512
HALF = 256
QUERIES = 200
BAND = ("band_0", "band_1", "band_2")
CHAN = ("chan_0", "chan_1")
ALL = BAND + CHAN
EPS = 1e-05
F32 = jnp.float32
BF16 = jnp.bfloat16
OWN_ROWS = 80
VECTORS = 64
FINE_EDGE = 72
COARSE_EDGE = 80
SIDE_ROWS = 96
MASK_AT = 72
XORS = (4, 1, 2, 5, 6, 3, 7)
SHARD_ROWS = 80


def dot(a, b):
    return lax.dot_general(a, b, (((1,), (0,)), ((), ())), preferred_element_type=F32)


def local_stats(values, lane, offset):
    blocks = values.reshape(GROUPS, D // GROUPS, COLS)
    count = D // GROUPS * COLS
    mean = jnp.sum(jnp.sum(blocks, axis=2, keepdims=True), axis=1, keepdims=True) / count
    dev = blocks - mean
    m2 = jnp.sum(jnp.sum(dev * dev, axis=2, keepdims=True), axis=1, keepdims=True)
    group = lax.broadcasted_iota(jnp.int32, (GROUPS, 1, 128), 0)
    row = jnp.where(lane == group + offset, mean, 0.0)
    row = row + jnp.where(lane == group + (offset + GROUPS), m2, 0.0)
    return jnp.sum(row, axis=0)


def combine(stats):
    devices = stats.shape[0]
    count = D // GROUPS * COLS
    mean = jnp.sum(stats, axis=0, keepdims=True) / devices
    dev = stats - mean
    spread = jnp.sum(dev * dev, axis=0, keepdims=True) * (1.0 / devices)
    return mean, spread, mean * (1.0 / count)


def stat_cols(rows, image):
    mean, spread, inner = rows
    lane = lax.broadcasted_iota(jnp.int32, (D, 128), 1)
    group = lax.broadcasted_iota(jnp.int32, (D, 128), 0) // (D // GROUPS)
    at_mean = lane == group + image * 2 * GROUPS
    at_m2 = lane == group + (image * 2 + 1) * GROUPS
    mean_col = jnp.sum(jnp.where(at_mean, mean, 0.0), axis=1, keepdims=True)
    var_col = jnp.sum(
        jnp.where(at_mean, spread, 0.0) + jnp.where(at_m2, inner, 0.0), axis=1, keepdims=True
    )
    return mean_col, var_col


def combine_kernel(stats_ref, rows_ref):
    mean, spread, inner = combine(stats_ref[...])
    rows_ref[0:1] = mean
    rows_ref[1:2] = spread
    rows_ref[2:3] = inner
    rows_ref[3:8] = jnp.zeros((5, 128), F32)


def vector_col(lat_weight_ref, index):
    return lat_weight_ref[:, 128:256].astype(F32)[:, VECTORS + index : VECTORS + index + 1]


def lanes_of(shape):
    return lax.broadcasted_iota(jnp.int32, shape, len(shape) - 1)


def fine_rows(ref, image, low, high):
    return jnp.concatenate(
        [ref[s, 24 * image : 24 * image + 24, low:high] for s in range(8)], axis=0
    )


def pack_own_kernel(fine_hbm, coarse_hbm, weight_hbm, *refs):
    vec_hbm, own_hbm = refs[:5], refs[5]
    fine_ref, coarse_ref, weight_ref, vec_ref, own_ref, rows, coarse, sems, out_sems = refs[6:]
    pairs = [(coarse_hbm, coarse_ref), (weight_hbm, weight_ref)]
    pairs += [(vec, vec_ref.at[i]) for i, vec in enumerate(vec_hbm)] + [(fine_hbm, fine_ref)]
    copies = [
        pltpu.make_async_copy(source, target, sems.at[i])
        for i, (source, target) in enumerate(pairs)
    ]
    for copy in copies:
        copy.start()
    for copy in copies[:-1]:
        copy.wait()
    for n in range(2):
        for t in range(2):
            piece = coarse_ref[n, :, :, 128 * t : 128 * t + 128].astype(F32)
            piece = jnp.concatenate([piece, jnp.zeros_like(piece)], axis=1)
            coarse[n, t, 0:256] = piece.reshape(256, 128)
    lane = lanes_of((32, 128))
    vec_lane = lanes_of((32, 32))
    vec_row = lax.broadcasted_iota(jnp.int32, (32, 32), 0)
    weight = weight_ref[...].astype(F32)
    second = jnp.concatenate([weight[:, 128:IN_CH], jnp.zeros((32, 256 - IN_CH), F32)], axis=1)
    for i in range(5):
        vec = jnp.where(vec_lane == vec_row, vec_ref[i].astype(F32), 0.0)
        second += jnp.where(lane == VECTORS + i, jnp.sum(vec, axis=1, keepdims=True), 0.0)
    first = weight[:, 0:128].astype(BF16)
    tails = []
    for h in range(2):
        for q in range(4):
            d = 2 * q + h
            tail = second
            own_ref[d, 48:64, 0:128] = first[0:16]
            own_ref[d, 48:64, 256:384] = first[16:32]
            for n in range(2):
                row = coarse[n, h, pl.ds(q, 32, stride=8), :].astype(BF16)
                own_ref[d, 64:80, 128 * n : 128 * n + 128] = row[0:16]
                own_ref[d, 64:80, 256 + 128 * n : 384 + 128 * n] = row[16:32]
                row = coarse[n, 1 - h, pl.ds(q, 32, stride=8), :]
                edge = row[:, 0:1] if h == 0 else row[:, 127:128]
                tail = jnp.where(lane // 4 == COARSE_EDGE // 4 + n, edge, tail)
            tails.append(tail)
    copies[-1].wait()
    for t in range(4):
        piece = fine_ref[:, :, :, 128 * t : 128 * t + 128].astype(F32)
        rows[t, 0:384] = piece.reshape(48 * 8, 128)
    out = []
    for h in range(2):
        for q in range(4):
            d = 2 * q + h
            tail = tails[4 * h + q]
            for r in range(2):
                for t in range(2):
                    row = rows[2 * h + t, pl.ds(2 * q + r, 48, stride=8), :]
                    at = 256 * r + 128 * t
                    own_ref[d, 0:48, at : at + 128] = row.astype(BF16)
                row = rows[2 - h, pl.ds(2 * q + r, 48, stride=8), :]
                edge = row[:, 0:1] if h == 0 else row[:, 127:128]
                for n in range(2):
                    column = jnp.concatenate(
                        [edge[24 * n : 24 * n + 24], jnp.zeros((8, 1), F32)], axis=0
                    )
                    tail = jnp.where(lane == FINE_EDGE + 4 * n + 1 + r, column, tail)
            tail = tail.astype(BF16)
            own_ref[d, 48:64, 128:256] = tail[0:16]
            own_ref[d, 48:64, 384:512] = tail[16:32]
            out.append(pltpu.make_async_copy(own_ref.at[d], own_hbm.at[d], out_sems.at[d]))
            out[-1].start()
    for copy in out:
        copy.wait()


def pack_weights_kernel(conv_ref, mask_ref, shard_ref):
    half = pl.multiple_of(16 * lax.axis_index("band_2"), 16)
    for k in range(10):
        if k < 9:
            piece = conv_ref[k // 3, k % 3, pl.ds(half, 16), :].astype(F32)
        else:
            piece = mask_ref[pl.ds(half, 16), :].astype(F32)
        piece = jnp.concatenate([piece[0:8], piece[8:16]], axis=1).astype(BF16)
        shard_ref[8 * k : 8 * k + 8] = piece


def arrange_kernel(*refs):
    chan = lax.axis_index("chan_0") * 2 + lax.axis_index("chan_1")
    all_ref = refs[-1]
    for k, ref in enumerate(refs[:-1]):
        all_ref[chan ^ k] = ref[...]


def lateral_kernel(own_ref, weight_ref, stats_ref, one_ref, two_ref):
    for s in range(8):
        for half in range(2):
            weight_ref[32 * s + 16 * half : 32 * s + 16 * half + 16, :] = own_ref[
                s, 48:64, 256 * half : 256 * half + 256
            ]
    odd = lax.axis_index("chan_0") % 2
    for ref, row in ((one_ref, 1 - odd), (two_ref, odd)):
        at = pl.multiple_of(256 * row, 256)
        for s in range(8):
            ref[s, 0:48, :] = own_ref[s, 0:48, pl.ds(at, 256)]
            ref[s, 48:64, :] = own_ref[s, 64:80, 0:256]
            ref[s, 64:80, :] = own_ref[s, 64:80, 256:512]
            ref[s, 80:96, 0:128] = own_ref[s, 48:64, 128:256]
            ref[s, 80:96, 128:256] = own_ref[s, 48:64, 384:512]
    lane = lax.broadcasted_iota(jnp.int32, (GROUPS, 1, 128), 2)
    total = jnp.zeros((1, 128), F32)
    for n in range(2):
        lateral = dot(weight_ref[:, 0:IN_CH], fine_rows(own_ref, n, 0, COLS))
        total = total + local_stats(lateral, lane, 64 * n)
    stats_ref[...] = jnp.broadcast_to(total, stats_ref.shape)


def join_kernel(
    own_ref, one_ref, two_ref, lat_weight_ref, lat_stats_ref, joined_ref, beside_ref,
    above_ref, below_ref,
):
    odd = lax.axis_index("chan_0") % 2 == 1
    for s in range(8):
        one, two = one_ref[s], two_ref[s]
        above_ref[s] = jnp.where(odd, one, two)
        below_ref[s] = jnp.where(odd, two, one)
    core = lax.axis_index("band_2")
    band = (lax.axis_index("band_0") * 2 + lax.axis_index("band_1")) * 2 + core
    side = lax.axis_index("chan_1")
    pair = band * 4 + lax.axis_index("chan_0")
    at_top = pair == 0
    at_bottom = pair == 127
    source = lax.broadcasted_iota(jnp.int32, (128, HALF), 0)
    column = lanes_of((128, HALF))
    inner_edge = jnp.where(side == 0, HALF - 1, 0)
    near = column // 2
    far = jnp.clip(near - 1 + 2 * (column % 2), 0, 127)
    spread = jnp.where(source == near, 0.75, 0.0) + jnp.where(
        jnp.logical_and(source == far, column != inner_edge), 0.25, 0.0
    )
    spreads = [
        jnp.concatenate([low * spread, (1.0 - low) * spread], axis=0).astype(BF16)
        for low in (0.75, 0.25)
    ]
    gain = vector_col(lat_weight_ref, 0)
    shift = vector_col(lat_weight_ref, 1)
    stats = (lat_stats_ref[0:1], lat_stats_ref[1:2], lat_stats_ref[2:3])
    lane_at = lanes_of((D, HALF))
    small = lanes_of((D, 128))
    first_image = small < 4
    time = small % 4
    norm = [stat_cols(stats, n) for n in range(2)]
    norm = [(mean, lax.rsqrt(var + EPS) * gain) for mean, var in norm]
    lat_weight = lat_weight_ref[:, 0:IN_CH]

    def coarse_main(ref, low, high, n):
        at = 128 * n
        if high is None:
            pieces = [ref[s, low : low + 32, at : at + 128] for s in range(8)]
        else:
            pieces = []
            for s in range(8):
                pieces.append(ref[s, low : low + 16, at : at + 128])
                pieces.append(ref[s, low : low + 16, high + at : high + at + 128])
        return jnp.concatenate(pieces, axis=0)

    def extras(tile, move):
        fine = jnp.concatenate([tile[32 * s : 32 * s + 24] for s in range(8)], axis=0)
        fine = pltpu.roll(dot(lat_weight, fine), 128 - FINE_EDGE + move, axis=1)
        return fine, pltpu.roll(tile.astype(F32), 128 - COARSE_EDGE, axis=1)

    def tile_of(ref):
        pieces = []
        for s in range(8):
            pieces.append(ref[s, 80:96, 0:128])
            pieces.append(ref[s, 80:96, 128:256])
        return jnp.concatenate(pieces, axis=0)

    fine_above, extra_above = extras(tile_of(above_ref), -2)
    fine_own, extra_own = extras(lat_weight_ref[:, 128:256], 0)
    fine_below, extra_below = extras(tile_of(below_ref), 2)
    extra_above = jnp.where(at_top, extra_own, extra_above)
    extra_below = jnp.where(at_bottom, extra_own, extra_below)
    mains = []
    for n in range(2):
        middle = coarse_main(own_ref, 64, 256, n)
        upper = coarse_main(above_ref, 48, None, n)
        lower = coarse_main(below_ref, 48, None, n)
        upper = jnp.where(at_top, middle, upper)
        lower = jnp.where(at_bottom, middle, lower)
        mains.append((upper, middle, lower))
    edge_at = jnp.where(side == 0, 127, 0)
    beyond, columns = [], []
    for k, extra in enumerate((extra_above, extra_own, extra_below)):
        edges = []
        for n in range(2):
            main = mains[n][k]
            edges.append(
                jnp.sum(jnp.where(small == edge_at, main.astype(F32), 0.0), axis=1, keepdims=True)
            )
        columns.append(0.75 * extra + 0.25 * jnp.where(first_image, edges[0], edges[1]))
        beyond.append(extra)

    lateral = jnp.where(
        time == 0, fine_above, jnp.where(time == 3, fine_below, fine_own)
    )
    upsampled = jnp.where(
        time == 0,
        0.75 * columns[0] + 0.25 * columns[1],
        jnp.where(
            time == 1,
            0.25 * columns[0] + 0.75 * columns[1],
            jnp.where(
                time == 2,
                0.75 * columns[1] + 0.25 * columns[2],
                0.25 * columns[1] + 0.75 * columns[2],
            ),
        ),
    )
    mean = jnp.where(first_image, norm[0][0], norm[1][0])
    scale = jnp.where(first_image, norm[0][1], norm[1][1])
    value = (lateral - mean) * scale + shift + upsampled
    outside = jnp.logical_or(
        jnp.logical_and(time == 0, at_top), jnp.logical_and(time == 3, at_bottom)
    )
    value = jnp.where(outside, 0.0, value)
    beside_ref[...] = jnp.concatenate(
        [value, pltpu.roll(value, 127, axis=1), pltpu.roll(value, 126, axis=1)], axis=0
    ).astype(BF16)

    for n in range(2):
        mean, scale = norm[n]
        both = [jnp.concatenate(mains[n][k : k + 2], axis=1) for k in range(2)]
        edge = [value[:, 4 * n : 4 * n + 1] for value in beyond]

        def upsampled_row(k, which):
            low = (0.75, 0.25)[which]
            outer = 0.25 * (low * edge[k] + (1.0 - low) * edge[k + 1])
            return dot(both[k], spreads[which]) + jnp.where(lane_at == inner_edge, outer, 0.0)

        rows = (
            (fine_rows(above_ref, n, 0, HALF), upsampled_row(0, 0)),
            (fine_rows(own_ref, n, 0, HALF), upsampled_row(0, 1)),
            (fine_rows(own_ref, n, HALF, COLS), upsampled_row(1, 0)),
            (fine_rows(below_ref, n, 0, HALF), upsampled_row(1, 1)),
        )
        for t, (fine, upsampled) in enumerate(rows):
            value = ((dot(lat_weight, fine) - mean) * scale + shift + upsampled).astype(BF16)
            if t == 0:
                value = jnp.where(at_top, jnp.zeros_like(value), value)
            if t == 3:
                value = jnp.where(at_bottom, jnp.zeros_like(value), value)
            for r in range(2):
                if 0 <= t - r <= 2:
                    joined_ref[
                        n, 256 * (t - r) : 256 * (t - r) + 256, HALF * r : HALF * r + HALF
                    ] = value


def conv_kernel(
    joined_ref, beside_ref, mine_ref, other_ref, keep_ref, send_ref, stats_ref, weight, taps
):
    core = lax.axis_index("band_2")
    side = lax.axis_index("chan_1")
    for part, ref in ((core, mine_ref), (1 - core, other_ref)):
        for s in range(8):
            at = pl.multiple_of(32 * s + 16 * part, 16)
            for a in range(3):
                for b in range(3):
                    piece = ref[s, (a * 3 + b) * 8 : (a * 3 + b) * 8 + 8, :]
                    both = jnp.concatenate([piece[:, 0:256], piece[:, 256:512]], axis=0)
                    weight[b, pl.ds(at, 16), 256 * a : 256 * a + 256] = both
    inner_edge = jnp.where(side == 0, HALF - 1, 0)
    lane = lax.broadcasted_iota(jnp.int32, (GROUPS, 1, 128), 2)
    lane_at = lanes_of((D, HALF))
    beside = dot(weight[jnp.where(side == 0, 2, 0)], beside_ref[...])
    total = jnp.zeros((1, 128), F32)
    for n in range(2):
        for b in range(3):
            taps[b] = dot(weight[b], joined_ref[n])
        out = []
        for r in range(2):
            at = HALF * r
            left = pltpu.roll(taps[0, :, at : at + HALF], 1, axis=1)
            right = pltpu.roll(taps[2, :, at : at + HALF], HALF - 1, axis=1)
            value = taps[1, :, at : at + HALF] + jnp.where(lane_at == 0, 0.0, left)
            value = value + jnp.where(lane_at == HALF - 1, 0.0, right)
            column = beside[:, 4 * n + r : 4 * n + r + 1]
            out.append(value + jnp.where(lane_at == inner_edge, column, 0.0))
        keep_ref[n] = jnp.where(side == 0, out[0], out[1])
        send_ref[n] = jnp.where(side == 0, out[1], out[0])
        total = total + local_stats(jnp.concatenate(out, axis=1), lane, 64 * n)
    stats_ref[...] = jnp.broadcast_to(total, stats_ref.shape)


def query_kernel(
    keep_ref, taken_ref, out_stats_ref, lat_weight_ref, mine_ref, other_ref,
    query_ref, out_ref, weight,
):
    core = lax.axis_index("band_2")
    side = lax.axis_index("chan_1")
    for part, ref in ((core, mine_ref), (1 - core, other_ref)):
        for s in range(8):
            at = pl.multiple_of(32 * s + 16 * part, 16)
            piece = ref[s, MASK_AT : MASK_AT + 8, :]
            both = jnp.concatenate([piece[:, 0:256], piece[:, 256:512]], axis=0)
            weight[pl.ds(at, 16), :] = both
    gain = vector_col(lat_weight_ref, 2)
    shift = vector_col(lat_weight_ref, 3)
    bias = vector_col(lat_weight_ref, 4)
    rows = combine(out_stats_ref[...])
    for n in range(2):
        mean, var = stat_cols(rows, n)
        scale = lax.rsqrt(var + EPS) * gain
        for ref, half in ((keep_ref, side), (taken_ref, 1 - side)):
            activated = jnp.maximum((ref[n] - mean) * scale + shift, 0.0).astype(BF16)
            features = (dot(weight[...], activated) + bias).astype(BF16)
            logits = dot(query_ref[...], features)
            shifted = logits - jnp.max(logits, axis=0, keepdims=True)
            result = shifted - jnp.log(jnp.sum(jnp.exp(shifted), axis=0, keepdims=True))
            for t in range(2):
                at = 4 * QUERIES * n + 2 * half + t
                out_ref[pl.ds(at, QUERIES, stride=4), :] = result[:, 128 * t : 128 * t + 128]


def call(kernel, out_shape, scratch=(), flops=0, space=pltpu.VMEM, out_space=pltpu.VMEM, limit=40 << 20):
    out = pl.BlockSpec(memory_space=out_space)
    single = not isinstance(out_shape, (tuple, list))
    return lambda *args: pl.pallas_call(
        kernel,
        out_shape=out_shape,
        in_specs=[pl.BlockSpec(memory_space=space)] * len(args),
        out_specs=out if single else [out] * len(out_shape),
        scratch_shapes=list(scratch),
        cost_estimate=pl.CostEstimate(flops=flops, bytes_accessed=1 << 20, transcendentals=0),
        compiler_params=pltpu.CompilerParams(vmem_limit_bytes=limit),
    )(*args)


def per_device(
    fine_features,
    coarse_level,
    lat_weight,
    lat_gain,
    lat_shift,
    out_weight,
    out_gain,
    out_shift,
    mask_weight,
    mask_bias,
    queries,
):
    everyone = lax.axis_size(ALL)
    stats_shape = jax.ShapeDtypeStruct((everyone, 128), F32)
    shard_shape = jax.ShapeDtypeStruct((SHARD_ROWS, COLS), BF16)
    all_shape = jax.ShapeDtypeStruct((8, SHARD_ROWS, COLS), BF16)
    side_shape = jax.ShapeDtypeStruct((8, SIDE_ROWS, HALF), BF16)
    half_shape = jax.ShapeDtypeStruct((2, D, HALF), F32)
    swap = [(0, 1), (1, 0)]

    vectors = [v.reshape(1, 32) for v in (lat_gain, lat_shift, out_gain, out_shift, mask_bias)]
    own_out = call(
        pack_own_kernel,
        jax.ShapeDtypeStruct((8, OWN_ROWS, COLS), BF16),
        (
            pltpu.VMEM((2, 24, 8, COLS), BF16),
            pltpu.VMEM((2, 32, 4, 256), BF16),
            pltpu.VMEM((32, IN_CH), BF16),
            pltpu.VMEM((5, 1, 32), BF16),
            pltpu.VMEM((8, OWN_ROWS, COLS), BF16),
            pltpu.VMEM((4, 48 * 8 + 8, 128), F32),
            pltpu.VMEM((2, 2, 256 + 8, 128), F32),
            pltpu.SemaphoreType.DMA((8,)),
            pltpu.SemaphoreType.DMA((8,)),
        ),
        space=pltpu.HBM,
        out_space=pltpu.HBM,
        limit=60 << 20,
    )(fine_features, coarse_level, lat_weight, *vectors)
    own = lax.all_to_all(own_out, CHAN, 0, 0, tiled=True)
    shard = call(pack_weights_kernel, shard_shape)(out_weight, mask_weight)
    moved = [lax.ppermute(shard, CHAN, [(i, i ^ k) for i in range(8)]) for k in XORS]

    full_lat, stats, first, second = call(
        lateral_kernel,
        [jax.ShapeDtypeStruct((D, 256), BF16), stats_shape, side_shape, side_shape],
        flops=2 * 2 * 256 * 256 * 512,
    )(own)
    pairs = everyone // 2
    swap_at = lambda shift: [
        (2 * p + yl, 2 * ((((p + shift) % pairs ^ 1) - shift) % pairs) + yl)
        for p in range(pairs)
        for yl in range(2)
    ]
    first = lax.ppermute(first, ALL, swap_at(0))
    second = lax.ppermute(second, ALL, swap_at(1))
    stats = lax.all_to_all(stats, ALL, 0, 0, tiled=True)
    stats = call(combine_kernel, jax.ShapeDtypeStruct((8, 128), F32), flops=1 << 20)(stats)

    by_xor = dict(zip(XORS, moved))
    mine = call(arrange_kernel, all_shape)(shard, *[by_xor[k] for k in range(1, 8)])
    other = lax.ppermute(mine, "band_2", swap)
    joined, beside = call(
        join_kernel,
        [jax.ShapeDtypeStruct((2, 3 * D, COLS), BF16), jax.ShapeDtypeStruct((3 * D, 128), BF16)],
        (
            pltpu.VMEM((8, SIDE_ROWS, HALF), BF16),
            pltpu.VMEM((8, SIDE_ROWS, HALF), BF16),
        ),
        flops=2 * 2 * 256 * 256 * 512 * 7,
    )(own, first, second, full_lat, stats)
    keep, send, stats = call(
        conv_kernel,
        [half_shape, half_shape, stats_shape],
        (pltpu.VMEM((3, D, 3 * D), BF16), pltpu.VMEM((3, D, COLS), F32)),
        flops=2 * 2 * 256 * 256 * 512 * 9,
    )(joined, beside, mine, other)
    taken = lax.ppermute(send, "chan_1", swap)
    stats = lax.all_to_all(stats, ALL, 0, 0, tiled=True)
    log_probs = call(
        query_kernel,
        jax.ShapeDtypeStruct((2 * QUERIES * 4, 128), F32),
        (pltpu.VMEM((D, D), BF16),),
        flops=2 * 2 * 256 * 256 * 512 * 2,
    )(keep, taken, stats, full_lat, mine, other, queries)
    return log_probs.reshape(2, QUERIES, 1, COLS)


def solution(mesh):
    finer = Mesh(
        mesh.devices.reshape(8, 2, 2, 4, 2), ("band_0", "band_1", "band_2", "chan_0", "chan_1")
    )

    return jax.shard_map(
        per_device,
        mesh=finer,
        in_specs=(
            P(None, CHAN, BAND, None),
            P(None, CHAN, BAND, None),
            P(CHAN, None),
            P(CHAN),
            P(CHAN),
            P(None, None, CHAN, None),
            P(CHAN),
            P(CHAN),
            P(CHAN, None),
            P(CHAN),
            P(),
        ),
        out_specs=P(None, None, BAND + CHAN, None),
        check_vma=False,
    )
```
